32 devices in a mesh: fsdp: 8 (over z, x), tp: 4 (over y, core).
Axes of the slice: x: 2, y: 2, z: 4, core: 2. Of those that a mesh axis runs over, the one named last changes fastest.
Arguments:
- block_input: bfloat16 [2, 2048, 2048], P(None, 'fsdp'), may hold values from -6 to 6
- doc_lengths: int32 [2, 6], replicated, may hold values from 1 to 1536, 2048 in all within a row
- ln1_gain: float32 [2048], replicated, may hold values from 0.5 to 1.5
- ln1_bias: float32 [2048], replicated, may hold values from -2 to 2
- w_qkv: bfloat16 [2048, 3, 2048], P('fsdp', None, 'tp'), may hold values from -0.125 to 0.125
- qkv_bias: float32 [3, 2048], P(None, 'tp'), may hold values from -2 to 2
- w_out: bfloat16 [2048, 2048], P('fsdp', 'tp'), may hold values from -2 to 2
- ln2_gain: float32 [2048], replicated, may hold values from 0.5 to 1.5
- ln2_bias: float32 [2048], replicated, may hold values from -2 to 2
- w_gate_up: bfloat16 [2048, 2, 5632], P('fsdp', None, 'tp'), may hold values from -0.125 to 0.125
- w_down: bfloat16 [2048, 5632], P('fsdp', 'tp'), may hold values from -0.078125 to 0.078125
- grad_y: bfloat16 [2, 2048, 2048], P(None, 'fsdp'), may hold values from -6 to 6
Outputs:
- block_output: bfloat16 [2, 2048, 2048], P(None, 'fsdp')
- grad_input: bfloat16 [2, 2048, 2048], P(None, 'fsdp')
- grad_ln1_gain: float32 [2048], replicated
- grad_ln1_bias: float32 [2048], replicated
- grad_w_qkv: float32 [2048, 3, 2048], P('fsdp', None, 'tp')
- grad_qkv_bias: float32 [3, 2048], P(None, 'tp')
- grad_w_out: float32 [2048, 2048], P('fsdp', 'tp')
- grad_ln2_gain: float32 [2048], replicated
- grad_ln2_bias: float32 [2048], replicated
- grad_w_gate_up: float32 [2048, 2, 5632], P('fsdp', None, 'tp')
- grad_w_down: float32 [2048, 5632], P('fsdp', 'tp')
The draws below stay inside these ranges and needn't reach their ends.
Inputs may be any that keep to these rules, and one draw needn't show every extreme that they name: `doc_lengths`: each row sums to 2048, and in each row the longest document has exactly 1536 tokens.
All inputs are finite; a program needn't handle non-finite values.
Results may differ from the reference program's by a relative error of at most 0.025.
Values may be sent and summed in bfloat16 or wider, within the bound.
A program may use at most 256 MiB of HBM per device.

```python
import math
import jax
import jax.numpy as jnp
import numpy as np
from jax import lax

D = 2048
HEADS = 32
HD = 64
ROT = 16
FF = 5632
LEN = 2048
MAX_DOC = 1536
DOCS = 6
SEQS = 2


def level_of(rng, shape, pieces, least, high):
    def one(position, shards_of):
        heights = jax.random.uniform(jax.random.fold_in(jax.random.fold_in(rng, 6), position), (shards_of,), jnp.float32, least / len(pieces), high / len(pieces))
        return jnp.repeat(jnp.exp(heights), shape[position] // shards_of).reshape((-1,) + (1,) * (len(shape) - position - 1))

    gain = one(*pieces[0])
    for cut in pieces[1:]:
        gain = gain * one(*cut)
    return gain


def profile(count, total, limit, slope):
    portions = [(1 << 20) // math.isqrt(rank ** slope) + 1 for rank in range(2, count + 1)]
    rest, given = total - limit - (count - 1), [1] * (count - 1)
    while rest > 0:
        candidates = [i for i in range(count - 1) if given[i] < limit]
        whole, left = sum([portions[i] for i in candidates]), rest
        for i in candidates:
            more = min(limit - given[i], max(1, left * portions[i] // whole), rest)
            given[i] = given[i] + more
            rest = rest - more
    return np.array([limit] + given)


def uneven_parts(stream_key, count, total, most, slope):
    if count == 2:
        one = jax.random.randint(stream_key, (), max(1, total - most), min(most, total - 1) + 1)
        return jnp.stack([one, total - one])
    sizes = jnp.asarray(profile(count, total, most, slope), jnp.int32)
    couples = (count - 1) // 2
    donor, sink = sizes[1:1 + 2 * couples:2], sizes[2:2 + 2 * couples:2]
    margin = jnp.minimum(donor - 1, most - sink)
    moved = jax.random.randint(jax.random.fold_in(stream_key, 1), (couples,), 0, 1 << 20) % (margin + 1)
    sizes = sizes.at[1:1 + 2 * couples:2].set(donor - moved).at[2:2 + 2 * couples:2].set(sink + moved)
    return sizes[jax.random.permutation(jax.random.fold_in(stream_key, 2), count)]


def bell_draw(own_key, shape, width, limit, split=(), held_as=jnp.bfloat16):
    result = width * jax.random.normal(own_key, shape, jnp.float32)
    if split:
        result = result * level_of(own_key, shape, split, -0.22, 0.18)
    return jnp.clip(result, -limit, limit).astype(held_as)


def setup_inputs(seed: int = 0) -> dict:
    streams_of = jax.random.split(jax.random.key(seed), 13)
    block_input = bell_draw(streams_of[0], (SEQS, LEN, D), 1.0, 6.0, ((1, 8),))
    doc_lengths = jax.vmap(lambda own: uneven_parts(own, DOCS, LEN, MAX_DOC, 2))(jax.random.split(streams_of[1], SEQS)).reshape((SEQS, DOCS)).astype(jnp.int32)
    ln1_gain = jnp.clip(1.0 + 0.1 * jax.random.normal(streams_of[2], (D,), jnp.float32), 0.5, 1.5)
    ln1_bias = bell_draw(streams_of[3], (D,), 0.3, 2.0, (), jnp.float32)
    w_qkv = bell_draw(streams_of[4], (D, 3, D), D ** -0.5, 0.125, ((0, 8), (2, 4)))
    qkv_bias = bell_draw(streams_of[5], (3, D), 0.5, 2.0, ((1, 4),), jnp.float32)
    w_out = bell_draw(streams_of[6], (D, D), (max(D // 256, 4)) ** -0.5, 2.0, ((0, 8), (1, 4)))
    ln2_gain = jnp.clip(1.0 + 0.1 * jax.random.normal(streams_of[7], (D,), jnp.float32), 0.5, 1.5)
    ln2_bias = bell_draw(streams_of[8], (D,), 0.3, 2.0, (), jnp.float32)
    w_gate_up = bell_draw(streams_of[9], (D, 2, FF), D ** -0.5, 0.125, ((0, 8), (2, 4)))
    w_down = bell_draw(streams_of[10], (D, FF), FF ** -0.5, 0.078125, ((0, 8), (1, 4)))
    grad_y = bell_draw(streams_of[11], (SEQS, LEN, D), 1.0, 6.0, ((1, 8),))
    return dict(block_input=block_input, doc_lengths=doc_lengths, ln1_gain=ln1_gain, ln1_bias=ln1_bias, w_qkv=w_qkv, qkv_bias=qkv_bias, w_out=w_out, ln2_gain=ln2_gain, ln2_bias=ln2_bias, w_gate_up=w_gate_up, w_down=w_down, grad_y=grad_y)


epsilon = 1e-05

def layer_norm(matrix_in, norm_gain, norm_shift):
    center = lax.optimization_barrier(jnp.mean(matrix_in, axis=-1, keepdims=True))
    centered = matrix_in - center
    spread = lax.optimization_barrier(jnp.mean(centered * centered, axis=-1, keepdims=True))
    inverse = lax.rsqrt(spread + epsilon)
    normed = centered * inverse
    return (normed * norm_gain + norm_shift, normed, inverse)

def norm_back(incoming, normed, inverse, norm_gain):
    scaled = incoming * norm_gain
    first_mean = lax.optimization_barrier(jnp.mean(scaled, axis=-1, keepdims=True))
    cross_mean = lax.optimization_barrier(jnp.mean(scaled * normed, axis=-1, keepdims=True))
    return inverse * (scaled - first_mean - normed * cross_mean)

def doc_layout(lengths, places):
    doc_ends = jnp.cumsum(lengths, axis=-1).astype(jnp.int32)
    passed = (places[:, :, None] >= doc_ends[:, None, :]).astype(jnp.int32)
    segment = lax.optimization_barrier(jnp.sum(passed, axis=-1)).astype(jnp.int32)
    begins = lax.optimization_barrier(jnp.sum(passed * lengths[:, None, :], axis=-1)).astype(jnp.int32)
    return (segment, places - begins)

def rotary_tables(offset):
    halfway = ROT // 2
    exponent = jnp.arange(halfway, dtype=jnp.float32) * (2.0 / ROT)
    frequency = jnp.exp(-math.log(10000.0) * exponent)
    angles = offset.astype(jnp.float32)[..., None] * frequency
    return (jnp.cos(angles), jnp.sin(angles))

def rotate(head_rows, cosine_table, sine_table, direction):
    halfway = ROT // 2
    leading = head_rows[..., :halfway]
    behind = head_rows[..., halfway:ROT]
    cosine_part = cosine_table[..., None, :]
    sine_part = sine_table[..., None, :] * direction
    return jnp.concatenate([leading * cosine_part - behind * sine_part, behind * cosine_part + leading * sine_part, head_rows[..., ROT:]], axis=-1)

def reference(block_input, doc_lengths, ln1_gain, ln1_bias, w_qkv, qkv_bias, w_out, ln2_gain, ln2_bias, w_gate_up, w_down, grad_y):
    floats = jnp.float32
    halves = jnp.bfloat16
    factor = 1.0 / math.sqrt(HD)
    flat_qkv = w_qkv.reshape(D, 3 * D)
    flat_gate_up = w_gate_up.reshape(D, 2 * FF)
    bias_heads = qkv_bias.reshape(3, HEADS, HD)
    places = jnp.arange(LEN, dtype=jnp.int32)

    def one_sequence(totals, inputs):
        seq_rows, seq_lengths, seq_grad = inputs
        segment, offset = doc_layout(seq_lengths[None, :], places[None, :])
        segment = segment[0]
        offset = offset[0]
        allowed = (segment[:, None] == segment[None, :]) & (places[None, :] <= places[:, None])
        cosine_table, sine_table = rotary_tables(offset)
        input_wide = seq_rows.astype(floats)
        first_norm, normed1, inverse1 = layer_norm(input_wide, ln1_gain, ln1_bias)
        first_low = first_norm.astype(halves)
        projected = jnp.dot(first_low, flat_qkv, preferred_element_type=floats).reshape(LEN, 3, HEADS, HD) + bias_heads
        query = rotate(projected[:, 0], cosine_table, sine_table, 1.0).astype(halves)
        key_rows = rotate(projected[:, 1], cosine_table, sine_table, 1.0).astype(halves)
        value_rows = projected[:, 2].astype(halves)
        query_heads = jnp.swapaxes(query, 0, 1)
        key_heads = jnp.swapaxes(key_rows, 0, 1)
        value_heads = jnp.swapaxes(value_rows, 0, 1)

        def head_forward(operands):
            query_head, key_head, value_head = operands
            scores = jnp.dot(query_head, key_head.T, preferred_element_type=floats) * factor
            scores = jnp.where(allowed, scores, -jnp.inf)
            highest = lax.optimization_barrier(jnp.max(scores, axis=-1, keepdims=True))
            weights = jnp.exp(scores - highest)
            denominator = lax.optimization_barrier(jnp.sum(weights, axis=-1, keepdims=True))
            output_head = (jnp.dot(weights.astype(halves), value_head, preferred_element_type=floats) / denominator).astype(halves)
            return (output_head, (highest + jnp.log(denominator))[:, 0])
        attended_heads, lse_heads = lax.map(head_forward, (query_heads, key_heads, value_heads))
        attended = jnp.swapaxes(attended_heads, 0, 1).reshape(LEN, D)
        residual = input_wide + jnp.dot(attended, w_out.T, preferred_element_type=floats)
        second_norm, normed2, inverse2 = layer_norm(residual, ln2_gain, ln2_bias)
        second_low = second_norm.astype(halves)
        gate_up = jnp.dot(second_low, flat_gate_up, preferred_element_type=floats).reshape(LEN, 2, FF)
        gate = gate_up[:, 0]
        up_part = gate_up[:, 1]
        sigmoid_gate = jax.nn.sigmoid(gate)
        hidden = (gate * sigmoid_gate * up_part).astype(halves)
        block_output = (residual + jnp.dot(hidden, w_down.T, preferred_element_type=floats)).astype(halves)
        grad_hidden = jnp.dot(seq_grad, w_down, preferred_element_type=floats)
        grad_gate = grad_hidden * up_part * sigmoid_gate * (1.0 + gate * (1.0 - sigmoid_gate))
        grad_upper = grad_hidden * gate * sigmoid_gate
        grad_gate_up = jnp.stack([grad_gate, grad_upper], axis=1).astype(halves).reshape(LEN, 2 * FF)
        grad_second = jnp.dot(grad_gate_up, flat_gate_up.T, preferred_element_type=floats)
        grad_residual = seq_grad.astype(floats) + norm_back(grad_second, normed2, inverse2, ln2_gain)
        residual_low = grad_residual.astype(halves)
        grad_attended = jnp.dot(residual_low, w_out, preferred_element_type=floats).astype(halves)
        delta = lax.optimization_barrier(jnp.sum((grad_attended.astype(floats) * attended.astype(floats)).reshape(LEN, HEADS, HD), axis=-1))
        grad_heads = jnp.swapaxes(grad_attended.reshape(LEN, HEADS, HD), 0, 1)

        def head_backward(operands):
            query_head, key_head, value_head, grad_head, lse_head, delta_head = operands
            scores = jnp.dot(query_head, key_head.T, preferred_element_type=floats) * factor
            softmax_out = jnp.where(allowed, jnp.exp(scores - lse_head[:, None]), 0.0)
            grad_probs = jnp.dot(grad_head, value_head.T, preferred_element_type=floats)
            grad_scores = (softmax_out * (grad_probs - delta_head[:, None]) * factor).astype(halves)
            grad_query = jnp.dot(grad_scores, key_head, preferred_element_type=floats)
            grad_key = jnp.dot(grad_scores.T, query_head, preferred_element_type=floats)
            grad_value = jnp.dot(softmax_out.astype(halves).T, grad_head, preferred_element_type=floats)
            return (grad_query, grad_key, grad_value)
        grad_query, grad_key, grad_value = lax.map(head_backward, (query_heads, key_heads, value_heads, grad_heads, lse_heads, delta.T))
        grad_query = rotate(jnp.swapaxes(grad_query, 0, 1), cosine_table, sine_table, -1.0)
        grad_key = rotate(jnp.swapaxes(grad_key, 0, 1), cosine_table, sine_table, -1.0)
        grad_value = jnp.swapaxes(grad_value, 0, 1)
        grad_projected = jnp.stack([grad_query, grad_key, grad_value], axis=1)
        grad_bias = lax.optimization_barrier(jnp.sum(grad_projected, axis=0)).reshape(3, D)
        grad_qkv = grad_projected.astype(halves).reshape(LEN, 3 * D)
        grad_first = jnp.dot(grad_qkv, flat_qkv.T, preferred_element_type=floats)
        grad_input = (grad_residual + norm_back(grad_first, normed1, inverse1, ln1_gain)).astype(halves)
        g_ln1_gain, g_ln1_bias, g_qkv, g_bias, g_out, g_ln2_gain, g_ln2_bias, g_gate_up, g_down = totals
        g_ln1_gain = g_ln1_gain + lax.optimization_barrier(jnp.sum(grad_first * normed1, axis=0))
        g_ln1_bias = g_ln1_bias + lax.optimization_barrier(jnp.sum(grad_first, axis=0))
        g_qkv = g_qkv + jnp.dot(first_low.T, grad_qkv, preferred_element_type=floats)
        g_bias = g_bias + grad_bias
        g_out = g_out + jnp.dot(residual_low.T, attended, preferred_element_type=floats)
        g_ln2_gain = g_ln2_gain + lax.optimization_barrier(jnp.sum(grad_second * normed2, axis=0))
        g_ln2_bias = g_ln2_bias + lax.optimization_barrier(jnp.sum(grad_second, axis=0))
        g_gate_up = g_gate_up + jnp.dot(second_low.T, grad_gate_up, preferred_element_type=floats)
        g_down = g_down + jnp.dot(seq_grad.T, hidden, preferred_element_type=floats)
        totals = (g_ln1_gain, g_ln1_bias, g_qkv, g_bias, g_out, g_ln2_gain, g_ln2_bias, g_gate_up, g_down)
        return (totals, (block_output, grad_input))
    start_totals = (jnp.zeros((D,), floats), jnp.zeros((D,), floats), jnp.zeros((D, 3 * D), floats), jnp.zeros((3, D), floats), jnp.zeros((D, D), floats), jnp.zeros((D,), floats), jnp.zeros((D,), floats), jnp.zeros((D, 2 * FF), floats), jnp.zeros((D, FF), floats))
    totals, outputs = lax.scan(one_sequence, start_totals, (block_input, doc_lengths, grad_y))
    g_ln1_gain, g_ln1_bias, g_qkv, g_bias, g_out, g_ln2_gain, g_ln2_bias, g_gate_up, g_down = totals
    block_output, grad_input = outputs
    return (block_output, grad_input, g_ln1_gain, g_ln1_bias, g_qkv.reshape(D, 3, D), g_bias, g_out, g_ln2_gain, g_ln2_bias, g_gate_up.reshape(D, 2, FF), g_down)
```

```python
import functools
import math

import jax
import jax.numpy as jnp
from jax import lax
from jax.experimental import pallas as pl
from jax.experimental.pallas import tpu as pltpu
from jax.sharding import Mesh
from jax.sharding import PartitionSpec as P

HD = 64
ROT = 16
LEN = 2048
SEQ_MB = 1
MICRO = 2


epsilon = 1e-05
negative = -1e30


def layer_norm(matrix_in, norm_gain, norm_shift):
    center = jnp.mean(matrix_in, axis=-1, keepdims=True)
    centered = matrix_in - center
    spread = jnp.mean(centered * centered, axis=-1, keepdims=True)
    inverse = lax.rsqrt(spread + epsilon)
    normed = centered * inverse
    return (normed * norm_gain + norm_shift, normed, inverse)


def norm_back(incoming, normed, inverse, norm_gain):
    scaled = incoming * norm_gain
    first_mean = jnp.mean(scaled, axis=-1, keepdims=True)
    cross_mean = jnp.mean(scaled * normed, axis=-1, keepdims=True)
    return inverse * (scaled - first_mean - normed * cross_mean)


def doc_layout(lengths, places):
    doc_ends = jnp.cumsum(lengths, axis=-1)
    passed = (places[:, :, None] >= doc_ends[:, None, :]).astype(jnp.int32)
    segment = jnp.sum(passed, axis=-1)
    begins = jnp.sum(passed * lengths[:, None, :], axis=-1)
    return (segment, places - begins)


def rotary_tables(offset):
    halfway = ROT // 2
    exponent = jnp.arange(halfway, dtype=jnp.float32) * (2.0 / ROT)
    frequency = jnp.exp(-math.log(10000.0) * exponent)
    angles = offset.astype(jnp.float32)[..., None] * frequency
    return (jnp.cos(angles), jnp.sin(angles))


def rotate(head_rows, cosine_table, sine_table, direction):
    halfway = ROT // 2
    leading = head_rows[..., :halfway]
    behind = head_rows[..., halfway:ROT]
    cosine_part = cosine_table[..., None, :]
    sine_part = sine_table[..., None, :] * direction
    return jnp.concatenate(
        [
            leading * cosine_part - behind * sine_part,
            behind * cosine_part + leading * sine_part,
            head_rows[..., ROT:],
        ],
        axis=-1,
    )


def pair_mask(query_seg, query_place, key_seg, key_place):
    same_doc = query_seg[:, :, None] == key_seg[:, None, :]
    causal = key_place[:, None, :] <= query_place[:, :, None]
    return (same_doc & causal)[:, :, None, :]


def fold_blocks(update, folded, part_arrays, block_len):
    extent = part_arrays[0].shape[1]
    number = extent // block_len
    blocks = tuple(
        (
            jnp.swapaxes(
                part_array.reshape((part_array.shape[0], number, block_len) + part_array.shape[2:]),
                0,
                1,
            )
            for part_array in part_arrays
        )
    )

    def advance(running, element):
        block_index, block_parts = element
        return (update(running, block_parts, block_index * block_len), None)

    folded, unused = lax.scan(advance, folded, (jnp.arange(number, dtype=jnp.int32), blocks))
    return folded


def fetch_weights(w_qkv, w_out, w_gate_up, w_down):
    return (
        lax.all_gather(w_qkv, "fsdp", axis=0, tiled=True),
        lax.all_gather(w_out, "fsdp", axis=0, tiled=True),
        lax.all_gather(w_gate_up, "fsdp", axis=0, tiled=True),
        lax.all_gather(w_down, "fsdp", axis=0, tiled=True),
    )


def on_device(
    block_input,
    doc_lengths,
    ln1_gain,
    ln1_bias,
    w_qkv,
    qkv_bias,
    w_out,
    ln2_gain,
    ln2_bias,
    w_gate_up,
    w_down,
    grad_y,
):
    floats = jnp.float32
    halves = jnp.bfloat16
    factor = 1.0 / math.sqrt(HD)
    per_batch = SEQ_MB
    shard_len = block_input.shape[1]
    model_width = block_input.shape[2]
    head_cols = qkv_bias.shape[1]
    heads_local = head_cols // HD
    hidden_cols = w_down.shape[1]
    row_count = per_batch * shard_len
    rows_owned = model_width // lax.axis_size("fsdp")
    first_row = lax.axis_index("fsdp") * shard_len
    query_place = jnp.broadcast_to(
        first_row + jnp.arange(shard_len, dtype=jnp.int32), (per_batch, shard_len)
    )
    key_block = min(LEN, 512)
    block_count = LEN // key_block
    g_ln1_gain = jnp.zeros((model_width,), floats)
    g_ln1_bias = jnp.zeros((model_width,), floats)
    g_ln2_gain = jnp.zeros((model_width,), floats)
    g_ln2_bias = jnp.zeros((model_width,), floats)
    g_bias = jnp.zeros((3, head_cols), floats)
    stored = []
    output_parts = []
    input_grads = []
    for batch in range(MICRO):
        lower = batch * per_batch
        seq_rows = block_input[lower : lower + per_batch]
        lengths = doc_lengths[lower : lower + per_batch]
        seq_grad = grad_y[lower : lower + per_batch]
        query_seg, offset = doc_layout(lengths, query_place)
        cosine_table, sine_table = rotary_tables(offset)
        gathered = fetch_weights(w_qkv, w_out, w_gate_up, w_down)
        full_qkv, full_out, full_gate_up, full_down = gathered
        input_wide = seq_rows.reshape(row_count, model_width).astype(floats)
        first_norm, normed1, inverse1 = layer_norm(input_wide, ln1_gain, ln1_bias)
        first_low = first_norm.astype(halves)
        projected = (
            jnp.dot(
                first_low,
                full_qkv.reshape(model_width, 3 * head_cols),
                preferred_element_type=floats,
            ).reshape(row_count, 3, head_cols)
            + qkv_bias
        )
        projected = projected.reshape(per_batch, shard_len, 3, heads_local, HD)
        query_heads = rotate(projected[:, :, 0], cosine_table, sine_table, 1.0).astype(halves)
        key_heads = rotate(projected[:, :, 1], cosine_table, sine_table, 1.0).astype(halves)
        value_heads = projected[:, :, 2].astype(halves)
        key_flat = key_heads.reshape(per_batch, shard_len, head_cols)
        value_flat = value_heads.reshape(per_batch, shard_len, head_cols)

        def attend(running, block_parts, offset_at):
            key_part, value_part = block_parts
            extent = key_part.shape[1]
            key_place = jnp.broadcast_to(
                offset_at + jnp.arange(extent, dtype=jnp.int32), (per_batch, extent)
            )
            key_seg = doc_layout(lengths, key_place)[0]
            allowed = pair_mask(query_seg, query_place, key_seg, key_place)
            scores = (
                jnp.einsum(
                    "sqhd,skhd->sqhk",
                    query_heads,
                    key_part.reshape(per_batch, extent, heads_local, HD),
                    preferred_element_type=floats,
                )
                * factor
            )
            scores = jnp.where(allowed, scores, negative)
            highest, denominator, summed = running
            new_high = jnp.maximum(highest, jnp.max(scores, axis=-1))
            shrink = jnp.exp(highest - new_high)
            weights = jnp.where(allowed, jnp.exp(scores - new_high[..., None]), 0.0)
            denominator = denominator * shrink + jnp.sum(weights, axis=-1)
            summed = summed * shrink[..., None] + jnp.einsum(
                "sqhk,skhd->sqhd",
                weights.astype(halves),
                value_part.reshape(per_batch, extent, heads_local, HD),
                preferred_element_type=floats,
            )
            return (new_high, denominator, summed)

        start_state = (
            jnp.full((per_batch, shard_len, heads_local), negative, floats),
            jnp.zeros((per_batch, shard_len, heads_local), floats),
            jnp.zeros((per_batch, shard_len, heads_local, HD), floats),
        )
        highest, denominator, summed = fold_blocks(
            attend,
            start_state,
            (
                lax.all_gather(key_flat, "fsdp", axis=1, tiled=True),
                lax.all_gather(value_flat, "fsdp", axis=1, tiled=True),
            ),
            key_block,
        )
        lse_rows = highest + jnp.log(denominator)
        attended = (summed / denominator[..., None]).astype(halves).reshape(row_count, head_cols)
        attn_part = jnp.einsum("rc,oc->ro", attended, full_out, preferred_element_type=floats)
        residual = input_wide + lax.psum(attn_part.astype(jnp.bfloat16), "tp").astype(jnp.float32)
        second_norm, normed2, inverse2 = layer_norm(residual, ln2_gain, ln2_bias)
        second_low = second_norm.astype(halves)
        gate_up = jnp.dot(
            second_low,
            full_gate_up.reshape(model_width, 2 * hidden_cols),
            preferred_element_type=floats,
        ).reshape(row_count, 2, hidden_cols)
        gate = gate_up[:, 0]
        up_part = gate_up[:, 1]
        sigmoid_gate = jax.nn.sigmoid(gate)
        hidden = (gate * sigmoid_gate * up_part).astype(halves)
        ffn_part = jnp.einsum("rf,of->ro", hidden, full_down, preferred_element_type=floats)
        residual_out = residual + lax.psum(ffn_part.astype(jnp.bfloat16), "tp").astype(jnp.float32)
        output_parts.append(residual_out.astype(halves).reshape(per_batch, shard_len, model_width))
        full_qkv, full_out, full_gate_up, full_down = (
            lax.all_gather(w_qkv, "fsdp", axis=0, tiled=True),
            lax.all_gather(w_out, "fsdp", axis=0, tiled=True),
            lax.all_gather(w_gate_up, "fsdp", axis=0, tiled=True),
            lax.all_gather(w_down, "fsdp", axis=0, tiled=True),
        )
        grad_rows = seq_grad.reshape(row_count, model_width)
        grad_hidden = jnp.dot(grad_rows, full_down, preferred_element_type=floats)
        grad_gate = grad_hidden * up_part * sigmoid_gate * (1.0 + gate * (1.0 - sigmoid_gate))
        grad_upper = grad_hidden * gate * sigmoid_gate
        grad_gate_up = (
            jnp.stack([grad_gate, grad_upper], axis=1)
            .astype(halves)
            .reshape(row_count, 2 * hidden_cols)
        )
        second_part = jnp.einsum(
            "rg,dg->rd",
            grad_gate_up,
            full_gate_up.reshape(model_width, 2 * hidden_cols),
            preferred_element_type=floats,
        )
        grad_second = lax.psum(second_part.astype(jnp.bfloat16), "tp").astype(jnp.float32)
        grad_residual = grad_rows.astype(floats) + norm_back(
            grad_second, normed2, inverse2, ln2_gain
        )
        g_ln2_gain = g_ln2_gain + jnp.sum(grad_second * normed2, axis=0)
        g_ln2_bias = g_ln2_bias + jnp.sum(grad_second, axis=0)
        residual_low = grad_residual.astype(halves)
        grad_attended = jnp.dot(residual_low, full_out, preferred_element_type=floats).astype(
            halves
        )
        delta_rows = jnp.sum(
            (grad_attended.astype(floats) * attended.astype(floats)).reshape(
                per_batch, shard_len, heads_local, HD
            ),
            axis=-1,
        )
        grad_heads = grad_attended.reshape(per_batch, shard_len, heads_local, HD)
        all_keys, all_values = (
            lax.all_gather(key_flat, "fsdp", axis=1, tiled=True),
            lax.all_gather(value_flat, "fsdp", axis=1, tiled=True),
        )

        def backward_block(running, block_index):
            offset_at = block_index * key_block
            key_part = lax.dynamic_slice_in_dim(all_keys, offset_at, key_block, 1).reshape(
                per_batch, key_block, heads_local, HD
            )
            value_part = lax.dynamic_slice_in_dim(all_values, offset_at, key_block, 1).reshape(
                per_batch, key_block, heads_local, HD
            )
            key_place = jnp.broadcast_to(
                offset_at + jnp.arange(key_block, dtype=jnp.int32), (per_batch, key_block)
            )
            key_seg = doc_layout(lengths, key_place)[0]
            allowed = pair_mask(query_seg, query_place, key_seg, key_place)
            scores = (
                jnp.einsum("sqhd,skhd->sqhk", query_heads, key_part, preferred_element_type=floats)
                * factor
            )
            softmax_out = jnp.where(allowed, jnp.exp(scores - lse_rows[..., None]), 0.0)
            grad_probs = jnp.einsum(
                "sqhd,skhd->sqhk", grad_heads, value_part, preferred_element_type=floats
            )
            grad_scores = (softmax_out * (grad_probs - delta_rows[..., None]) * factor).astype(
                halves
            )
            running = running + jnp.einsum(
                "sqhk,skhd->sqhd", grad_scores, key_part, preferred_element_type=floats
            )
            key_term = jnp.einsum(
                "sqhk,sqhd->skhd", grad_scores, query_heads, preferred_element_type=floats
            )
            value_term = jnp.einsum(
                "sqhk,sqhd->skhd",
                softmax_out.astype(halves),
                grad_heads,
                preferred_element_type=floats,
            )
            return (running, (key_term, value_term))

        zero_heads = jnp.zeros((per_batch, shard_len, heads_local, HD), floats)
        grad_query, block_terms = lax.scan(
            backward_block, zero_heads, jnp.arange(block_count, dtype=jnp.int32)
        )
        key_terms = jnp.swapaxes(block_terms[0], 0, 1).reshape(per_batch, LEN, head_cols)
        value_terms = jnp.swapaxes(block_terms[1], 0, 1).reshape(per_batch, LEN, head_cols)
        grad_key, grad_value = (
            lax.psum_scatter(
                key_terms.astype(jnp.bfloat16), "fsdp", scatter_dimension=1, tiled=True
            ).astype(jnp.float32),
            lax.psum_scatter(
                value_terms.astype(jnp.bfloat16), "fsdp", scatter_dimension=1, tiled=True
            ).astype(jnp.float32),
        )
        grad_key = grad_key.reshape(per_batch, shard_len, heads_local, HD)
        grad_value = grad_value.reshape(per_batch, shard_len, heads_local, HD)
        grad_query = rotate(grad_query, cosine_table, sine_table, -1.0)
        grad_key = rotate(grad_key, cosine_table, sine_table, -1.0)
        grad_projected = jnp.stack([grad_query, grad_key, grad_value], axis=2).reshape(
            row_count, 3, head_cols
        )
        g_bias = g_bias + jnp.sum(grad_projected, axis=0)
        grad_qkv = grad_projected.astype(halves).reshape(row_count, 3 * head_cols)
        first_part = jnp.einsum(
            "rc,dc->rd",
            grad_qkv,
            full_qkv.reshape(model_width, 3 * head_cols),
            preferred_element_type=floats,
        )
        grad_first = lax.psum(first_part.astype(jnp.bfloat16), "tp").astype(jnp.float32)
        g_ln1_gain = g_ln1_gain + jnp.sum(grad_first * normed1, axis=0)
        g_ln1_bias = g_ln1_bias + jnp.sum(grad_first, axis=0)
        grad_input = (grad_residual + norm_back(grad_first, normed1, inverse1, ln1_gain)).astype(
            halves
        )
        input_grads.append(grad_input.reshape(per_batch, shard_len, model_width))
        kept_rows = (
            first_low,
            grad_qkv,
            residual_low,
            attended,
            second_low,
            grad_gate_up,
            grad_rows,
            hidden,
        )
        stored.append(kept_rows)
    joined = tuple(
        (jnp.concatenate([entry[column] for entry in stored], axis=0) for column in range(8))
    )
    first_low, grad_qkv, residual_low, attended, second_low, grad_gate_up, grad_rows, hidden = (
        joined
    )

    def product(left_rows, right_rows):
        return lax.dot_general(
            left_rows, right_rows, (((0,), (0,)), ((), ())), preferred_element_type=floats
        )

    weight_grads = lax.psum_scatter(
        jnp.concatenate(
            [
                product(first_low, grad_qkv),
                product(residual_low, attended),
                product(second_low, grad_gate_up),
                product(grad_rows, hidden),
            ],
            axis=1,
        ).astype(jnp.bfloat16),
        "fsdp",
        scatter_dimension=0,
        tiled=True,
    ).astype(jnp.float32)
    g_ln1_gain, g_ln1_bias, g_bias, g_ln2_gain, g_ln2_bias = (
        lax.psum(g_ln1_gain.astype(jnp.bfloat16), "fsdp").astype(jnp.float32),
        lax.psum(g_ln1_bias.astype(jnp.bfloat16), "fsdp").astype(jnp.float32),
        lax.psum(g_bias.astype(jnp.bfloat16), "fsdp").astype(jnp.float32),
        lax.psum(g_ln2_gain.astype(jnp.bfloat16), "fsdp").astype(jnp.float32),
        lax.psum(g_ln2_bias.astype(jnp.bfloat16), "fsdp").astype(jnp.float32),
    )
    grad_w_qkv = weight_grads[:, : 3 * head_cols].reshape(rows_owned, 3, head_cols)
    grad_w_out = weight_grads[:, 3 * head_cols : 4 * head_cols]
    grad_w_gate_up = weight_grads[:, 4 * head_cols : 4 * head_cols + 2 * hidden_cols].reshape(
        rows_owned, 2, hidden_cols
    )
    grad_w_down = weight_grads[:, 4 * head_cols + 2 * hidden_cols :]
    block_output = jnp.concatenate(output_parts, axis=0)
    grad_block = jnp.concatenate(input_grads, axis=0)
    return (
        block_output,
        grad_block,
        g_ln1_gain,
        g_ln1_bias,
        grad_w_qkv,
        g_bias,
        grad_w_out,
        g_ln2_gain,
        g_ln2_bias,
        grad_w_gate_up,
        grad_w_down,
    )


FLIP = ((0, 1), (1, 0))
LINE = 4
QUARTER = 128


def flip(block, axis):
    return lax.ppermute(block, axis, FLIP)


def head_rows(lanes_of, head):
    return (lanes_of >= head * HD) & (lanes_of < (head + 1) * HD)


def place_rows(place_ref, own_ref, other_ref, target, column):
    at_z, at_x, at_c = place_ref[0], place_ref[1], place_ref[2]
    for rel_c in range(2):
        for rel_z in range(LINE):
            source = pl.ds((rel_c * LINE + rel_z) * QUARTER, QUARTER)
            base = lax.rem(at_z + rel_z, LINE) * (4 * QUARTER) + jnp.abs(at_c - rel_c) * QUARTER
            mine = pl.multiple_of(base + at_x * (2 * QUARTER), QUARTER)
            theirs = pl.multiple_of(base + (1 - at_x) * (2 * QUARTER), QUARTER)
            target[pl.ds(mine, QUARTER), :] = column(own_ref, source)
            target[pl.ds(theirs, QUARTER), :] = column(other_ref, source)


def fetch_rows(place_ref, own_ref, other_ref, origin, write):
    at_z, at_x, at_c = place_ref[0], place_ref[1], place_ref[2]
    for rel_c in range(2):
        for rel_z in range(LINE):
            goal = pl.ds((rel_c * LINE + rel_z) * QUARTER, QUARTER)
            base = lax.rem(at_z + rel_z, LINE) * (4 * QUARTER) + jnp.abs(at_c - rel_c) * QUARTER
            mine = pl.multiple_of(base + at_x * (2 * QUARTER), QUARTER)
            theirs = pl.multiple_of(base + (1 - at_x) * (2 * QUARTER), QUARTER)
            write(own_ref, goal, origin(pl.ds(mine, QUARTER)))
            write(other_ref, goal, origin(pl.ds(theirs, QUARTER)))


def allowed_block(begin_row, key_at, query_at, key_len, query_len):
    keys = key_at + lax.broadcasted_iota(jnp.int32, (key_len, query_len), 0)
    queries = query_at + lax.broadcasted_iota(jnp.int32, (key_len, query_len), 1)
    return (keys <= queries) & (keys >= begin_row)


def attend_kernel(
    block, place_ref, first_ref, begin_ref, own_ref, other_ref, out_own, out_other, lse_ref, qs, ks, vs, vt, ot
):
    floats, halves = jnp.float32, jnp.bfloat16
    length = qs.shape[0]
    scale = jnp.asarray(1.0 / math.sqrt(HD), halves)
    place_rows(place_ref, own_ref, other_ref, qs, lambda ref, rows: ref[0, rows, :] * scale)
    place_rows(place_ref, own_ref, other_ref, ks, lambda ref, rows: ref[1, rows, :])
    place_rows(place_ref, own_ref, other_ref, vs, lambda ref, rows: ref[2, rows, :])
    vt[...] = vs[...].astype(floats).T.astype(halves)
    lanes_of = lax.broadcasted_iota(jnp.int32, (block, 2 * HD), 1)

    def one_query(index, carry):
        query_at = pl.multiple_of(index * block, block)
        query_both = qs[pl.ds(query_at, block), :]
        begin_row = begin_ref[:, pl.ds(query_at, block)]
        start = first_ref[index]
        for head in range(2):
            query_head = jnp.where(head_rows(lanes_of, head), query_both, jnp.zeros_like(query_both))

            def one_key(step, running):
                highest, total, summed = running
                key_at = pl.multiple_of(step * block, block)
                scores = lax.dot_general(
                    ks[pl.ds(key_at, block), :],
                    query_head,
                    (((1,), (1,)), ((), ())),
                    preferred_element_type=floats,
                )
                allowed = allowed_block(begin_row, key_at, query_at, block, block)
                scores = jnp.where(allowed, scores, negative)
                new_high = jnp.maximum(highest, jnp.max(scores, axis=0, keepdims=True))
                shrink = jnp.exp(highest - new_high)
                weights = jnp.exp(scores - new_high)
                total = total * shrink + jnp.sum(weights, axis=0, keepdims=True)
                summed = summed * shrink + jnp.dot(
                    vt[head * HD : (head + 1) * HD, pl.ds(key_at, block)],
                    weights.astype(halves),
                    preferred_element_type=floats,
                )
                return (new_high, total, summed)

            highest, total, summed = lax.fori_loop(
                start,
                index + 1,
                one_key,
                (
                    jnp.full((1, block), negative, floats),
                    jnp.zeros((1, block), floats),
                    jnp.zeros((HD, block), floats),
                ),
            )
            ot[head * HD : (head + 1) * HD, pl.ds(query_at, block)] = summed / total
            lse_ref[head : head + 1, pl.ds(query_at, block)] = highest + jnp.log(total)
        return carry

    lax.fori_loop(0, length // block, one_query, 0)
    qs[...] = ot[...].T.astype(halves)

    def write(ref, rows, content):
        ref[rows, :] = content

    fetch_rows(place_ref, out_own, out_other, lambda rows: qs[rows, :], write)


def attend_back_kernel(
    block,
    place_ref,
    last_ref,
    begin_ref,
    own_ref,
    other_ref,
    att_own,
    att_other,
    grad_own,
    grad_other,
    lse_ref,
    cos_ref,
    up_ref,
    down_ref,
    out_own,
    out_other,
    bias_ref,
    qs,
    ks,
    kt,
    vs,
    gs,
    at,
    dq,
    dk,
    dv,
    delta,
):
    floats, halves = jnp.float32, jnp.bfloat16
    length = qs.shape[0]
    scale = jnp.asarray(1.0 / math.sqrt(HD), halves)
    place_rows(place_ref, own_ref, other_ref, qs, lambda ref, rows: ref[0, rows, :] * scale)
    place_rows(place_ref, own_ref, other_ref, ks, lambda ref, rows: ref[1, rows, :])
    place_rows(place_ref, own_ref, other_ref, vs, lambda ref, rows: ref[2, rows, :])
    place_rows(place_ref, grad_own, grad_other, gs, lambda ref, rows: ref[rows, :])
    place_rows(place_ref, att_own, att_other, at, lambda ref, rows: ref[rows, :])
    kt[...] = (ks[...] * scale).astype(floats).T.astype(halves)
    pairs = gs[...].astype(floats) * at[...].astype(floats)
    whole_lanes = lax.broadcasted_iota(jnp.int32, (8, 2 * HD), 1)
    for head in range(2):
        chosen = jnp.where(head_rows(whole_lanes, head), 1.0, 0.0)
        delta[8 * head : 8 * head + 8, :] = lax.dot_general(
            chosen,
            pairs,
            (((1,), (1,)), ((), ())),
            precision=lax.Precision.HIGHEST,
            preferred_element_type=floats,
        )
    dq[...] = jnp.zeros_like(dq)
    lanes_of = lax.broadcasted_iota(jnp.int32, (block, 2 * HD), 1)

    def one_key(index, carry):
        key_at = pl.multiple_of(index * block, block)
        key_both = ks[pl.ds(key_at, block), :]
        value_both = vs[pl.ds(key_at, block), :]
        finish = last_ref[index]

        def one_query(step, running):
            grad_key, grad_value = running
            query_at = pl.multiple_of(step * block, block)
            query_both = qs[pl.ds(query_at, block), :]
            grad_both = gs[pl.ds(query_at, block), :]
            begin_row = begin_ref[:, pl.ds(query_at, block)]
            allowed = allowed_block(begin_row, key_at, query_at, block, block)
            for head in range(2):
                chosen = head_rows(lanes_of, head)
                query_head = jnp.where(chosen, query_both, jnp.zeros_like(query_both))
                grad_head = jnp.where(chosen, grad_both, jnp.zeros_like(grad_both))
                scores = lax.dot_general(
                    key_both, query_head, (((1,), (1,)), ((), ())), preferred_element_type=floats
                )
                lse_row = lse_ref[head : head + 1, pl.ds(query_at, block)]
                probs = jnp.where(allowed, jnp.exp(scores - lse_row), 0.0)
                grad_probs = lax.dot_general(
                    value_both, grad_head, (((1,), (1,)), ((), ())), preferred_element_type=floats
                )
                delta_row = delta[8 * head : 8 * head + 1, pl.ds(query_at, block)]
                grad_scores = (probs * (grad_probs - delta_row)).astype(halves)
                grad_value = grad_value + jnp.dot(
                    probs.astype(halves), grad_head, preferred_element_type=floats
                )
                grad_key = grad_key + jnp.dot(
                    grad_scores, query_head, preferred_element_type=floats
                )
                rows = pl.ds(head * HD, HD)
                dq[rows, pl.ds(query_at, block)] += jnp.dot(
                    kt[rows, pl.ds(key_at, block)], grad_scores, preferred_element_type=floats
                )
            return (grad_key, grad_value)

        zero = jnp.zeros((block, 2 * HD), floats)
        grad_key, grad_value = lax.fori_loop(index, finish, one_query, (zero, zero))
        dk[pl.ds(key_at, block), :] = grad_key
        dv[pl.ds(key_at, block), :] = grad_value
        return carry

    lax.fori_loop(0, length // block, one_key, 0)

    def turn_back(rows, content):
        return (
            content * cos_ref[rows, :]
            - pltpu.roll(content, 8, 1) * up_ref[rows, :]
            - pltpu.roll(content, 2 * HD - 8, 1) * down_ref[rows, :]
        )

    sums = [jnp.zeros((1, 2 * HD), floats)] * 3
    for part in range(length // block):
        rows = pl.ds(part * block, block)
        parts = (
            turn_back(rows, dq[:, rows].T),
            turn_back(rows, dk[rows, :]),
            dv[rows, :],
        )
        for kind in range(3):
            sums[kind] = sums[kind] + jnp.sum(parts[kind], axis=0, keepdims=True)
        qs[rows, :] = parts[0].astype(halves)
        ks[rows, :] = parts[1].astype(halves)
        vs[rows, :] = parts[2].astype(halves)
    for kind in range(3):
        bias_ref[kind : kind + 1, :] = sums[kind]

        def write(ref, rows, content, kind=kind):
            ref[kind, rows, :] = content

        held = (qs, ks, vs)[kind]
        fetch_rows(place_ref, out_own, out_other, lambda rows, held=held: held[rows, :], write)


def qkv_kernel(rows_ref, weight_ref, bias_ref, cos_ref, up_ref, down_ref, out_ref):
    floats = jnp.float32
    width = 2 * HD
    for part in range(2):
        product = jnp.dot(
            rows_ref[...],
            weight_ref[:, part * 3 * width : (part + 1) * 3 * width],
            preferred_element_type=floats,
        )
        for kind in range(3):
            content = product[:, kind * width : (kind + 1) * width]
            content = content + bias_ref[part * 3 + kind : part * 3 + kind + 1, :]
            if kind < 2:
                content = (
                    content * cos_ref[...]
                    + pltpu.roll(content, 8, 1) * up_ref[...]
                    + pltpu.roll(content, width - 8, 1) * down_ref[...]
                )
            out_ref[part, kind] = content.astype(out_ref.dtype)


def whole_specs(count):
    return [pl.BlockSpec(memory_space=pltpu.VMEM)] * count


def lane_tables(offset):
    lane = jnp.arange(2 * HD, dtype=jnp.int32) % HD
    halfway = ROT // 2
    exponent = (lane % halfway).astype(jnp.float32) * (2.0 / ROT)
    frequency = jnp.exp(-math.log(10000.0) * exponent)
    angles = offset.astype(jnp.float32)[:, None] * frequency[None, :]
    cosine, sine = (jnp.cos(angles), jnp.sin(angles))
    cosine = jnp.where(lane < ROT, cosine, 1.0)
    upper = jnp.where((lane >= halfway) & (lane < ROT), sine, 0.0)
    lower = jnp.where(lane < halfway, -sine, 0.0)
    return (cosine, upper, lower)


def line_gather(own, at_z):
    down, above = [own], [own]
    for step in range(1, LINE):
        down.append(
            lax.ppermute(down[-1], "z", [(k, k - 1) for k in range(1, LINE - step + 1)])
        )
        above.append(
            lax.ppermute(above[-1], "z", [(k, k + 1) for k in range(step - 1, LINE - 1)])
        )
    blocks = [own]
    for step in range(1, LINE):
        blocks.append(jnp.where(at_z + step < LINE, down[step], above[LINE - step]))
    return jnp.concatenate(blocks + [flip(block, "c") for block in blocks], axis=0)


def line_reduce(keep, send):
    together = keep + flip(send, "c").astype(jnp.float32)
    parts = together.reshape((LINE, QUARTER) + together.shape[1:])
    down = above = None
    for step in range(1, LINE):
        falling, rising = parts[step], parts[LINE - step]
        if down is not None:
            falling, rising = falling + down.astype(jnp.float32), rising + above.astype(jnp.float32)
        down = lax.ppermute(
            falling.astype(jnp.bfloat16), "z", [(k, k - 1) for k in range(LINE - step, LINE)]
        )
        above = lax.ppermute(
            rising.astype(jnp.bfloat16), "z", [(k, k + 1) for k in range(step)]
        )
    return parts[0] + down.astype(jnp.float32) + above.astype(jnp.float32)


def line_trade(parts, at_z):
    held = jnp.zeros_like(parts)
    mine = lax.dynamic_index_in_dim(parts, at_z, 0, keepdims=True)
    held = lax.dynamic_update_slice_in_dim(held, mine, at_z, 0)
    for step in range(1, LINE):
        going = lax.dynamic_index_in_dim(parts, lax.rem(at_z + step, LINE), 0, keepdims=True)
        came = lax.ppermute(going, "z", [(k, (k + step) % LINE) for k in range(LINE)])
        held = lax.dynamic_update_slice_in_dim(held, came, lax.rem(at_z + LINE - step, LINE), 0)
    return held


def widen(parts, at_z, first):
    held = line_trade(parts, at_z)
    held = held.reshape(held.shape[0] * held.shape[1], held.shape[2])
    if first == "y":
        held = jnp.concatenate([held, flip(held, "y")], axis=1)
        return jnp.concatenate([held, flip(held, "x")], axis=0)
    held = jnp.concatenate([held, flip(held, "x")], axis=0)
    return jnp.concatenate([held, flip(held, "y")], axis=1)


def narrow(total, at_z, first):
    floats, halves = jnp.float32, jnp.bfloat16
    half_rows, half_cols = total.shape[0] // 2, total.shape[1] // 2
    if first == "x":
        came = flip(total[half_rows:].astype(halves), "x").astype(floats)
        total = total[:half_rows] + came
        came = flip(total[:, half_cols:].astype(halves), "y").astype(floats)
        total = total[:, :half_cols] + came
    else:
        came = flip(total[:, half_cols:].astype(halves), "y").astype(floats)
        total = total[:, :half_cols] + came
        came = flip(total[half_rows:].astype(halves), "x").astype(floats)
        total = total[:half_rows] + came
    parts = total.astype(halves).reshape(LINE, half_rows // LINE, half_cols)
    return line_trade(parts, at_z)


def block_device(
    block_input,
    doc_lengths,
    ln1_gain,
    ln1_bias,
    w_qkv,
    qkv_bias,
    w_out,
    ln2_gain,
    ln2_bias,
    w_gate_up,
    w_down,
    grad_y,
):
    floats, halves = jnp.float32, jnp.bfloat16
    at_z, at_x, at_y, at_c = (lax.axis_index(name) for name in ("z", "x", "y", "c"))
    model_width = block_input.shape[2]
    shard_len = block_input.shape[1]
    head_cols = w_out.shape[1]
    hidden_cols = w_down.shape[1]
    rows_owned = w_out.shape[0]
    wide = -(-hidden_cols // (LINE * QUARTER)) * QUARTER
    cut = head_cols // LINE
    tokens = 2 * LINE * QUARTER

    def features(content):
        lead = content.shape[:-1]
        split = content.reshape(lead + (LINE, 2, rows_owned))
        near = lax.dynamic_index_in_dim(split, at_x, split.ndim - 2, keepdims=False)
        far = lax.dynamic_index_in_dim(split, 1 - at_x, split.ndim - 2, keepdims=False)
        flat = lead + (LINE * rows_owned,)
        return jnp.concatenate([near.reshape(flat), far.reshape(flat)], axis=-1)

    def plain_features(content):
        lead = content.shape[:-1]
        split = content.reshape(lead + (2, LINE, rows_owned))
        even = jnp.where(at_x == 0, split[..., 0, :, :], split[..., 1, :, :])
        odd = jnp.where(at_x == 0, split[..., 1, :, :], split[..., 0, :, :])
        return jnp.stack([even, odd], axis=-2).reshape(lead + (model_width,))

    def own_rows(content):
        seq_rows = lax.dynamic_index_in_dim(content, at_y, 0, keepdims=False)
        return features(lax.dynamic_slice_in_dim(seq_rows, at_c * QUARTER, QUARTER, 0))

    def spread_output(content):
        content = plain_features(content).astype(halves)
        beside = flip(content, "c")
        pair = jnp.concatenate(
            [
                jnp.where(at_c == 0, content, beside),
                jnp.where(at_c == 0, beside, content),
            ],
            axis=0,
        )
        across = flip(pair, "y")
        return jnp.stack(
            [jnp.where(at_y == 0, pair, across), jnp.where(at_y == 0, across, pair)], axis=0
        )

    def quarters(matrix, size):
        grown = jnp.pad(matrix, ((0, 0), (0, LINE * size - matrix.shape[1])))
        return jnp.swapaxes(grown.reshape(matrix.shape[0], LINE, size), 0, 1)

    part_qkv = jnp.concatenate([quarters(w_qkv[:, kind], cut) for kind in range(3)], axis=2)
    part_out = quarters(w_out, cut)
    part_gate_up = jnp.concatenate([quarters(w_gate_up[:, kind], wide) for kind in range(2)], axis=2)
    part_down = quarters(w_down, wide)

    lengths = lax.dynamic_index_in_dim(doc_lengths, at_y, 0, keepdims=False)
    doc_ends = jnp.cumsum(lengths)

    def begin_of(places):
        passed = (places[:, None] >= doc_ends[None, :]).astype(jnp.int32)
        return jnp.sum(passed * lengths[None, :], axis=-1)

    length = 2 * tokens
    block = 256
    all_places = jnp.arange(length, dtype=jnp.int32)
    begin_all = begin_of(all_places)
    block_begin = begin_all.reshape(length // block, block)[:, 0]
    first_block = block_begin // block
    block_ends = (jnp.arange(length // block, dtype=jnp.int32) + 1) * block
    last_block = jnp.sum((block_begin[None, :] < block_ends[:, None]).astype(jnp.int32), axis=1)
    rel = jnp.arange(tokens, dtype=jnp.int32)
    rel_c, rel_z, rel_r = rel // (LINE * QUARTER), (rel // QUARTER) % LINE, rel % QUARTER
    places = (
        ((at_z + rel_z) % LINE) * (2 * shard_len)
        + at_x * shard_len
        + jnp.abs(at_c - rel_c) * QUARTER
        + rel_r
    )
    row_tables = lane_tables(places - begin_of(places))
    all_tables = lane_tables(all_places - begin_all)
    place = jnp.stack([at_z, at_x, at_c]).astype(jnp.int32)

    input_wide = own_rows(block_input).astype(floats)
    gain1, shift1, gain2, shift2 = (features(v) for v in (ln1_gain, ln1_bias, ln2_gain, ln2_bias))
    first_norm, normed1, inverse1 = layer_norm(input_wide, gain1, shift1)
    first_low = line_gather(first_norm.astype(halves), at_z)
    full_qkv = widen(part_qkv, at_z, "y")
    full_out = widen(part_out, at_z, "y")
    full_gate_up = widen(part_gate_up, at_z, "x")
    full_down = widen(part_down, at_z, "y")
    grad_rows = line_gather(own_rows(grad_y), at_z)

    own_bias = lax.dynamic_slice_in_dim(qkv_bias, at_z * cut, cut, 1)
    bias_parts = jnp.concatenate([own_bias, flip(own_bias, "y")], axis=0)
    projected = pl.pallas_call(
        qkv_kernel,
        out_shape=jax.ShapeDtypeStruct((2, 3, tokens, cut), halves),
        in_specs=whole_specs(6),
        out_specs=pl.BlockSpec(memory_space=pltpu.VMEM),
        name="project",
    )(first_low, full_qkv, bias_parts, *row_tables)
    crossed = at_x ^ at_y
    qkv_own = lax.dynamic_index_in_dim(projected, crossed, 0, keepdims=False)
    qkv_other = flip(lax.dynamic_index_in_dim(projected, 1 - crossed, 0, keepdims=False), "x")

    smem = pl.BlockSpec(memory_space=pltpu.SMEM)
    half_shape = jax.ShapeDtypeStruct((tokens, cut), halves)
    out_own, out_other, lse = pl.pallas_call(
        functools.partial(attend_kernel, block),
        out_shape=(half_shape, half_shape, jax.ShapeDtypeStruct((2, length), floats)),
        in_specs=[smem, smem] + whole_specs(3),
        out_specs=tuple(whole_specs(3)),
        scratch_shapes=[pltpu.VMEM((length, cut), halves)] * 3
        + [pltpu.VMEM((cut, length), halves), pltpu.VMEM((cut, length), floats)],
        name="attend",
    )(place, first_block, begin_all[None, :], qkv_own, qkv_other)

    def join_heads(own, other):
        near = jnp.where(crossed == 0, own, other)
        far = jnp.where(crossed == 0, other, own)
        return jnp.concatenate([near, far], axis=-1)

    attended = join_heads(out_own, flip(out_other, "x"))
    half = tokens // 2

    def spread(left, right):
        send = lax.dot_general(
            left[half:], right, (((1,), (1,)), ((), ())), preferred_element_type=floats
        ).astype(halves)
        keep = lax.dot_general(
            left[:half], right, (((1,), (1,)), ((), ())), preferred_element_type=floats
        )
        return line_reduce(keep, send)

    residual = input_wide + spread(attended, full_out)
    second_norm, normed2, inverse2 = layer_norm(residual, gain2, shift2)
    second_low = line_gather(second_norm.astype(halves), at_z)
    gate_up = jnp.dot(second_low, full_gate_up, preferred_element_type=floats)
    gate_up = gate_up.reshape(tokens, 2, 2, wide)
    gate, up_part = gate_up[:, :, 0], gate_up[:, :, 1]
    sigmoid_gate = jax.nn.sigmoid(gate)
    hidden = (gate * sigmoid_gate * up_part).astype(halves).reshape(tokens, 2 * wide)
    grad_hidden = jnp.dot(grad_rows, full_down, preferred_element_type=floats)
    grad_hidden = grad_hidden.reshape(tokens, 2, wide)
    grad_gate = grad_hidden * up_part * sigmoid_gate * (1.0 + gate * (1.0 - sigmoid_gate))
    grad_upper = grad_hidden * gate * sigmoid_gate
    grad_gate_up = jnp.stack([grad_gate, grad_upper], axis=2).astype(halves)
    grad_gate_up = grad_gate_up.reshape(tokens, 4 * wide)

    grad_second = spread(grad_gate_up, full_gate_up)
    block_output = spread_output(residual + spread(hidden, full_down))

    def product(left_rows, right_rows):
        return lax.dot_general(
            left_rows, right_rows, (((0,), (0,)), ((), ())), preferred_element_type=floats
        )

    grad_own = own_rows(grad_y).astype(floats)
    g_gate_up = narrow(product(second_low, grad_gate_up), at_z, "x")
    g_down = narrow(product(grad_rows, hidden), at_z, "y")
    grad_residual = grad_own + norm_back(grad_second, normed2, inverse2, gain2)
    low_own = grad_residual.astype(halves)
    residual_low = line_gather(low_own, at_z)
    grad_attended = jnp.dot(residual_low, full_out, preferred_element_type=floats).astype(halves)
    grad_near, grad_far = grad_attended[:, :cut], grad_attended[:, cut:]
    grad_mine = jnp.where(crossed == 0, grad_near, grad_far)
    grad_their = flip(jnp.where(crossed == 0, grad_far, grad_near), "x")

    qkv_shape = jax.ShapeDtypeStruct((3, tokens, cut), halves)
    back_own, back_other, bias_sums = pl.pallas_call(
        functools.partial(attend_back_kernel, block),
        out_shape=(qkv_shape, qkv_shape, jax.ShapeDtypeStruct((3, cut), floats)),
        in_specs=[smem, smem] + whole_specs(11),
        out_specs=tuple(whole_specs(3)),
        scratch_shapes=[
            pltpu.VMEM((length, cut), halves),
            pltpu.VMEM((length, cut), halves),
            pltpu.VMEM((cut, length), halves),
            pltpu.VMEM((length, cut), halves),
            pltpu.VMEM((length, cut), halves),
            pltpu.VMEM((length, cut), halves),
            pltpu.VMEM((cut, length), floats),
            pltpu.VMEM((length, cut), floats),
            pltpu.VMEM((length, cut), floats),
            pltpu.VMEM((16, length), floats),
        ],
        name="attend_back",
    )(
        place,
        last_block,
        begin_all[None, :],
        qkv_own,
        qkv_other,
        out_own,
        out_other,
        grad_mine,
        grad_their,
        lse,
        *all_tables,
    )
    came_back = flip(back_other, "x")
    near = jnp.where(crossed == 0, back_own, came_back)
    far = jnp.where(crossed == 0, came_back, back_own)
    grad_qkv = jnp.concatenate([near[0], near[1], near[2], far[0], far[1], far[2]], axis=1)
    grad_first = spread(grad_qkv, full_qkv)
    g_qkv = narrow(product(first_low, grad_qkv), at_z, "y")
    g_out = narrow(product(residual_low, attended), at_z, "y")
    grad_input = spread_output(grad_residual + norm_back(grad_first, normed1, inverse1, gain1))

    sums = jnp.stack(
        [
            jnp.sum(grad_first * normed1, axis=0),
            jnp.sum(grad_first, axis=0),
            jnp.sum(grad_second * normed2, axis=0),
            jnp.sum(grad_second, axis=0),
        ]
    )
    sums = lax.psum(plain_features(sums), ("z", "x", "y", "c"))
    bias_all = lax.all_gather(bias_sums, ("z", "x", "y"), axis=0)
    bias_all = jnp.sum(bias_all.reshape(LINE, 2, 2, 3, cut), axis=2)
    bias_all = lax.dynamic_index_in_dim(bias_all, at_y, 1, keepdims=False)
    g_bias = jnp.swapaxes(bias_all, 0, 1).reshape(3, head_cols)

    def columns(parts, offset, size, count):
        matrix = jnp.swapaxes(parts[:, :, offset : offset + size], 0, 1)
        return matrix.reshape(rows_owned, LINE * size)[:, :count].astype(floats)

    grad_w_qkv = jnp.stack([columns(g_qkv, kind * cut, cut, head_cols) for kind in range(3)], axis=1)
    grad_w_gate_up = jnp.stack(
        [columns(g_gate_up, kind * wide, wide, hidden_cols) for kind in range(2)], axis=1
    )
    return (
        block_output,
        grad_input,
        sums[0],
        sums[1],
        grad_w_qkv,
        g_bias,
        columns(g_out, 0, cut, head_cols),
        sums[2],
        sums[3],
        grad_w_gate_up,
        columns(g_down, 0, wide, hidden_cols),
    )


def solution(mesh):
    sizes = (mesh.shape["fsdp"], mesh.shape["tp"])
    if sizes == (2 * LINE, 4):
        names = ("z", "x", "y", "c")
        rows, cols = ("z", "x"), ("y", "c")
        mesh = Mesh(mesh.devices.reshape(LINE, 2, 2, 2), names)
        device_step = block_device
    else:
        rows, cols = "fsdp", "tp"
        device_step = on_device
    placed = (
        P(None, rows, None),
        P(),
        P(),
        P(),
        P(rows, None, cols),
        P(None, cols),
        P(rows, cols),
        P(),
        P(),
        P(rows, None, cols),
        P(rows, cols),
        P(None, rows, None),
    )
    return jax.shard_map(
        device_step,
        mesh=mesh,
        in_specs=placed,
        out_specs=(
            P(None, rows, None),
            P(None, rows, None),
            P(),
            P(),
            P(rows, None, cols),
            P(None, cols),
            P(rows, cols),
            P(),
            P(),
            P(rows, None, cols),
            P(rows, cols),
        ),
        check_vma=False,
    )
```

```python
import functools
import math

import jax
import jax.numpy as jnp
from jax import lax
from jax.experimental import pallas as pl
from jax.experimental.pallas import tpu as pltpu
from jax.sharding import Mesh
from jax.sharding import PartitionSpec as P

HD = 64
ROT = 16
LEN = 2048
SEQ_MB = 1
MICRO = 2


epsilon = 1e-05
negative = -1e30


def layer_norm(matrix_in, norm_gain, norm_shift):
    center = jnp.mean(matrix_in, axis=-1, keepdims=True)
    centered = matrix_in - center
    spread = jnp.mean(centered * centered, axis=-1, keepdims=True)
    inverse = lax.rsqrt(spread + epsilon)
    normed = centered * inverse
    return (normed * norm_gain + norm_shift, normed, inverse)


def norm_back(incoming, normed, inverse, norm_gain):
    scaled = incoming * norm_gain
    first_mean = jnp.mean(scaled, axis=-1, keepdims=True)
    cross_mean = jnp.mean(scaled * normed, axis=-1, keepdims=True)
    return inverse * (scaled - first_mean - normed * cross_mean)


def doc_layout(lengths, places):
    doc_ends = jnp.cumsum(lengths, axis=-1)
    passed = (places[:, :, None] >= doc_ends[:, None, :]).astype(jnp.int32)
    segment = jnp.sum(passed, axis=-1)
    begins = jnp.sum(passed * lengths[:, None, :], axis=-1)
    return (segment, places - begins)


def rotary_tables(offset):
    halfway = ROT // 2
    exponent = jnp.arange(halfway, dtype=jnp.float32) * (2.0 / ROT)
    frequency = jnp.exp(-math.log(10000.0) * exponent)
    angles = offset.astype(jnp.float32)[..., None] * frequency
    return (jnp.cos(angles), jnp.sin(angles))


def rotate(head_rows, cosine_table, sine_table, direction):
    halfway = ROT // 2
    leading = head_rows[..., :halfway]
    behind = head_rows[..., halfway:ROT]
    cosine_part = cosine_table[..., None, :]
    sine_part = sine_table[..., None, :] * direction
    return jnp.concatenate(
        [
            leading * cosine_part - behind * sine_part,
            behind * cosine_part + leading * sine_part,
            head_rows[..., ROT:],
        ],
        axis=-1,
    )


def pair_mask(query_seg, query_place, key_seg, key_place):
    same_doc = query_seg[:, :, None] == key_seg[:, None, :]
    causal = key_place[:, None, :] <= query_place[:, :, None]
    return (same_doc & causal)[:, :, None, :]


def fold_blocks(update, folded, part_arrays, block_len):
    extent = part_arrays[0].shape[1]
    number = extent // block_len
    blocks = tuple(
        (
            jnp.swapaxes(
                part_array.reshape((part_array.shape[0], number, block_len) + part_array.shape[2:]),
                0,
                1,
            )
            for part_array in part_arrays
        )
    )

    def advance(running, element):
        block_index, block_parts = element
        return (update(running, block_parts, block_index * block_len), None)

    folded, unused = lax.scan(advance, folded, (jnp.arange(number, dtype=jnp.int32), blocks))
    return folded


def fetch_weights(w_qkv, w_out, w_gate_up, w_down):
    return (
        lax.all_gather(w_qkv, "fsdp", axis=0, tiled=True),
        lax.all_gather(w_out, "fsdp", axis=0, tiled=True),
        lax.all_gather(w_gate_up, "fsdp", axis=0, tiled=True),
        lax.all_gather(w_down, "fsdp", axis=0, tiled=True),
    )


def on_device(
    block_input,
    doc_lengths,
    ln1_gain,
    ln1_bias,
    w_qkv,
    qkv_bias,
    w_out,
    ln2_gain,
    ln2_bias,
    w_gate_up,
    w_down,
    grad_y,
):
    floats = jnp.float32
    halves = jnp.bfloat16
    factor = 1.0 / math.sqrt(HD)
    per_batch = SEQ_MB
    shard_len = block_input.shape[1]
    model_width = block_input.shape[2]
    head_cols = qkv_bias.shape[1]
    heads_local = head_cols // HD
    hidden_cols = w_down.shape[1]
    row_count = per_batch * shard_len
    rows_owned = model_width // lax.axis_size("fsdp")
    first_row = lax.axis_index("fsdp") * shard_len
    query_place = jnp.broadcast_to(
        first_row + jnp.arange(shard_len, dtype=jnp.int32), (per_batch, shard_len)
    )
    key_block = min(LEN, 512)
    block_count = LEN // key_block
    g_ln1_gain = jnp.zeros((model_width,), floats)
    g_ln1_bias = jnp.zeros((model_width,), floats)
    g_ln2_gain = jnp.zeros((model_width,), floats)
    g_ln2_bias = jnp.zeros((model_width,), floats)
    g_bias = jnp.zeros((3, head_cols), floats)
    stored = []
    output_parts = []
    input_grads = []
    for batch in range(MICRO):
        lower = batch * per_batch
        seq_rows = block_input[lower : lower + per_batch]
        lengths = doc_lengths[lower : lower + per_batch]
        seq_grad = grad_y[lower : lower + per_batch]
        query_seg, offset = doc_layout(lengths, query_place)
        cosine_table, sine_table = rotary_tables(offset)
        gathered = fetch_weights(w_qkv, w_out, w_gate_up, w_down)
        full_qkv, full_out, full_gate_up, full_down = gathered
        input_wide = seq_rows.reshape(row_count, model_width).astype(floats)
        first_norm, normed1, inverse1 = layer_norm(input_wide, ln1_gain, ln1_bias)
        first_low = first_norm.astype(halves)
        projected = (
            jnp.dot(
                first_low,
                full_qkv.reshape(model_width, 3 * head_cols),
                preferred_element_type=floats,
            ).reshape(row_count, 3, head_cols)
            + qkv_bias
        )
        projected = projected.reshape(per_batch, shard_len, 3, heads_local, HD)
        query_heads = rotate(projected[:, :, 0], cosine_table, sine_table, 1.0).astype(halves)
        key_heads = rotate(projected[:, :, 1], cosine_table, sine_table, 1.0).astype(halves)
        value_heads = projected[:, :, 2].astype(halves)
        key_flat = key_heads.reshape(per_batch, shard_len, head_cols)
        value_flat = value_heads.reshape(per_batch, shard_len, head_cols)

        def attend(running, block_parts, offset_at):
            key_part, value_part = block_parts
            extent = key_part.shape[1]
            key_place = jnp.broadcast_to(
                offset_at + jnp.arange(extent, dtype=jnp.int32), (per_batch, extent)
            )
            key_seg = doc_layout(lengths, key_place)[0]
            allowed = pair_mask(query_seg, query_place, key_seg, key_place)
            scores = (
                jnp.einsum(
                    "sqhd,skhd->sqhk",
                    query_heads,
                    key_part.reshape(per_batch, extent, heads_local, HD),
                    preferred_element_type=floats,
                )
                * factor
            )
            scores = jnp.where(allowed, scores, negative)
            highest, denominator, summed = running
            new_high = jnp.maximum(highest, jnp.max(scores, axis=-1))
            shrink = jnp.exp(highest - new_high)
            weights = jnp.where(allowed, jnp.exp(scores - new_high[..., None]), 0.0)
            denominator = denominator * shrink + jnp.sum(weights, axis=-1)
            summed = summed * shrink[..., None] + jnp.einsum(
                "sqhk,skhd->sqhd",
                weights.astype(halves),
                value_part.reshape(per_batch, extent, heads_local, HD),
                preferred_element_type=floats,
            )
            return (new_high, denominator, summed)

        start_state = (
            jnp.full((per_batch, shard_len, heads_local), negative, floats),
            jnp.zeros((per_batch, shard_len, heads_local), floats),
            jnp.zeros((per_batch, shard_len, heads_local, HD), floats),
        )
        highest, denominator, summed = fold_blocks(
            attend,
            start_state,
            (
                lax.all_gather(key_flat, "fsdp", axis=1, tiled=True),
                lax.all_gather(value_flat, "fsdp", axis=1, tiled=True),
            ),
            key_block,
        )
        lse_rows = highest + jnp.log(denominator)
        attended = (summed / denominator[..., None]).astype(halves).reshape(row_count, head_cols)
        attn_part = jnp.einsum("rc,oc->ro", attended, full_out, preferred_element_type=floats)
        residual = input_wide + lax.psum(attn_part.astype(jnp.bfloat16), "tp").astype(jnp.float32)
        second_norm, normed2, inverse2 = layer_norm(residual, ln2_gain, ln2_bias)
        second_low = second_norm.astype(halves)
        gate_up = jnp.dot(
            second_low,
            full_gate_up.reshape(model_width, 2 * hidden_cols),
            preferred_element_type=floats,
        ).reshape(row_count, 2, hidden_cols)
        gate = gate_up[:, 0]
        up_part = gate_up[:, 1]
        sigmoid_gate = jax.nn.sigmoid(gate)
        hidden = (gate * sigmoid_gate * up_part).astype(halves)
        ffn_part = jnp.einsum("rf,of->ro", hidden, full_down, preferred_element_type=floats)
        residual_out = residual + lax.psum(ffn_part.astype(jnp.bfloat16), "tp").astype(jnp.float32)
        output_parts.append(residual_out.astype(halves).reshape(per_batch, shard_len, model_width))
        full_qkv, full_out, full_gate_up, full_down = (
            lax.all_gather(w_qkv, "fsdp", axis=0, tiled=True),
            lax.all_gather(w_out, "fsdp", axis=0, tiled=True),
            lax.all_gather(w_gate_up, "fsdp", axis=0, tiled=True),
            lax.all_gather(w_down, "fsdp", axis=0, tiled=True),
        )
        grad_rows = seq_grad.reshape(row_count, model_width)
        grad_hidden = jnp.dot(grad_rows, full_down, preferred_element_type=floats)
        grad_gate = grad_hidden * up_part * sigmoid_gate * (1.0 + gate * (1.0 - sigmoid_gate))
        grad_upper = grad_hidden * gate * sigmoid_gate
        grad_gate_up = (
            jnp.stack([grad_gate, grad_upper], axis=1)
            .astype(halves)
            .reshape(row_count, 2 * hidden_cols)
        )
        second_part = jnp.einsum(
            "rg,dg->rd",
            grad_gate_up,
            full_gate_up.reshape(model_width, 2 * hidden_cols),
            preferred_element_type=floats,
        )
        grad_second = lax.psum(second_part.astype(jnp.bfloat16), "tp").astype(jnp.float32)
        grad_residual = grad_rows.astype(floats) + norm_back(
            grad_second, normed2, inverse2, ln2_gain
        )
        g_ln2_gain = g_ln2_gain + jnp.sum(grad_second * normed2, axis=0)
        g_ln2_bias = g_ln2_bias + jnp.sum(grad_second, axis=0)
        residual_low = grad_residual.astype(halves)
        grad_attended = jnp.dot(residual_low, full_out, preferred_element_type=floats).astype(
            halves
        )
        delta_rows = jnp.sum(
            (grad_attended.astype(floats) * attended.astype(floats)).reshape(
                per_batch, shard_len, heads_local, HD
            ),
            axis=-1,
        )
        grad_heads = grad_attended.reshape(per_batch, shard_len, heads_local, HD)
        all_keys, all_values = (
            lax.all_gather(key_flat, "fsdp", axis=1, tiled=True),
            lax.all_gather(value_flat, "fsdp", axis=1, tiled=True),
        )

        def backward_block(running, block_index):
            offset_at = block_index * key_block
            key_part = lax.dynamic_slice_in_dim(all_keys, offset_at, key_block, 1).reshape(
                per_batch, key_block, heads_local, HD
            )
            value_part = lax.dynamic_slice_in_dim(all_values, offset_at, key_block, 1).reshape(
                per_batch, key_block, heads_local, HD
            )
            key_place = jnp.broadcast_to(
                offset_at + jnp.arange(key_block, dtype=jnp.int32), (per_batch, key_block)
            )
            key_seg = doc_layout(lengths, key_place)[0]
            allowed = pair_mask(query_seg, query_place, key_seg, key_place)
            scores = (
                jnp.einsum("sqhd,skhd->sqhk", query_heads, key_part, preferred_element_type=floats)
                * factor
            )
            softmax_out = jnp.where(allowed, jnp.exp(scores - lse_rows[..., None]), 0.0)
            grad_probs = jnp.einsum(
                "sqhd,skhd->sqhk", grad_heads, value_part, preferred_element_type=floats
            )
            grad_scores = (softmax_out * (grad_probs - delta_rows[..., None]) * factor).astype(
                halves
            )
            running = running + jnp.einsum(
                "sqhk,skhd->sqhd", grad_scores, key_part, preferred_element_type=floats
            )
            key_term = jnp.einsum(
                "sqhk,sqhd->skhd", grad_scores, query_heads, preferred_element_type=floats
            )
            value_term = jnp.einsum(
                "sqhk,sqhd->skhd",
                softmax_out.astype(halves),
                grad_heads,
                preferred_element_type=floats,
            )
            return (running, (key_term, value_term))

        zero_heads = jnp.zeros((per_batch, shard_len, heads_local, HD), floats)
        grad_query, block_terms = lax.scan(
            backward_block, zero_heads, jnp.arange(block_count, dtype=jnp.int32)
        )
        key_terms = jnp.swapaxes(block_terms[0], 0, 1).reshape(per_batch, LEN, head_cols)
        value_terms = jnp.swapaxes(block_terms[1], 0, 1).reshape(per_batch, LEN, head_cols)
        grad_key, grad_value = (
            lax.psum_scatter(
                key_terms.astype(jnp.bfloat16), "fsdp", scatter_dimension=1, tiled=True
            ).astype(jnp.float32),
            lax.psum_scatter(
                value_terms.astype(jnp.bfloat16), "fsdp", scatter_dimension=1, tiled=True
            ).astype(jnp.float32),
        )
        grad_key = grad_key.reshape(per_batch, shard_len, heads_local, HD)
        grad_value = grad_value.reshape(per_batch, shard_len, heads_local, HD)
        grad_query = rotate(grad_query, cosine_table, sine_table, -1.0)
        grad_key = rotate(grad_key, cosine_table, sine_table, -1.0)
        grad_projected = jnp.stack([grad_query, grad_key, grad_value], axis=2).reshape(
            row_count, 3, head_cols
        )
        g_bias = g_bias + jnp.sum(grad_projected, axis=0)
        grad_qkv = grad_projected.astype(halves).reshape(row_count, 3 * head_cols)
        first_part = jnp.einsum(
            "rc,dc->rd",
            grad_qkv,
            full_qkv.reshape(model_width, 3 * head_cols),
            preferred_element_type=floats,
        )
        grad_first = lax.psum(first_part.astype(jnp.bfloat16), "tp").astype(jnp.float32)
        g_ln1_gain = g_ln1_gain + jnp.sum(grad_first * normed1, axis=0)
        g_ln1_bias = g_ln1_bias + jnp.sum(grad_first, axis=0)
        grad_input = (grad_residual + norm_back(grad_first, normed1, inverse1, ln1_gain)).astype(
            halves
        )
        input_grads.append(grad_input.reshape(per_batch, shard_len, model_width))
        kept_rows = (
            first_low,
            grad_qkv,
            residual_low,
            attended,
            second_low,
            grad_gate_up,
            grad_rows,
            hidden,
        )
        stored.append(kept_rows)
    joined = tuple(
        (jnp.concatenate([entry[column] for entry in stored], axis=0) for column in range(8))
    )
    first_low, grad_qkv, residual_low, attended, second_low, grad_gate_up, grad_rows, hidden = (
        joined
    )

    def product(left_rows, right_rows):
        return lax.dot_general(
            left_rows, right_rows, (((0,), (0,)), ((), ())), preferred_element_type=floats
        )

    weight_grads = lax.psum_scatter(
        jnp.concatenate(
            [
                product(first_low, grad_qkv),
                product(residual_low, attended),
                product(second_low, grad_gate_up),
                product(grad_rows, hidden),
            ],
            axis=1,
        ).astype(jnp.bfloat16),
        "fsdp",
        scatter_dimension=0,
        tiled=True,
    ).astype(jnp.float32)
    g_ln1_gain, g_ln1_bias, g_bias, g_ln2_gain, g_ln2_bias = (
        lax.psum(g_ln1_gain.astype(jnp.bfloat16), "fsdp").astype(jnp.float32),
        lax.psum(g_ln1_bias.astype(jnp.bfloat16), "fsdp").astype(jnp.float32),
        lax.psum(g_bias.astype(jnp.bfloat16), "fsdp").astype(jnp.float32),
        lax.psum(g_ln2_gain.astype(jnp.bfloat16), "fsdp").astype(jnp.float32),
        lax.psum(g_ln2_bias.astype(jnp.bfloat16), "fsdp").astype(jnp.float32),
    )
    grad_w_qkv = weight_grads[:, : 3 * head_cols].reshape(rows_owned, 3, head_cols)
    grad_w_out = weight_grads[:, 3 * head_cols : 4 * head_cols]
    grad_w_gate_up = weight_grads[:, 4 * head_cols : 4 * head_cols + 2 * hidden_cols].reshape(
        rows_owned, 2, hidden_cols
    )
    grad_w_down = weight_grads[:, 4 * head_cols + 2 * hidden_cols :]
    block_output = jnp.concatenate(output_parts, axis=0)
    grad_block = jnp.concatenate(input_grads, axis=0)
    return (
        block_output,
        grad_block,
        g_ln1_gain,
        g_ln1_bias,
        grad_w_qkv,
        g_bias,
        grad_w_out,
        g_ln2_gain,
        g_ln2_bias,
        grad_w_gate_up,
        grad_w_down,
    )


FLIP = ((0, 1), (1, 0))
LINE = 4
QUARTER = 128


def flip(block, axis):
    return lax.ppermute(block, axis, FLIP)


def head_rows(lanes_of, head):
    return (lanes_of >= head * HD) & (lanes_of < (head + 1) * HD)


def place_rows(place_ref, own_ref, other_ref, target, column):
    at_z, at_x, at_c = place_ref[0], place_ref[1], place_ref[2]
    for rel_c in range(2):
        for rel_z in range(LINE):
            source = pl.ds((rel_c * LINE + rel_z) * QUARTER, QUARTER)
            base = lax.rem(at_z + rel_z, LINE) * (4 * QUARTER) + jnp.abs(at_c - rel_c) * QUARTER
            mine = pl.multiple_of(base + at_x * (2 * QUARTER), QUARTER)
            theirs = pl.multiple_of(base + (1 - at_x) * (2 * QUARTER), QUARTER)
            target[pl.ds(mine, QUARTER), :] = column(own_ref, source)
            target[pl.ds(theirs, QUARTER), :] = column(other_ref, source)


def fetch_rows(place_ref, own_ref, other_ref, origin, write):
    at_z, at_x, at_c = place_ref[0], place_ref[1], place_ref[2]
    for rel_c in range(2):
        for rel_z in range(LINE):
            goal = pl.ds((rel_c * LINE + rel_z) * QUARTER, QUARTER)
            base = lax.rem(at_z + rel_z, LINE) * (4 * QUARTER) + jnp.abs(at_c - rel_c) * QUARTER
            mine = pl.multiple_of(base + at_x * (2 * QUARTER), QUARTER)
            theirs = pl.multiple_of(base + (1 - at_x) * (2 * QUARTER), QUARTER)
            write(own_ref, goal, origin(pl.ds(mine, QUARTER)))
            write(other_ref, goal, origin(pl.ds(theirs, QUARTER)))


def allowed_block(begin_row, key_at, query_at, key_len, query_len):
    keys = key_at + lax.broadcasted_iota(jnp.int32, (key_len, query_len), 0)
    queries = query_at + lax.broadcasted_iota(jnp.int32, (key_len, query_len), 1)
    return (keys <= queries) & (keys >= begin_row)


def attend_kernel(
    block, place_ref, first_ref, begin_ref, own_ref, other_ref, out_own, out_other, lse_ref, qs, ks, vs, vt, ot
):
    floats, halves = jnp.float32, jnp.bfloat16
    length = qs.shape[0]
    scale = jnp.asarray(1.0 / math.sqrt(HD), halves)
    place_rows(place_ref, own_ref, other_ref, qs, lambda ref, rows: ref[0, rows, :] * scale)
    place_rows(place_ref, own_ref, other_ref, ks, lambda ref, rows: ref[1, rows, :])
    place_rows(place_ref, own_ref, other_ref, vs, lambda ref, rows: ref[2, rows, :])
    vt[...] = vs[...].astype(floats).T.astype(halves)
    lanes_of = lax.broadcasted_iota(jnp.int32, (block, 2 * HD), 1)

    def one_query(index, carry):
        query_at = pl.multiple_of(index * block, block)
        query_both = qs[pl.ds(query_at, block), :]
        begin_row = begin_ref[:, pl.ds(query_at, block)]
        start = first_ref[index]
        for head in range(2):
            query_head = jnp.where(head_rows(lanes_of, head), query_both, jnp.zeros_like(query_both))

            def one_key(step, running):
                highest, total, summed = running
                key_at = pl.multiple_of(step * block, block)
                scores = lax.dot_general(
                    ks[pl.ds(key_at, block), :],
                    query_head,
                    (((1,), (1,)), ((), ())),
                    preferred_element_type=floats,
                )
                allowed = allowed_block(begin_row, key_at, query_at, block, block)
                scores = jnp.where(allowed, scores, negative)
                new_high = jnp.maximum(highest, jnp.max(scores, axis=0, keepdims=True))
                shrink = jnp.exp(highest - new_high)
                weights = jnp.exp(scores - new_high)
                total = total * shrink + jnp.sum(weights, axis=0, keepdims=True)
                summed = summed * shrink + jnp.dot(
                    vt[head * HD : (head + 1) * HD, pl.ds(key_at, block)],
                    weights.astype(halves),
                    preferred_element_type=floats,
                )
                return (new_high, total, summed)

            highest, total, summed = lax.fori_loop(
                start,
                index + 1,
                one_key,
                (
                    jnp.full((1, block), negative, floats),
                    jnp.zeros((1, block), floats),
                    jnp.zeros((HD, block), floats),
                ),
            )
            ot[head * HD : (head + 1) * HD, pl.ds(query_at, block)] = summed / total
            lse_ref[head : head + 1, pl.ds(query_at, block)] = highest + jnp.log(total)
        return carry

    lax.fori_loop(0, length // block, one_query, 0)
    qs[...] = ot[...].T.astype(halves)

    def write(ref, rows, content):
        ref[rows, :] = content

    fetch_rows(place_ref, out_own, out_other, lambda rows: qs[rows, :], write)


def attend_back_kernel(
    block,
    place_ref,
    last_ref,
    begin_ref,
    own_ref,
    other_ref,
    att_own,
    att_other,
    grad_own,
    grad_other,
    lse_ref,
    cos_ref,
    up_ref,
    down_ref,
    out_own,
    out_other,
    bias_ref,
    qs,
    ks,
    kt,
    vs,
    gs,
    at,
    dq,
    dk,
    dv,
    delta,
):
    floats, halves = jnp.float32, jnp.bfloat16
    length = qs.shape[0]
    scale = jnp.asarray(1.0 / math.sqrt(HD), halves)
    place_rows(place_ref, own_ref, other_ref, qs, lambda ref, rows: ref[0, rows, :] * scale)
    place_rows(place_ref, own_ref, other_ref, ks, lambda ref, rows: ref[1, rows, :])
    place_rows(place_ref, own_ref, other_ref, vs, lambda ref, rows: ref[2, rows, :])
    place_rows(place_ref, grad_own, grad_other, gs, lambda ref, rows: ref[rows, :])
    place_rows(place_ref, att_own, att_other, at, lambda ref, rows: ref[rows, :])
    kt[...] = (ks[...] * scale).astype(floats).T.astype(halves)
    pairs = gs[...].astype(floats) * at[...].astype(floats)
    whole_lanes = lax.broadcasted_iota(jnp.int32, (8, 2 * HD), 1)
    for head in range(2):
        chosen = jnp.where(head_rows(whole_lanes, head), 1.0, 0.0)
        delta[8 * head : 8 * head + 8, :] = lax.dot_general(
            chosen,
            pairs,
            (((1,), (1,)), ((), ())),
            precision=lax.Precision.HIGHEST,
            preferred_element_type=floats,
        )
    dq[...] = jnp.zeros_like(dq)
    lanes_of = lax.broadcasted_iota(jnp.int32, (block, 2 * HD), 1)

    def one_key(index, carry):
        key_at = pl.multiple_of(index * block, block)
        key_both = ks[pl.ds(key_at, block), :]
        value_both = vs[pl.ds(key_at, block), :]
        finish = last_ref[index]

        def one_query(step, running):
            grad_key, grad_value = running
            query_at = pl.multiple_of(step * block, block)
            query_both = qs[pl.ds(query_at, block), :]
            grad_both = gs[pl.ds(query_at, block), :]
            begin_row = begin_ref[:, pl.ds(query_at, block)]
            allowed = allowed_block(begin_row, key_at, query_at, block, block)
            for head in range(2):
                chosen = head_rows(lanes_of, head)
                query_head = jnp.where(chosen, query_both, jnp.zeros_like(query_both))
                grad_head = jnp.where(chosen, grad_both, jnp.zeros_like(grad_both))
                scores = lax.dot_general(
                    key_both, query_head, (((1,), (1,)), ((), ())), preferred_element_type=floats
                )
                lse_row = lse_ref[head : head + 1, pl.ds(query_at, block)]
                probs = jnp.where(allowed, jnp.exp(scores - lse_row), 0.0)
                grad_probs = lax.dot_general(
                    value_both, grad_head, (((1,), (1,)), ((), ())), preferred_element_type=floats
                )
                delta_row = delta[8 * head : 8 * head + 1, pl.ds(query_at, block)]
                grad_scores = (probs * (grad_probs - delta_row)).astype(halves)
                grad_value = grad_value + jnp.dot(
                    probs.astype(halves), grad_head, preferred_element_type=floats
                )
                grad_key = grad_key + jnp.dot(
                    grad_scores, query_head, preferred_element_type=floats
                )
                rows = pl.ds(head * HD, HD)
                dq[rows, pl.ds(query_at, block)] += jnp.dot(
                    kt[rows, pl.ds(key_at, block)], grad_scores, preferred_element_type=floats
                )
            return (grad_key, grad_value)

        zero = jnp.zeros((block, 2 * HD), floats)
        grad_key, grad_value = lax.fori_loop(index, finish, one_query, (zero, zero))
        dk[pl.ds(key_at, block), :] = grad_key
        dv[pl.ds(key_at, block), :] = grad_value
        return carry

    lax.fori_loop(0, length // block, one_key, 0)

    def turn_back(rows, content):
        return (
            content * cos_ref[rows, :]
            - pltpu.roll(content, 8, 1) * up_ref[rows, :]
            - pltpu.roll(content, 2 * HD - 8, 1) * down_ref[rows, :]
        )

    sums = [jnp.zeros((1, 2 * HD), floats)] * 3
    for part in range(length // block):
        rows = pl.ds(part * block, block)
        parts = (
            turn_back(rows, dq[:, rows].T),
            turn_back(rows, dk[rows, :]),
            dv[rows, :],
        )
        for kind in range(3):
            sums[kind] = sums[kind] + jnp.sum(parts[kind], axis=0, keepdims=True)
        qs[rows, :] = parts[0].astype(halves)
        ks[rows, :] = parts[1].astype(halves)
        vs[rows, :] = parts[2].astype(halves)
    for kind in range(3):
        bias_ref[kind : kind + 1, :] = sums[kind]

        def write(ref, rows, content, kind=kind):
            ref[kind, rows, :] = content

        held = (qs, ks, vs)[kind]
        fetch_rows(place_ref, out_own, out_other, lambda rows, held=held: held[rows, :], write)


MESH_IDS = pl.DeviceIdType.MESH
CHUNKS = 4
CHUNK = QUARTER // CHUNKS


def remote(source, goal, send_sem, recv_sem, where):
    return pltpu.make_async_remote_copy(
        src_ref=source,
        dst_ref=goal,
        send_sem=send_sem,
        recv_sem=recv_sem,
        device_id=where,
        device_id_type=MESH_IDS,
    )


class Sent:
    def __init__(self):
        self.moves = []

    def start(self, move, condition=None):
        self.moves.append((move, condition))
        guarded(condition, move.start)

    def finish(self):
        for move, condition in self.moves:
            guarded(condition, move.wait_send)


def guarded(condition, action):
    if condition is None:
        action()
    else:
        pl.when(condition)(action)


def greet(others):
    barrier = pltpu.get_barrier_semaphore()
    count = 0
    for where, condition in others:
        def signal(where=where):
            pl.semaphore_signal(barrier, inc=1, device_id=where, device_id_type=MESH_IDS)

        guarded(condition, signal)
        count = count + (1 if condition is None else condition.astype(jnp.int32))
    pl.semaphore_wait(barrier, count)


def line_peers(at_z, at_c):
    return [
        ({"z": jnp.maximum(at_z - 1, 0)}, at_z > 0),
        ({"z": jnp.minimum(at_z + 1, LINE - 1)}, at_z < LINE - 1),
        ({"c": 1 - at_c}, None),
    ]


class Reduce:
    def __init__(self, sent, at_z, at_c, send_ref, keep_ref, acc_ref, scratch):
        self.sent, self.at_z, self.at_c = sent, at_z, at_c
        self.send_ref, self.keep_ref, self.acc_ref = send_ref, keep_ref, acc_ref
        (
            self.came,
            self.down_from,
            self.above_from,
            self.down_to,
            self.above_to,
            self.core_out,
            self.core_in,
            self.down_out,
            self.down_in,
            self.above_out,
            self.above_in,
        ) = scratch

    def core_move(self, block, part):
        rows = pl.ds(block * QUARTER + part * CHUNK, CHUNK)
        return remote(
            self.send_ref.at[rows, :],
            self.came.at[rows, :],
            self.core_out.at[block, part],
            self.core_in.at[block, part],
            {"c": 1 - self.at_c},
        )

    def down_move(self, step, part):
        rows = pl.ds(part * CHUNK, CHUNK)
        return remote(
            self.down_from.at[step - 1, rows, :],
            self.down_to.at[step - 1, rows, :],
            self.down_out.at[step - 1, part],
            self.down_in.at[step - 1, part],
            {"z": jnp.maximum(self.at_z - 1, 0)},
        )

    def above_move(self, step, part):
        rows = pl.ds(part * CHUNK, CHUNK)
        return remote(
            self.above_from.at[step - 1, rows, :],
            self.above_to.at[step - 1, rows, :],
            self.above_out.at[step - 1, part],
            self.above_in.at[step - 1, part],
            {"z": jnp.minimum(self.at_z + 1, LINE - 1)},
        )

    def local(self, block, part):
        rows = pl.ds(block * QUARTER + part * CHUNK, CHUNK)
        return self.keep_ref[rows, :] + self.came[rows, :].astype(jnp.float32)

    def stage(self, step, part):
        at_z, rows = self.at_z, pl.ds(part * CHUNK, CHUNK)
        last = LINE - 1
        if step == 0:
            for block in (1, 3, 2, 0):
                self.sent.start(self.core_move(block, part))
            return
        if step <= last:
            for block in {1: (1, 3), 2: (2,), 3: (0,)}[step]:
                self.core_move(block, part).wait_recv()
            falling = at_z >= LINE - step
            rising = at_z <= step - 1

            def lead_down():
                self.down_from[step - 1, rows, :] = self.local(step, part).astype(jnp.bfloat16)

            def add_down():
                self.down_move(step - 1, part).wait_recv()
                held = self.down_to[step - 2, rows, :].astype(jnp.float32)
                self.down_from[step - 1, rows, :] = (self.local(step, part) + held).astype(
                    jnp.bfloat16
                )

            def lead_above():
                self.above_from[step - 1, rows, :] = self.local(LINE - step, part).astype(
                    jnp.bfloat16
                )

            def add_above():
                self.above_move(step - 1, part).wait_recv()
                held = self.above_to[step - 2, rows, :].astype(jnp.float32)
                self.above_from[step - 1, rows, :] = (
                    self.local(LINE - step, part) + held
                ).astype(jnp.bfloat16)

            pl.when(at_z == last)(lead_down)
            if step > 1:
                pl.when(falling & (at_z < last))(add_down)
            self.sent.start(self.down_move(step, part), falling)
            pl.when(at_z == 0)(lead_above)
            if step > 1:
                pl.when(rising & (at_z > 0))(add_above)
            self.sent.start(self.above_move(step, part), rising)
            return
        self.acc_ref[...] = self.local(0, part)

        @pl.when(at_z < last)
        def _():
            self.down_move(last, part).wait_recv()
            self.acc_ref[...] += self.down_to[last - 1, rows, :].astype(jnp.float32)

        @pl.when(at_z > 0)
        def _():
            self.above_move(last, part).wait_recv()
            self.acc_ref[...] += self.above_to[last - 1, rows, :].astype(jnp.float32)


def reduce_scratch(width):
    halves = jnp.bfloat16
    steps = (LINE - 1, CHUNKS)
    dma = pltpu.SemaphoreType.DMA
    return [
        pltpu.VMEM((LINE * QUARTER, width), halves),
        pltpu.VMEM((LINE - 1, QUARTER, width), halves),
        pltpu.VMEM((LINE - 1, QUARTER, width), halves),
        pltpu.VMEM((LINE - 1, QUARTER, width), halves),
        pltpu.VMEM((LINE - 1, QUARTER, width), halves),
        dma((LINE, CHUNKS)),
        dma((LINE, CHUNKS)),
        dma(steps),
        dma(steps),
        dma(steps),
        dma(steps),
    ]


class Gather:
    def __init__(self, sent, at_z, at_c, full_ref, scratch):
        self.sent, self.at_z, self.at_c, self.full = sent, at_z, at_c, full_ref
        (
            self.down_out,
            self.down_in,
            self.above_out,
            self.above_in,
            self.core_out,
            self.core_in,
        ) = scratch

    def rows(self, slot, part):
        return pl.ds(slot * QUARTER + part * CHUNK, CHUNK)

    def down_move(self, step, part):
        return remote(
            self.full.at[self.rows(step - 1, part), :],
            self.full.at[self.rows(step, part), :],
            self.down_out.at[step - 1, part],
            self.down_in.at[step - 1, part],
            {"z": jnp.maximum(self.at_z - 1, 0)},
        )

    def above_move(self, step, part):
        return remote(
            self.full.at[self.rows((LINE + 1 - step) % LINE, part), :],
            self.full.at[self.rows(LINE - step, part), :],
            self.above_out.at[step - 1, part],
            self.above_in.at[step - 1, part],
            {"z": jnp.minimum(self.at_z + 1, LINE - 1)},
        )

    def core_move(self, slot, part):
        return remote(
            self.full.at[self.rows(slot, part), :],
            self.full.at[self.rows(LINE + slot, part), :],
            self.core_out.at[slot, part],
            self.core_in.at[slot, part],
            {"c": 1 - self.at_c},
        )

    def stage(self, step, part):
        at_z, last = self.at_z, LINE - 1
        if step == 0:
            self.sent.start(self.down_move(1, part), at_z > 0)
            self.sent.start(self.above_move(1, part), at_z < last)
            self.sent.start(self.core_move(0, part))
            return
        if step <= last:
            from_above = at_z + step <= last
            from_below = at_z >= step
            guarded(from_above, self.down_move(step, part).wait_recv)
            if step < last:
                self.sent.start(self.down_move(step + 1, part), from_above & (at_z > 0))
            guarded(from_below, self.above_move(step, part).wait_recv)
            if step < last:
                self.sent.start(self.above_move(step + 1, part), from_below & (at_z < last))
            self.sent.start(self.core_move(step, part), from_above)
            self.sent.start(self.core_move(LINE - step, part), from_below)
            return
        for slot in range(LINE):
            self.core_move(slot, part).wait_recv()


def gather_scratch():
    dma = pltpu.SemaphoreType.DMA
    steps = (LINE - 1, CHUNKS)
    return [dma(steps)] * 4 + [dma((LINE, CHUNKS))] * 2


def pipeline(stages):
    for tick in range(CHUNKS + len(stages) - 1):
        for depth in reversed(range(len(stages))):
            part = tick - depth
            if 0 <= part < CHUNKS:
                stages[depth](part)


def row_norm(matrix_in):
    center = jnp.mean(matrix_in, axis=-1, keepdims=True)
    centered = matrix_in - center
    inverse = lax.rsqrt(jnp.mean(centered * centered, axis=-1, keepdims=True) + epsilon)
    return (centered * inverse, inverse)


REDUCE_REFS = 11
GATHER_REFS = 6


def middle_kernel(
    send_ref, keep_ref, base_ref, gain_ref, shift_ref, full_ref, residual_ref, acc_ref, *scratch
):
    at_z, at_c = lax.axis_index("z"), lax.axis_index("c")
    greet(line_peers(at_z, at_c))
    sent = Sent()
    reduce = Reduce(sent, at_z, at_c, send_ref, keep_ref, acc_ref, scratch[:REDUCE_REFS])
    gather = Gather(sent, at_z, at_c, full_ref, scratch[REDUCE_REFS:])

    def settle(part):
        rows = pl.ds(part * CHUNK, CHUNK)
        reduce.stage(LINE, part)
        residual = base_ref[rows, :] + acc_ref[...]
        residual_ref[rows, :] = residual
        normed = row_norm(residual)[0]
        full_ref[rows, :] = (normed * gain_ref[...] + shift_ref[...]).astype(full_ref.dtype)
        gather.stage(0, part)

    pipeline(
        [functools.partial(reduce.stage, step) for step in range(LINE)]
        + [settle]
        + [functools.partial(gather.stage, step) for step in range(1, LINE + 1)]
    )
    sent.finish()


def middle_back_kernel(
    send_ref,
    keep_ref,
    residual_ref,
    grad_ref,
    gain_ref,
    full_ref,
    turned_ref,
    sums_ref,
    acc_ref,
    *scratch,
):
    at_z, at_c = lax.axis_index("z"), lax.axis_index("c")
    greet(line_peers(at_z, at_c))
    sent = Sent()
    reduce = Reduce(sent, at_z, at_c, send_ref, keep_ref, acc_ref, scratch[:REDUCE_REFS])
    gather = Gather(sent, at_z, at_c, full_ref, scratch[REDUCE_REFS:])
    sums_ref[...] = jnp.zeros_like(sums_ref)

    def settle(part):
        rows = pl.ds(part * CHUNK, CHUNK)
        reduce.stage(LINE, part)
        incoming = acc_ref[...]
        normed, inverse = row_norm(residual_ref[rows, :])
        sums_ref[0:1, :] += jnp.sum(incoming * normed, axis=0, keepdims=True)
        sums_ref[1:2, :] += jnp.sum(incoming, axis=0, keepdims=True)
        turned = grad_ref[rows, :].astype(jnp.float32) + norm_back(
            incoming, normed, inverse, gain_ref[...]
        )
        turned_ref[rows, :] = turned
        full_ref[rows, :] = turned.astype(full_ref.dtype)
        gather.stage(0, part)

    pipeline(
        [functools.partial(reduce.stage, step) for step in range(LINE)]
        + [settle]
        + [functools.partial(gather.stage, step) for step in range(1, LINE + 1)]
    )
    sent.finish()


def last_kernel(
    send_ref,
    keep_ref,
    base_ref,
    turned_ref,
    gain_ref,
    early_ref,
    spread_ref,
    total_ref,
    acc_ref,
    *scratch,
):
    at_z, at_x, at_y, at_c = (lax.axis_index(name) for name in ("z", "x", "y", "c"))
    peers = [({"c": 1 - at_c}, None), ({"y": 1 - at_y}, None), ({"x": 1 - at_x}, None)]
    peers += [({"z": lax.rem(at_z + step, LINE)}, None) for step in range(1, LINE)]
    greet(peers)
    sent = Sent()
    reduce = Reduce(sent, at_z, at_c, send_ref, keep_ref, acc_ref, scratch[:REDUCE_REFS])
    spread_out, spread_in, folds, came, lines, fold_out, fold_in, line_out, line_in = scratch[
        REDUCE_REFS:
    ]
    folds[0] = early_ref[...]
    half = folds.shape[2] // 2
    span = half // LINE

    def spread_move(kind, part, arriving=False):
        slot, where, across = {
            "core": (0, {"c": 1 - at_c}, False),
            "across": (1, {"y": 1 - at_y}, False),
            "both": (2, {"c": 1 - at_c}, True),
        }[kind]
        seq, core = (1 - at_y if across else at_y), at_c
        if arriving:
            seq = 1 - seq if kind == "across" else seq
            core = 1 - core if kind != "across" else core
        rows = pl.ds(pl.multiple_of(core * QUARTER + part * CHUNK, CHUNK), CHUNK)
        return remote(
            spread_ref.at[seq, rows, :],
            spread_ref.at[seq, rows, :],
            spread_out.at[slot, part],
            spread_in.at[slot, part],
            where,
        )

    def settle(part):
        rows = pl.ds(part * CHUNK, CHUNK)
        reduce.stage(LINE, part)
        incoming = acc_ref[...]
        normed, inverse = row_norm(base_ref[rows, :])
        folds[0, 0:1, :] += jnp.sum(incoming * normed, axis=0, keepdims=True)
        folds[0, 1:2, :] += jnp.sum(incoming, axis=0, keepdims=True)
        turned = turned_ref[rows, :] + norm_back(incoming, normed, inverse, gain_ref[...])
        turned = turned.astype(spread_ref.dtype)
        goal = pl.ds(pl.multiple_of(at_c * QUARTER + part * CHUNK, CHUNK), CHUNK)
        for rel_x in range(2):
            for line in range(LINE):
                lanes = pl.multiple_of((2 * line + jnp.abs(at_x - rel_x)) * span, span)
                start = rel_x * half + line * span
                spread_ref[at_y, goal, pl.ds(lanes, span)] = turned[:, start : start + span]
        sent.start(spread_move("across", part))
        sent.start(spread_move("core", part))

    def pass_on(part):
        spread_move("across", part, arriving=True).wait_recv()
        sent.start(spread_move("both", part))

    pipeline(
        [functools.partial(reduce.stage, step) for step in range(LINE)] + [settle, pass_on]
    )
    for slot, where in enumerate(({"c": 1 - at_c}, {"y": 1 - at_y}, {"x": 1 - at_x})):
        move = remote(folds.at[slot], came.at[slot], fold_out.at[slot], fold_in.at[slot], where)
        sent.start(move)
        move.wait_recv()
        if slot < 2:
            folds[slot + 1] = folds[slot] + came[slot]
        else:
            folds[3, :, :half] = folds[2, :, :half] + came[2, :, half:]
            folds[3, :, half:] = folds[2, :, half:] + came[2, :, :half]

    def line_move(step, arriving=False):
        origin = lax.rem(at_z + LINE - step, LINE) if arriving else at_z
        return remote(
            folds.at[3],
            lines.at[origin],
            line_out.at[step - 1],
            line_in.at[step - 1],
            {"z": lax.rem(at_z + step, LINE)},
        )

    for step in range(1, LINE):
        sent.start(line_move(step))
    lines[at_z] = folds[3]
    for step in range(1, LINE):
        line_move(step, arriving=True).wait_recv()
    total_ref[...] = (lines[0] + lines[1]) + (lines[2] + lines[3])
    for part in range(CHUNKS):
        spread_move("core", part, arriving=True).wait_recv()
        spread_move("both", part, arriving=True).wait_recv()
    sent.finish()


def open_kernel(
    own_ref, part_ref, full_ref, near_ref, over_x_ref, over_y_ref, over_xy_ref, local_sem, *scratch
):
    at_z, at_x, at_y, at_c = (lax.axis_index(name) for name in ("z", "x", "y", "c"))
    peers = [({"c": 1 - at_c}, None), ({"y": 1 - at_y}, None), ({"x": 1 - at_x}, None)]
    peers += [({"z": lax.rem(at_z + step, LINE)}, None) for step in range(1, LINE)]
    greet(peers)
    sent = Sent()
    gather = Gather(sent, at_z, at_c, full_ref, scratch[:GATHER_REFS])
    trade_out, trade_in, flip_out, flip_in = scratch[GATHER_REFS:]
    rows_of = part_ref.shape[1]

    def trade_move(step, arriving=False):
        origin = lax.rem(at_z + LINE - step, LINE) if arriving else at_z
        rows = pl.ds(pl.multiple_of(origin * rows_of, rows_of), rows_of)
        return remote(
            part_ref.at[lax.rem(at_z + step, LINE)],
            near_ref.at[rows, :],
            trade_out.at[step - 1],
            trade_in.at[step - 1],
            {"z": lax.rem(at_z + step, LINE)},
        )

    def flip_move(kind, source, goal, turn, where):
        block = lax.rem(at_z + LINE - turn, LINE) * rows_of
        rows = pl.ds(pl.multiple_of(block, rows_of), rows_of)
        return remote(
            source.at[rows, :],
            goal.at[rows, :],
            flip_out.at[kind, turn],
            flip_in.at[kind, turn],
            where,
        )

    def to_x(turn):
        return flip_move(0, near_ref, over_x_ref, turn, {"x": 1 - at_x})

    def to_y(turn):
        return flip_move(1, near_ref, over_y_ref, turn, {"y": 1 - at_y})

    def to_xy(turn):
        if turn % 2 == 0:
            return flip_move(2, over_x_ref, over_xy_ref, turn, {"y": 1 - at_y})
        return flip_move(2, over_y_ref, over_xy_ref, turn, {"x": 1 - at_x})

    for step in (2, 1, 3):
        sent.start(trade_move(step))
    mine = pltpu.make_async_copy(
        part_ref.at[at_z],
        near_ref.at[pl.ds(pl.multiple_of(at_z * rows_of, rows_of), rows_of), :],
        local_sem.at[0],
    )
    mine.start()
    rows_copy = pltpu.make_async_copy(
        own_ref, full_ref.at[pl.ds(0, QUARTER), :], local_sem.at[1]
    )
    rows_copy.start()
    mine.wait()
    sent.start(to_x(0))
    sent.start(to_y(0))
    rows_copy.wait()
    for part in range(CHUNKS):
        gather.stage(0, part)
    for turn in range(1, LINE):
        trade_move(turn, arriving=True).wait_recv()
        sent.start(to_x(turn))
        sent.start(to_y(turn))
    for step in range(1, LINE):
        for part in range(CHUNKS):
            gather.stage(step, part)
        if step == 1:
            for turn in range(LINE):
                if turn % 2 == 0:
                    to_x(turn).wait_recv()
                else:
                    to_y(turn).wait_recv()
                sent.start(to_xy(turn))
    for part in range(CHUNKS):
        gather.stage(LINE, part)
    for turn in range(LINE):
        if turn % 2 == 0:
            to_y(turn).wait_recv()
        else:
            to_x(turn).wait_recv()
        to_xy(turn).wait_recv()
    sent.finish()


def qkv_kernel(
    rows_ref, near_ref, over_x_ref, over_y_ref, over_xy_ref, bias_ref, cos_ref, up_ref, down_ref, out_ref
):
    floats = jnp.float32
    width = 2 * HD
    half = near_ref.shape[0]
    for part, (first, second) in enumerate(((near_ref, over_x_ref), (over_y_ref, over_xy_ref))):
        product = jnp.dot(rows_ref[:, :half], first[...], preferred_element_type=floats)
        product = product + jnp.dot(rows_ref[:, half:], second[...], preferred_element_type=floats)
        for kind in range(3):
            content = product[:, kind * width : (kind + 1) * width]
            content = content + bias_ref[part * 3 + kind : part * 3 + kind + 1, :]
            if kind < 2:
                content = (
                    content * cos_ref[...]
                    + pltpu.roll(content, 8, 1) * up_ref[...]
                    + pltpu.roll(content, width - 8, 1) * down_ref[...]
                )
            out_ref[part, kind] = content.astype(out_ref.dtype)


def feed_kernel(
    low_ref,
    grad_ref,
    up_near,
    up_x,
    up_y,
    up_xy,
    down_near,
    down_x,
    down_y,
    down_xy,
    hidden_ref,
    turned_ref,
):
    floats = jnp.float32
    half, wide = down_near.shape
    pieces = ((up_near, up_x, down_near, down_x), (up_y, up_xy, down_y, down_xy))
    for part, (gate_a, gate_b, back_a, back_b) in enumerate(pieces):
        gate_up = jnp.dot(low_ref[:, :half], gate_a[...], preferred_element_type=floats)
        gate_up = gate_up + jnp.dot(low_ref[:, half:], gate_b[...], preferred_element_type=floats)
        grad_hidden = jnp.dot(grad_ref[:, :half], back_a[...], preferred_element_type=floats)
        grad_hidden = grad_hidden + jnp.dot(
            grad_ref[:, half:], back_b[...], preferred_element_type=floats
        )
        gate, up_part = gate_up[:, :wide], gate_up[:, wide:]
        sigmoid_gate = jax.nn.sigmoid(gate)
        silu = gate * sigmoid_gate
        hidden_ref[:, part * wide : (part + 1) * wide] = (silu * up_part).astype(hidden_ref.dtype)
        grad_gate = grad_hidden * up_part * sigmoid_gate * (1.0 + gate * (1.0 - sigmoid_gate))
        base = 2 * part * wide
        turned_ref[:, base : base + wide] = grad_gate.astype(turned_ref.dtype)
        turned_ref[:, base + wide : base + 2 * wide] = (grad_hidden * silu).astype(turned_ref.dtype)


def spread_kernel(left_ref, near_ref, over_x_ref, over_y_ref, over_xy_ref, send_ref, keep_ref):
    floats = jnp.float32
    half, width = near_ref.shape
    rows = left_ref.shape[0] // 2
    for base, (first, second) in ((0, (near_ref, over_y_ref)), (half, (over_x_ref, over_xy_ref))):
        for goal, lines in ((send_ref, slice(rows, 2 * rows)), (keep_ref, slice(0, rows))):
            product = lax.dot_general(
                left_ref[lines, :width], first[...], (((1,), (1,)), ((), ())), preferred_element_type=floats
            )
            product = product + lax.dot_general(
                left_ref[lines, width:], second[...], (((1,), (1,)), ((), ())), preferred_element_type=floats
            )
            goal[:, base : base + half] = product.astype(goal.dtype)


def whole_specs(count):
    return [pl.BlockSpec(memory_space=pltpu.VMEM)] * count


def remote_call(kernel, number, shapes, scratch, name):
    def call(*operands):
        return pl.pallas_call(
            kernel,
            out_shape=shapes,
            in_specs=whole_specs(len(operands)),
            out_specs=tuple(whole_specs(len(shapes))),
            scratch_shapes=scratch,
            compiler_params=pltpu.CompilerParams(collective_id=number, has_side_effects=True),
            name=name,
        )(*operands)

    return call


def lane_tables(offset):
    lane = jnp.arange(2 * HD, dtype=jnp.int32) % HD
    halfway = ROT // 2
    exponent = (lane % halfway).astype(jnp.float32) * (2.0 / ROT)
    frequency = jnp.exp(-math.log(10000.0) * exponent)
    angles = offset.astype(jnp.float32)[:, None] * frequency[None, :]
    cosine, sine = (jnp.cos(angles), jnp.sin(angles))
    cosine = jnp.where(lane < ROT, cosine, 1.0)
    upper = jnp.where((lane >= halfway) & (lane < ROT), sine, 0.0)
    lower = jnp.where(lane < halfway, -sine, 0.0)
    return (cosine, upper, lower)


def line_gather(own, at_z):
    down, above = [own], [own]
    for step in range(1, LINE):
        down.append(
            lax.ppermute(down[-1], "z", [(k, k - 1) for k in range(1, LINE - step + 1)])
        )
        above.append(
            lax.ppermute(above[-1], "z", [(k, k + 1) for k in range(step - 1, LINE - 1)])
        )
    blocks = [own]
    for step in range(1, LINE):
        blocks.append(jnp.where(at_z + step < LINE, down[step], above[LINE - step]))
    return jnp.concatenate(blocks + [flip(block, "c") for block in blocks], axis=0)


def line_reduce(keep, send):
    together = keep + flip(send, "c").astype(jnp.float32)
    parts = together.reshape((LINE, QUARTER) + together.shape[1:])
    down = above = None
    for step in range(1, LINE):
        falling, rising = parts[step], parts[LINE - step]
        if down is not None:
            falling, rising = falling + down.astype(jnp.float32), rising + above.astype(jnp.float32)
        down = lax.ppermute(
            falling.astype(jnp.bfloat16), "z", [(k, k - 1) for k in range(LINE - step, LINE)]
        )
        above = lax.ppermute(
            rising.astype(jnp.bfloat16), "z", [(k, k + 1) for k in range(step)]
        )
    return parts[0] + down.astype(jnp.float32) + above.astype(jnp.float32)


def line_trade(parts, at_z):
    held = jnp.zeros_like(parts)
    mine = lax.dynamic_index_in_dim(parts, at_z, 0, keepdims=True)
    held = lax.dynamic_update_slice_in_dim(held, mine, at_z, 0)
    for step in range(1, LINE):
        going = lax.dynamic_index_in_dim(parts, lax.rem(at_z + step, LINE), 0, keepdims=True)
        came = lax.ppermute(going, "z", [(k, (k + step) % LINE) for k in range(LINE)])
        held = lax.dynamic_update_slice_in_dim(held, came, lax.rem(at_z + LINE - step, LINE), 0)
    return held


def widen(parts, at_z):
    near = line_trade(parts, at_z)
    near = near.reshape(near.shape[0] * near.shape[1], near.shape[2])
    half = near.shape[0] // 2
    over_x, over_y = flip(near, "x"), flip(near, "y")
    over_xy = jnp.concatenate([flip(over_x[:half], "y"), flip(over_y[half:], "x")], axis=0)
    return (near, over_x, over_y, over_xy)


def narrow(total, at_z, first):
    floats, halves = jnp.float32, jnp.bfloat16
    half_rows, half_cols = total.shape[0] // 2, total.shape[1] // 2
    if first == "x":
        came = flip(total[half_rows:].astype(halves), "x").astype(floats)
        total = total[:half_rows] + came
        came = flip(total[:, half_cols:].astype(halves), "y").astype(floats)
        total = total[:, :half_cols] + came
    else:
        came = flip(total[:, half_cols:].astype(halves), "y").astype(floats)
        total = total[:, :half_cols] + came
        came = flip(total[half_rows:].astype(halves), "x").astype(floats)
        total = total[:half_rows] + came
    parts = total.astype(halves).reshape(LINE, half_rows // LINE, half_cols)
    return line_trade(parts, at_z)


def block_device(
    block_input,
    doc_lengths,
    ln1_gain,
    ln1_bias,
    w_qkv,
    qkv_bias,
    w_out,
    ln2_gain,
    ln2_bias,
    w_gate_up,
    w_down,
    grad_y,
):
    floats, halves = jnp.float32, jnp.bfloat16
    at_z, at_x, at_y, at_c = (lax.axis_index(name) for name in ("z", "x", "y", "c"))
    model_width = block_input.shape[2]
    shard_len = block_input.shape[1]
    head_cols = w_out.shape[1]
    hidden_cols = w_down.shape[1]
    rows_owned = w_out.shape[0]
    wide = -(-hidden_cols // (LINE * QUARTER)) * QUARTER
    cut = head_cols // LINE
    tokens = 2 * LINE * QUARTER

    def features(content):
        lead = content.shape[:-1]
        split = content.reshape(lead + (LINE, 2, rows_owned))
        near = lax.dynamic_index_in_dim(split, at_x, split.ndim - 2, keepdims=False)
        far = lax.dynamic_index_in_dim(split, 1 - at_x, split.ndim - 2, keepdims=False)
        flat = lead + (LINE * rows_owned,)
        return jnp.concatenate([near.reshape(flat), far.reshape(flat)], axis=-1)

    def plain_features(content):
        lead = content.shape[:-1]
        split = content.reshape(lead + (2, LINE, rows_owned))
        even = jnp.where(at_x == 0, split[..., 0, :, :], split[..., 1, :, :])
        odd = jnp.where(at_x == 0, split[..., 1, :, :], split[..., 0, :, :])
        return jnp.stack([even, odd], axis=-2).reshape(lead + (model_width,))

    def own_rows(content):
        seq_rows = lax.dynamic_index_in_dim(content, at_y, 0, keepdims=False)
        return features(lax.dynamic_slice_in_dim(seq_rows, at_c * QUARTER, QUARTER, 0))

    def spread_output(content):
        content = plain_features(content).astype(halves)
        beside = flip(content, "c")
        pair = jnp.concatenate(
            [
                jnp.where(at_c == 0, content, beside),
                jnp.where(at_c == 0, beside, content),
            ],
            axis=0,
        )
        across = flip(pair, "y")
        return jnp.stack(
            [jnp.where(at_y == 0, pair, across), jnp.where(at_y == 0, across, pair)], axis=0
        )

    def quarters(matrix, size):
        grown = jnp.pad(matrix, ((0, 0), (0, LINE * size - matrix.shape[1])))
        return jnp.swapaxes(grown.reshape(matrix.shape[0], LINE, size), 0, 1)

    part_qkv = jnp.concatenate([quarters(w_qkv[:, kind], cut) for kind in range(3)], axis=2)
    part_out = quarters(w_out, cut)
    part_gate_up = jnp.concatenate([quarters(w_gate_up[:, kind], wide) for kind in range(2)], axis=2)
    part_down = quarters(w_down, wide)

    lengths = lax.dynamic_index_in_dim(doc_lengths, at_y, 0, keepdims=False)
    doc_ends = jnp.cumsum(lengths)

    def begin_of(places):
        passed = (places[:, None] >= doc_ends[None, :]).astype(jnp.int32)
        return jnp.sum(passed * lengths[None, :], axis=-1)

    length = 2 * tokens
    block = 256
    all_places = jnp.arange(length, dtype=jnp.int32)
    begin_all = begin_of(all_places)
    block_begin = begin_all.reshape(length // block, block)[:, 0]
    first_block = block_begin // block
    block_ends = (jnp.arange(length // block, dtype=jnp.int32) + 1) * block
    last_block = jnp.sum((block_begin[None, :] < block_ends[:, None]).astype(jnp.int32), axis=1)
    rel = jnp.arange(tokens, dtype=jnp.int32)
    rel_c, rel_z, rel_r = rel // (LINE * QUARTER), (rel // QUARTER) % LINE, rel % QUARTER
    places = (
        ((at_z + rel_z) % LINE) * (2 * shard_len)
        + at_x * shard_len
        + jnp.abs(at_c - rel_c) * QUARTER
        + rel_r
    )
    row_tables = lane_tables(places - begin_of(places))
    all_tables = lane_tables(all_places - begin_all)
    place = jnp.stack([at_z, at_x, at_c]).astype(jnp.int32)

    input_wide = own_rows(block_input).astype(floats)
    gain1, shift1, gain2, shift2 = (features(v) for v in (ln1_gain, ln1_bias, ln2_gain, ln2_bias))
    first_norm = layer_norm(input_wide, gain1, shift1)[0]
    half_rows = model_width // 2
    piece = jax.ShapeDtypeStruct((half_rows, 3 * cut), halves)
    full_shape = jax.ShapeDtypeStruct((tokens, model_width), halves)
    dma = pltpu.SemaphoreType.DMA
    first_low, *pieces_qkv = remote_call(
        open_kernel,
        1,
        (full_shape, piece, piece, piece, piece),
        [dma((2,))] + gather_scratch() + [dma((LINE - 1,))] * 2 + [dma((3, LINE))] * 2,
        "open",
    )(first_norm.astype(halves), part_qkv)
    pieces_out = widen(part_out, at_z)
    pieces_gate_up = widen(part_gate_up, at_z)
    pieces_down = widen(part_down, at_z)
    grad_rows = line_gather(own_rows(grad_y), at_z)

    own_bias = lax.dynamic_slice_in_dim(qkv_bias, at_z * cut, cut, 1)
    bias_parts = jnp.concatenate([own_bias, flip(own_bias, "y")], axis=0)
    projected = pl.pallas_call(
        qkv_kernel,
        out_shape=jax.ShapeDtypeStruct((2, 3, tokens, cut), halves),
        in_specs=whole_specs(9),
        out_specs=pl.BlockSpec(memory_space=pltpu.VMEM),
        name="project",
    )(first_low, *pieces_qkv, bias_parts, *row_tables)
    crossed = at_x ^ at_y
    qkv_own = lax.dynamic_index_in_dim(projected, crossed, 0, keepdims=False)
    qkv_other = flip(lax.dynamic_index_in_dim(projected, 1 - crossed, 0, keepdims=False), "x")

    smem = pl.BlockSpec(memory_space=pltpu.SMEM)
    half_shape = jax.ShapeDtypeStruct((tokens, cut), halves)
    out_own, out_other, lse = pl.pallas_call(
        functools.partial(attend_kernel, block),
        out_shape=(half_shape, half_shape, jax.ShapeDtypeStruct((2, length), floats)),
        in_specs=[smem, smem] + whole_specs(3),
        out_specs=tuple(whole_specs(3)),
        scratch_shapes=[pltpu.VMEM((length, cut), halves)] * 3
        + [pltpu.VMEM((cut, length), halves), pltpu.VMEM((cut, length), floats)],
        name="attend",
    )(place, first_block, begin_all[None, :], qkv_own, qkv_other)

    def join_heads(own, other):
        near = jnp.where(crossed == 0, own, other)
        far = jnp.where(crossed == 0, other, own)
        return jnp.concatenate([near, far], axis=-1)

    attended = join_heads(out_own, flip(out_other, "x"))
    half = tokens // 2
    send_shape = jax.ShapeDtypeStruct((half, model_width), halves)
    keep_shape = jax.ShapeDtypeStruct((half, model_width), floats)
    own_shape = jax.ShapeDtypeStruct((QUARTER, model_width), floats)
    acc = pltpu.VMEM((CHUNK, model_width), floats)

    def spread(left, pieces):
        return pl.pallas_call(
            spread_kernel,
            out_shape=(send_shape, keep_shape),
            in_specs=whole_specs(5),
            out_specs=tuple(whole_specs(2)),
            name="spread",
        )(left, *pieces)

    second_low, residual = remote_call(
        middle_kernel,
        2,
        (full_shape, own_shape),
        [acc] + reduce_scratch(model_width) + gather_scratch(),
        "middle",
    )(*spread(attended, pieces_out), input_wide, gain2[None, :], shift2[None, :])
    step_rows = tokens // 2
    hidden, grad_gate_up = pl.pallas_call(
        feed_kernel,
        out_shape=(
            jax.ShapeDtypeStruct((tokens, 2 * wide), halves),
            jax.ShapeDtypeStruct((tokens, 4 * wide), halves),
        ),
        grid=(tokens // step_rows,),
        in_specs=[pl.BlockSpec((step_rows, model_width), lambda row: (row, 0))] * 2 + whole_specs(8),
        out_specs=(
            pl.BlockSpec((step_rows, 2 * wide), lambda row: (row, 0)),
            pl.BlockSpec((step_rows, 4 * wide), lambda row: (row, 0)),
        ),
        name="feed",
    )(second_low, grad_rows, *pieces_gate_up, *pieces_down)
    residual_low, grad_residual, sums2 = remote_call(
        middle_back_kernel,
        3,
        (full_shape, own_shape, jax.ShapeDtypeStruct((8, model_width), floats)),
        [acc] + reduce_scratch(model_width) + gather_scratch(),
        "middle_back",
    )(*spread(grad_gate_up, pieces_gate_up), residual, own_rows(grad_y), gain2[None, :])
    (second_low, grad_rows, hidden, grad_gate_up, out_left) = lax.optimization_barrier(
        (second_low, grad_rows, hidden, grad_gate_up, hidden, residual_low)
    )[:5]
    out_send, out_keep = spread(out_left, pieces_down)
    block_output = spread_output(residual + line_reduce(out_keep, out_send))

    def product(left_rows, right_rows):
        return lax.dot_general(
            left_rows, right_rows, (((0,), (0,)), ((), ())), preferred_element_type=floats
        )

    out_near, out_x, out_y, out_xy = pieces_out
    full_out = jnp.concatenate(
        [jnp.concatenate([out_near, out_y], axis=1), jnp.concatenate([out_x, out_xy], axis=1)], axis=0
    )
    grad_attended = jnp.dot(residual_low, full_out, preferred_element_type=floats).astype(halves)
    g_gate_up = narrow(product(second_low, grad_gate_up), at_z, "x")
    g_down = narrow(product(grad_rows, hidden), at_z, "y")
    grad_near, grad_far = grad_attended[:, :cut], grad_attended[:, cut:]
    grad_mine = jnp.where(crossed == 0, grad_near, grad_far)
    grad_their = flip(jnp.where(crossed == 0, grad_far, grad_near), "x")

    qkv_shape = jax.ShapeDtypeStruct((3, tokens, cut), halves)
    back_own, back_other, bias_sums = pl.pallas_call(
        functools.partial(attend_back_kernel, block),
        out_shape=(qkv_shape, qkv_shape, jax.ShapeDtypeStruct((3, cut), floats)),
        in_specs=[smem, smem] + whole_specs(11),
        out_specs=tuple(whole_specs(3)),
        scratch_shapes=[
            pltpu.VMEM((length, cut), halves),
            pltpu.VMEM((length, cut), halves),
            pltpu.VMEM((cut, length), halves),
            pltpu.VMEM((length, cut), halves),
            pltpu.VMEM((length, cut), halves),
            pltpu.VMEM((length, cut), halves),
            pltpu.VMEM((cut, length), floats),
            pltpu.VMEM((length, cut), floats),
            pltpu.VMEM((length, cut), floats),
            pltpu.VMEM((16, length), floats),
        ],
        name="attend_back",
    )(
        place,
        last_block,
        begin_all[None, :],
        qkv_own,
        qkv_other,
        out_own,
        out_other,
        grad_mine,
        grad_their,
        lse,
        *all_tables,
    )
    came_back = flip(back_other, "x")
    near = jnp.where(crossed == 0, back_own, came_back)
    far = jnp.where(crossed == 0, came_back, back_own)
    grad_qkv = jnp.concatenate([near[0], near[1], near[2], far[0], far[1], far[2]], axis=1)
    rows_wide = jax.ShapeDtypeStruct((2, shard_len, model_width), halves)
    early = jnp.roll(sums2, 2, axis=0)
    grad_input, sums = remote_call(
        last_kernel,
        4,
        (rows_wide, jax.ShapeDtypeStruct((8, model_width), floats)),
        [acc]
        + reduce_scratch(model_width)
        + [
            dma((3, CHUNKS)),
            dma((3, CHUNKS)),
            pltpu.VMEM((4, 8, model_width), floats),
            pltpu.VMEM((3, 8, model_width), floats),
            pltpu.VMEM((LINE, 8, model_width), floats),
            dma((3,)),
            dma((3,)),
            dma((LINE - 1,)),
            dma((LINE - 1,)),
        ],
        "last",
    )(*spread(grad_qkv, pieces_qkv), input_wide, grad_residual, gain1[None, :], early)
    sums = plain_features(sums[:4])
    g_qkv = narrow(product(first_low, grad_qkv), at_z, "y")
    g_out = narrow(product(residual_low, attended), at_z, "y")
    bias_sums = bias_sums + flip(bias_sums, "y")
    bias_sums = jnp.where(crossed == 0, bias_sums, flip(bias_sums, "x"))
    bias_all = jnp.zeros((LINE, 3, cut), floats)
    bias_all = lax.dynamic_update_slice_in_dim(bias_all, bias_sums[None], at_z, 0)
    for step in range(1, LINE):
        came = lax.ppermute(bias_sums, "z", [(k, (k + step) % LINE) for k in range(LINE)])
        bias_all = lax.dynamic_update_slice_in_dim(
            bias_all, came[None], lax.rem(at_z + LINE - step, LINE), 0
        )
    g_bias = jnp.swapaxes(bias_all, 0, 1).reshape(3, head_cols)

    def columns(parts, offset, size, count):
        matrix = jnp.swapaxes(parts[:, :, offset : offset + size], 0, 1)
        return matrix.reshape(rows_owned, LINE * size)[:, :count].astype(floats)

    grad_w_qkv = jnp.stack([columns(g_qkv, kind * cut, cut, head_cols) for kind in range(3)], axis=1)
    grad_w_gate_up = jnp.stack(
        [columns(g_gate_up, kind * wide, wide, hidden_cols) for kind in range(2)], axis=1
    )
    return (
        block_output,
        grad_input,
        sums[0],
        sums[1],
        grad_w_qkv,
        g_bias,
        columns(g_out, 0, cut, head_cols),
        sums[2],
        sums[3],
        grad_w_gate_up,
        columns(g_down, 0, wide, hidden_cols),
    )


def solution(mesh):
    sizes = (mesh.shape["fsdp"], mesh.shape["tp"])
    if sizes == (2 * LINE, 4):
        names = ("z", "x", "y", "c")
        rows, cols = ("z", "x"), ("y", "c")
        mesh = Mesh(mesh.devices.reshape(LINE, 2, 2, 2), names)
        device_step = block_device
    else:
        rows, cols = "fsdp", "tp"
        device_step = on_device
    placed = (
        P(None, rows, None),
        P(),
        P(),
        P(),
        P(rows, None, cols),
        P(None, cols),
        P(rows, cols),
        P(),
        P(),
        P(rows, None, cols),
        P(rows, cols),
        P(None, rows, None),
    )
    return jax.shard_map(
        device_step,
        mesh=mesh,
        in_specs=placed,
        out_specs=(
            P(None, rows, None),
            P(None, rows, None),
            P(),
            P(),
            P(rows, None, cols),
            P(None, cols),
            P(rows, cols),
            P(),
            P(),
            P(rows, None, cols),
            P(rows, cols),
        ),
        check_vma=False,
    )
```

```python
import functools
import math

import jax
import jax.numpy as jnp
from jax import lax
from jax.experimental import pallas as pl
from jax.experimental.pallas import tpu as pltpu
from jax.sharding import Mesh
from jax.sharding import PartitionSpec as P

HD = 64
ROT = 16
LEN = 2048
SEQ_MB = 1
MICRO = 2


epsilon = 1e-05
negative = -1e30


def layer_norm(matrix_in, norm_gain, norm_shift):
    center = jnp.mean(matrix_in, axis=-1, keepdims=True)
    centered = matrix_in - center
    spread = jnp.mean(centered * centered, axis=-1, keepdims=True)
    inverse = lax.rsqrt(spread + epsilon)
    normed = centered * inverse
    return (normed * norm_gain + norm_shift, normed, inverse)


def norm_back(incoming, normed, inverse, norm_gain):
    scaled = incoming * norm_gain
    first_mean = jnp.mean(scaled, axis=-1, keepdims=True)
    cross_mean = jnp.mean(scaled * normed, axis=-1, keepdims=True)
    return inverse * (scaled - first_mean - normed * cross_mean)


def doc_layout(lengths, places):
    doc_ends = jnp.cumsum(lengths, axis=-1)
    passed = (places[:, :, None] >= doc_ends[:, None, :]).astype(jnp.int32)
    segment = jnp.sum(passed, axis=-1)
    begins = jnp.sum(passed * lengths[:, None, :], axis=-1)
    return (segment, places - begins)


def rotary_tables(offset):
    halfway = ROT // 2
    exponent = jnp.arange(halfway, dtype=jnp.float32) * (2.0 / ROT)
    frequency = jnp.exp(-math.log(10000.0) * exponent)
    angles = offset.astype(jnp.float32)[..., None] * frequency
    return (jnp.cos(angles), jnp.sin(angles))


def rotate(head_rows, cosine_table, sine_table, direction):
    halfway = ROT // 2
    leading = head_rows[..., :halfway]
    behind = head_rows[..., halfway:ROT]
    cosine_part = cosine_table[..., None, :]
    sine_part = sine_table[..., None, :] * direction
    return jnp.concatenate(
        [
            leading * cosine_part - behind * sine_part,
            behind * cosine_part + leading * sine_part,
            head_rows[..., ROT:],
        ],
        axis=-1,
    )


def pair_mask(query_seg, query_place, key_seg, key_place):
    same_doc = query_seg[:, :, None] == key_seg[:, None, :]
    causal = key_place[:, None, :] <= query_place[:, :, None]
    return (same_doc & causal)[:, :, None, :]


def fold_blocks(update, folded, part_arrays, block_len):
    extent = part_arrays[0].shape[1]
    number = extent // block_len
    blocks = tuple(
        (
            jnp.swapaxes(
                part_array.reshape((part_array.shape[0], number, block_len) + part_array.shape[2:]),
                0,
                1,
            )
            for part_array in part_arrays
        )
    )

    def advance(running, element):
        block_index, block_parts = element
        return (update(running, block_parts, block_index * block_len), None)

    folded, unused = lax.scan(advance, folded, (jnp.arange(number, dtype=jnp.int32), blocks))
    return folded


def fetch_weights(w_qkv, w_out, w_gate_up, w_down):
    return (
        lax.all_gather(w_qkv, "fsdp", axis=0, tiled=True),
        lax.all_gather(w_out, "fsdp", axis=0, tiled=True),
        lax.all_gather(w_gate_up, "fsdp", axis=0, tiled=True),
        lax.all_gather(w_down, "fsdp", axis=0, tiled=True),
    )


def on_device(
    block_input,
    doc_lengths,
    ln1_gain,
    ln1_bias,
    w_qkv,
    qkv_bias,
    w_out,
    ln2_gain,
    ln2_bias,
    w_gate_up,
    w_down,
    grad_y,
):
    floats = jnp.float32
    halves = jnp.bfloat16
    factor = 1.0 / math.sqrt(HD)
    per_batch = SEQ_MB
    shard_len = block_input.shape[1]
    model_width = block_input.shape[2]
    head_cols = qkv_bias.shape[1]
    heads_local = head_cols // HD
    hidden_cols = w_down.shape[1]
    row_count = per_batch * shard_len
    rows_owned = model_width // lax.axis_size("fsdp")
    first_row = lax.axis_index("fsdp") * shard_len
    query_place = jnp.broadcast_to(
        first_row + jnp.arange(shard_len, dtype=jnp.int32), (per_batch, shard_len)
    )
    key_block = min(LEN, 512)
    block_count = LEN // key_block
    g_ln1_gain = jnp.zeros((model_width,), floats)
    g_ln1_bias = jnp.zeros((model_width,), floats)
    g_ln2_gain = jnp.zeros((model_width,), floats)
    g_ln2_bias = jnp.zeros((model_width,), floats)
    g_bias = jnp.zeros((3, head_cols), floats)
    stored = []
    output_parts = []
    input_grads = []
    for batch in range(MICRO):
        lower = batch * per_batch
        seq_rows = block_input[lower : lower + per_batch]
        lengths = doc_lengths[lower : lower + per_batch]
        seq_grad = grad_y[lower : lower + per_batch]
        query_seg, offset = doc_layout(lengths, query_place)
        cosine_table, sine_table = rotary_tables(offset)
        gathered = fetch_weights(w_qkv, w_out, w_gate_up, w_down)
        full_qkv, full_out, full_gate_up, full_down = gathered
        input_wide = seq_rows.reshape(row_count, model_width).astype(floats)
        first_norm, normed1, inverse1 = layer_norm(input_wide, ln1_gain, ln1_bias)
        first_low = first_norm.astype(halves)
        projected = (
            jnp.dot(
                first_low,
                full_qkv.reshape(model_width, 3 * head_cols),
                preferred_element_type=floats,
            ).reshape(row_count, 3, head_cols)
            + qkv_bias
        )
        projected = projected.reshape(per_batch, shard_len, 3, heads_local, HD)
        query_heads = rotate(projected[:, :, 0], cosine_table, sine_table, 1.0).astype(halves)
        key_heads = rotate(projected[:, :, 1], cosine_table, sine_table, 1.0).astype(halves)
        value_heads = projected[:, :, 2].astype(halves)
        key_flat = key_heads.reshape(per_batch, shard_len, head_cols)
        value_flat = value_heads.reshape(per_batch, shard_len, head_cols)

        def attend(running, block_parts, offset_at):
            key_part, value_part = block_parts
            extent = key_part.shape[1]
            key_place = jnp.broadcast_to(
                offset_at + jnp.arange(extent, dtype=jnp.int32), (per_batch, extent)
            )
            key_seg = doc_layout(lengths, key_place)[0]
            allowed = pair_mask(query_seg, query_place, key_seg, key_place)
            scores = (
                jnp.einsum(
                    "sqhd,skhd->sqhk",
                    query_heads,
                    key_part.reshape(per_batch, extent, heads_local, HD),
                    preferred_element_type=floats,
                )
                * factor
            )
            scores = jnp.where(allowed, scores, negative)
            highest, denominator, summed = running
            new_high = jnp.maximum(highest, jnp.max(scores, axis=-1))
            shrink = jnp.exp(highest - new_high)
            weights = jnp.where(allowed, jnp.exp(scores - new_high[..., None]), 0.0)
            denominator = denominator * shrink + jnp.sum(weights, axis=-1)
            summed = summed * shrink[..., None] + jnp.einsum(
                "sqhk,skhd->sqhd",
                weights.astype(halves),
                value_part.reshape(per_batch, extent, heads_local, HD),
                preferred_element_type=floats,
            )
            return (new_high, denominator, summed)

        start_state = (
            jnp.full((per_batch, shard_len, heads_local), negative, floats),
            jnp.zeros((per_batch, shard_len, heads_local), floats),
            jnp.zeros((per_batch, shard_len, heads_local, HD), floats),
        )
        highest, denominator, summed = fold_blocks(
            attend,
            start_state,
            (
                lax.all_gather(key_flat, "fsdp", axis=1, tiled=True),
                lax.all_gather(value_flat, "fsdp", axis=1, tiled=True),
            ),
            key_block,
        )
        lse_rows = highest + jnp.log(denominator)
        attended = (summed / denominator[..., None]).astype(halves).reshape(row_count, head_cols)
        attn_part = jnp.einsum("rc,oc->ro", attended, full_out, preferred_element_type=floats)
        residual = input_wide + lax.psum(attn_part.astype(jnp.bfloat16), "tp").astype(jnp.float32)
        second_norm, normed2, inverse2 = layer_norm(residual, ln2_gain, ln2_bias)
        second_low = second_norm.astype(halves)
        gate_up = jnp.dot(
            second_low,
            full_gate_up.reshape(model_width, 2 * hidden_cols),
            preferred_element_type=floats,
        ).reshape(row_count, 2, hidden_cols)
        gate = gate_up[:, 0]
        up_part = gate_up[:, 1]
        sigmoid_gate = jax.nn.sigmoid(gate)
        hidden = (gate * sigmoid_gate * up_part).astype(halves)
        ffn_part = jnp.einsum("rf,of->ro", hidden, full_down, preferred_element_type=floats)
        residual_out = residual + lax.psum(ffn_part.astype(jnp.bfloat16), "tp").astype(jnp.float32)
        output_parts.append(residual_out.astype(halves).reshape(per_batch, shard_len, model_width))
        full_qkv, full_out, full_gate_up, full_down = (
            lax.all_gather(w_qkv, "fsdp", axis=0, tiled=True),
            lax.all_gather(w_out, "fsdp", axis=0, tiled=True),
            lax.all_gather(w_gate_up, "fsdp", axis=0, tiled=True),
            lax.all_gather(w_down, "fsdp", axis=0, tiled=True),
        )
        grad_rows = seq_grad.reshape(row_count, model_width)
        grad_hidden = jnp.dot(grad_rows, full_down, preferred_element_type=floats)
        grad_gate = grad_hidden * up_part * sigmoid_gate * (1.0 + gate * (1.0 - sigmoid_gate))
        grad_upper = grad_hidden * gate * sigmoid_gate
        grad_gate_up = (
            jnp.stack([grad_gate, grad_upper], axis=1)
            .astype(halves)
            .reshape(row_count, 2 * hidden_cols)
        )
        second_part = jnp.einsum(
            "rg,dg->rd",
            grad_gate_up,
            full_gate_up.reshape(model_width, 2 * hidden_cols),
            preferred_element_type=floats,
        )
        grad_second = lax.psum(second_part.astype(jnp.bfloat16), "tp").astype(jnp.float32)
        grad_residual = grad_rows.astype(floats) + norm_back(
            grad_second, normed2, inverse2, ln2_gain
        )
        g_ln2_gain = g_ln2_gain + jnp.sum(grad_second * normed2, axis=0)
        g_ln2_bias = g_ln2_bias + jnp.sum(grad_second, axis=0)
        residual_low = grad_residual.astype(halves)
        grad_attended = jnp.dot(residual_low, full_out, preferred_element_type=floats).astype(
            halves
        )
        delta_rows = jnp.sum(
            (grad_attended.astype(floats) * attended.astype(floats)).reshape(
                per_batch, shard_len, heads_local, HD
            ),
            axis=-1,
        )
        grad_heads = grad_attended.reshape(per_batch, shard_len, heads_local, HD)
        all_keys, all_values = (
            lax.all_gather(key_flat, "fsdp", axis=1, tiled=True),
            lax.all_gather(value_flat, "fsdp", axis=1, tiled=True),
        )

        def backward_block(running, block_index):
            offset_at = block_index * key_block
            key_part = lax.dynamic_slice_in_dim(all_keys, offset_at, key_block, 1).reshape(
                per_batch, key_block, heads_local, HD
            )
            value_part = lax.dynamic_slice_in_dim(all_values, offset_at, key_block, 1).reshape(
                per_batch, key_block, heads_local, HD
            )
            key_place = jnp.broadcast_to(
                offset_at + jnp.arange(key_block, dtype=jnp.int32), (per_batch, key_block)
            )
            key_seg = doc_layout(lengths, key_place)[0]
            allowed = pair_mask(query_seg, query_place, key_seg, key_place)
            scores = (
                jnp.einsum("sqhd,skhd->sqhk", query_heads, key_part, preferred_element_type=floats)
                * factor
            )
            softmax_out = jnp.where(allowed, jnp.exp(scores - lse_rows[..., None]), 0.0)
            grad_probs = jnp.einsum(
                "sqhd,skhd->sqhk", grad_heads, value_part, preferred_element_type=floats
            )
            grad_scores = (softmax_out * (grad_probs - delta_rows[..., None]) * factor).astype(
                halves
            )
            running = running + jnp.einsum(
                "sqhk,skhd->sqhd", grad_scores, key_part, preferred_element_type=floats
            )
            key_term = jnp.einsum(
                "sqhk,sqhd->skhd", grad_scores, query_heads, preferred_element_type=floats
            )
            value_term = jnp.einsum(
                "sqhk,sqhd->skhd",
                softmax_out.astype(halves),
                grad_heads,
                preferred_element_type=floats,
            )
            return (running, (key_term, value_term))

        zero_heads = jnp.zeros((per_batch, shard_len, heads_local, HD), floats)
        grad_query, block_terms = lax.scan(
            backward_block, zero_heads, jnp.arange(block_count, dtype=jnp.int32)
        )
        key_terms = jnp.swapaxes(block_terms[0], 0, 1).reshape(per_batch, LEN, head_cols)
        value_terms = jnp.swapaxes(block_terms[1], 0, 1).reshape(per_batch, LEN, head_cols)
        grad_key, grad_value = (
            lax.psum_scatter(
                key_terms.astype(jnp.bfloat16), "fsdp", scatter_dimension=1, tiled=True
            ).astype(jnp.float32),
            lax.psum_scatter(
                value_terms.astype(jnp.bfloat16), "fsdp", scatter_dimension=1, tiled=True
            ).astype(jnp.float32),
        )
        grad_key = grad_key.reshape(per_batch, shard_len, heads_local, HD)
        grad_value = grad_value.reshape(per_batch, shard_len, heads_local, HD)
        grad_query = rotate(grad_query, cosine_table, sine_table, -1.0)
        grad_key = rotate(grad_key, cosine_table, sine_table, -1.0)
        grad_projected = jnp.stack([grad_query, grad_key, grad_value], axis=2).reshape(
            row_count, 3, head_cols
        )
        g_bias = g_bias + jnp.sum(grad_projected, axis=0)
        grad_qkv = grad_projected.astype(halves).reshape(row_count, 3 * head_cols)
        first_part = jnp.einsum(
            "rc,dc->rd",
            grad_qkv,
            full_qkv.reshape(model_width, 3 * head_cols),
            preferred_element_type=floats,
        )
        grad_first = lax.psum(first_part.astype(jnp.bfloat16), "tp").astype(jnp.float32)
        g_ln1_gain = g_ln1_gain + jnp.sum(grad_first * normed1, axis=0)
        g_ln1_bias = g_ln1_bias + jnp.sum(grad_first, axis=0)
        grad_input = (grad_residual + norm_back(grad_first, normed1, inverse1, ln1_gain)).astype(
            halves
        )
        input_grads.append(grad_input.reshape(per_batch, shard_len, model_width))
        kept_rows = (
            first_low,
            grad_qkv,
            residual_low,
            attended,
            second_low,
            grad_gate_up,
            grad_rows,
            hidden,
        )
        stored.append(kept_rows)
    joined = tuple(
        (jnp.concatenate([entry[column] for entry in stored], axis=0) for column in range(8))
    )
    first_low, grad_qkv, residual_low, attended, second_low, grad_gate_up, grad_rows, hidden = (
        joined
    )

    def product(left_rows, right_rows):
        return lax.dot_general(
            left_rows, right_rows, (((0,), (0,)), ((), ())), preferred_element_type=floats
        )

    weight_grads = lax.psum_scatter(
        jnp.concatenate(
            [
                product(first_low, grad_qkv),
                product(residual_low, attended),
                product(second_low, grad_gate_up),
                product(grad_rows, hidden),
            ],
            axis=1,
        ).astype(jnp.bfloat16),
        "fsdp",
        scatter_dimension=0,
        tiled=True,
    ).astype(jnp.float32)
    g_ln1_gain, g_ln1_bias, g_bias, g_ln2_gain, g_ln2_bias = (
        lax.psum(g_ln1_gain.astype(jnp.bfloat16), "fsdp").astype(jnp.float32),
        lax.psum(g_ln1_bias.astype(jnp.bfloat16), "fsdp").astype(jnp.float32),
        lax.psum(g_bias.astype(jnp.bfloat16), "fsdp").astype(jnp.float32),
        lax.psum(g_ln2_gain.astype(jnp.bfloat16), "fsdp").astype(jnp.float32),
        lax.psum(g_ln2_bias.astype(jnp.bfloat16), "fsdp").astype(jnp.float32),
    )
    grad_w_qkv = weight_grads[:, : 3 * head_cols].reshape(rows_owned, 3, head_cols)
    grad_w_out = weight_grads[:, 3 * head_cols : 4 * head_cols]
    grad_w_gate_up = weight_grads[:, 4 * head_cols : 4 * head_cols + 2 * hidden_cols].reshape(
        rows_owned, 2, hidden_cols
    )
    grad_w_down = weight_grads[:, 4 * head_cols + 2 * hidden_cols :]
    block_output = jnp.concatenate(output_parts, axis=0)
    grad_block = jnp.concatenate(input_grads, axis=0)
    return (
        block_output,
        grad_block,
        g_ln1_gain,
        g_ln1_bias,
        grad_w_qkv,
        g_bias,
        grad_w_out,
        g_ln2_gain,
        g_ln2_bias,
        grad_w_gate_up,
        grad_w_down,
    )


FLIP = ((0, 1), (1, 0))
LINE = 4
QUARTER = 128


def flip(block, axis):
    return lax.ppermute(block, axis, FLIP)


def head_rows(lanes_of, head):
    return (lanes_of >= head * HD) & (lanes_of < (head + 1) * HD)


def place_rows(place_ref, own_ref, other_ref, target, column):
    at_z, at_x, at_c = place_ref[0], place_ref[1], place_ref[2]
    for rel_c in range(2):
        for rel_z in range(LINE):
            source = pl.ds((rel_c * LINE + rel_z) * QUARTER, QUARTER)
            base = lax.rem(at_z + rel_z, LINE) * (4 * QUARTER) + jnp.abs(at_c - rel_c) * QUARTER
            mine = pl.multiple_of(base + at_x * (2 * QUARTER), QUARTER)
            theirs = pl.multiple_of(base + (1 - at_x) * (2 * QUARTER), QUARTER)
            target[pl.ds(mine, QUARTER), :] = column(own_ref, source)
            target[pl.ds(theirs, QUARTER), :] = column(other_ref, source)


def fetch_rows(place_ref, own_ref, other_ref, origin, write):
    at_z, at_x, at_c = place_ref[0], place_ref[1], place_ref[2]
    for rel_c in range(2):
        for rel_z in range(LINE):
            goal = pl.ds((rel_c * LINE + rel_z) * QUARTER, QUARTER)
            base = lax.rem(at_z + rel_z, LINE) * (4 * QUARTER) + jnp.abs(at_c - rel_c) * QUARTER
            mine = pl.multiple_of(base + at_x * (2 * QUARTER), QUARTER)
            theirs = pl.multiple_of(base + (1 - at_x) * (2 * QUARTER), QUARTER)
            write(own_ref, goal, origin(pl.ds(mine, QUARTER)))
            write(other_ref, goal, origin(pl.ds(theirs, QUARTER)))


def allowed_block(begin_row, key_at, query_at, key_len, query_len):
    keys = key_at + lax.broadcasted_iota(jnp.int32, (key_len, query_len), 0)
    queries = query_at + lax.broadcasted_iota(jnp.int32, (key_len, query_len), 1)
    return (keys <= queries) & (keys >= begin_row)


def doc_begins(lengths_ref, begin_ref):
    places = lax.broadcasted_iota(jnp.int32, begin_ref.shape, 1)
    begin = jnp.zeros(begin_ref.shape, jnp.int32)
    total = jnp.int32(0)
    for doc in range(lengths_ref.shape[0]):
        total = total + lengths_ref[doc]
        begin = begin + jnp.where(places >= total, lengths_ref[doc], 0)
    begin_ref[...] = begin


def begin_at(lengths_ref, place):
    begin, total = jnp.int32(0), jnp.int32(0)
    for doc in range(lengths_ref.shape[0]):
        total = total + lengths_ref[doc]
        begin = begin + jnp.where(place >= total, lengths_ref[doc], 0)
    return begin


def attend_kernel(
    block, place_ref, lengths_ref, own_ref, other_ref, out_own, out_other, lse_ref, begin_ref, qs, ks, vs, vt, ot
):
    floats, halves = jnp.float32, jnp.bfloat16
    length = qs.shape[0]
    scale = jnp.asarray(1.0 / math.sqrt(HD), halves)
    place_rows(place_ref, own_ref, other_ref, qs, lambda ref, rows: ref[0, rows, :] * scale)
    place_rows(place_ref, own_ref, other_ref, ks, lambda ref, rows: ref[1, rows, :])
    place_rows(place_ref, own_ref, other_ref, vs, lambda ref, rows: ref[2, rows, :])
    vt[...] = vs[...].astype(floats).T.astype(halves)
    doc_begins(lengths_ref, begin_ref)
    lanes_of = lax.broadcasted_iota(jnp.int32, (block, 2 * HD), 1)

    def one_query(index, carry):
        query_at = pl.multiple_of(index * block, block)
        query_both = qs[pl.ds(query_at, block), :]
        begin_row = begin_ref[:, pl.ds(query_at, block)]
        start = lax.div(begin_at(lengths_ref, query_at), block)
        for head in range(2):
            query_head = jnp.where(head_rows(lanes_of, head), query_both, jnp.zeros_like(query_both))

            def one_key(step, running):
                highest, total, summed = running
                key_at = pl.multiple_of(step * block, block)
                scores = lax.dot_general(
                    ks[pl.ds(key_at, block), :],
                    query_head,
                    (((1,), (1,)), ((), ())),
                    preferred_element_type=floats,
                )
                allowed = allowed_block(begin_row, key_at, query_at, block, block)
                scores = jnp.where(allowed, scores, negative)
                new_high = jnp.maximum(highest, jnp.max(scores, axis=0, keepdims=True))
                shrink = jnp.exp(highest - new_high)
                weights = jnp.exp(scores - new_high)
                total = total * shrink + jnp.sum(weights, axis=0, keepdims=True)
                summed = summed * shrink + jnp.dot(
                    vt[head * HD : (head + 1) * HD, pl.ds(key_at, block)],
                    weights.astype(halves),
                    preferred_element_type=floats,
                )
                return (new_high, total, summed)

            highest, total, summed = lax.fori_loop(
                start,
                index + 1,
                one_key,
                (
                    jnp.full((1, block), negative, floats),
                    jnp.zeros((1, block), floats),
                    jnp.zeros((HD, block), floats),
                ),
            )
            ot[head * HD : (head + 1) * HD, pl.ds(query_at, block)] = summed / total
            lse_ref[head : head + 1, pl.ds(query_at, block)] = highest + jnp.log(total)
        return carry

    lax.fori_loop(0, length // block, one_query, 0)
    qs[...] = ot[...].T.astype(halves)

    def write(ref, rows, content):
        ref[rows, :] = content

    fetch_rows(place_ref, out_own, out_other, lambda rows: qs[rows, :], write)


def attend_back_kernel(
    block,
    place_ref,
    lengths_ref,
    own_ref,
    other_ref,
    att_ref,
    grad_own,
    grad_other,
    lse_ref,
    cos_ref,
    up_ref,
    down_ref,
    out_own,
    out_other,
    bias_ref,
    begin_ref,
    qs,
    ks,
    kt,
    vs,
    gs,
    at,
    dq,
    dk,
    dv,
    delta,
):
    floats, halves = jnp.float32, jnp.bfloat16
    length = qs.shape[0]
    scale = jnp.asarray(1.0 / math.sqrt(HD), halves)
    place_rows(place_ref, own_ref, other_ref, qs, lambda ref, rows: ref[0, rows, :] * scale)
    place_rows(place_ref, own_ref, other_ref, ks, lambda ref, rows: ref[1, rows, :])
    place_rows(place_ref, own_ref, other_ref, vs, lambda ref, rows: ref[2, rows, :])
    place_rows(place_ref, grad_own, grad_other, gs, lambda ref, rows: ref[rows, :])
    place_rows(place_ref, att_ref.at[0], att_ref.at[1], at, lambda ref, rows: ref[rows, :])
    doc_begins(lengths_ref, begin_ref)
    kt[...] = (ks[...] * scale).astype(floats).T.astype(halves)
    pairs = gs[...].astype(floats) * at[...].astype(floats)
    whole_lanes = lax.broadcasted_iota(jnp.int32, (8, 2 * HD), 1)
    for head in range(2):
        chosen = jnp.where(head_rows(whole_lanes, head), 1.0, 0.0)
        delta[8 * head : 8 * head + 8, :] = lax.dot_general(
            chosen,
            pairs,
            (((1,), (1,)), ((), ())),
            precision=lax.Precision.HIGHEST,
            preferred_element_type=floats,
        )
    dq[...] = jnp.zeros_like(dq)
    lanes_of = lax.broadcasted_iota(jnp.int32, (block, 2 * HD), 1)

    def one_key(index, carry):
        key_at = pl.multiple_of(index * block, block)
        key_both = ks[pl.ds(key_at, block), :]
        value_both = vs[pl.ds(key_at, block), :]
        key_end = key_at + block
        finish = jnp.int32(0)
        for step in range(length // block):
            begins = begin_at(lengths_ref, step * block)
            finish = finish + jnp.where(begins < key_end, 1, 0)

        def one_query(step, running):
            grad_key, grad_value = running
            query_at = pl.multiple_of(step * block, block)
            query_both = qs[pl.ds(query_at, block), :]
            grad_both = gs[pl.ds(query_at, block), :]
            begin_row = begin_ref[:, pl.ds(query_at, block)]
            allowed = allowed_block(begin_row, key_at, query_at, block, block)
            for head in range(2):
                chosen = head_rows(lanes_of, head)
                query_head = jnp.where(chosen, query_both, jnp.zeros_like(query_both))
                grad_head = jnp.where(chosen, grad_both, jnp.zeros_like(grad_both))
                scores = lax.dot_general(
                    key_both, query_head, (((1,), (1,)), ((), ())), preferred_element_type=floats
                )
                lse_row = lse_ref[head : head + 1, pl.ds(query_at, block)]
                probs = jnp.where(allowed, jnp.exp(scores - lse_row), 0.0)
                grad_probs = lax.dot_general(
                    value_both, grad_head, (((1,), (1,)), ((), ())), preferred_element_type=floats
                )
                delta_row = delta[8 * head : 8 * head + 1, pl.ds(query_at, block)]
                grad_scores = (probs * (grad_probs - delta_row)).astype(halves)
                grad_value = grad_value + jnp.dot(
                    probs.astype(halves), grad_head, preferred_element_type=floats
                )
                grad_key = grad_key + jnp.dot(
                    grad_scores, query_head, preferred_element_type=floats
                )
                rows = pl.ds(head * HD, HD)
                dq[rows, pl.ds(query_at, block)] += jnp.dot(
                    kt[rows, pl.ds(key_at, block)], grad_scores, preferred_element_type=floats
                )
            return (grad_key, grad_value)

        zero = jnp.zeros((block, 2 * HD), floats)
        grad_key, grad_value = lax.fori_loop(index, finish, one_query, (zero, zero))
        dk[pl.ds(key_at, block), :] = grad_key
        dv[pl.ds(key_at, block), :] = grad_value
        return carry

    lax.fori_loop(0, length // block, one_key, 0)

    def turn_back(rows, content):
        return (
            content * cos_ref[rows, :]
            - pltpu.roll(content, 8, 1) * up_ref[rows, :]
            - pltpu.roll(content, 2 * HD - 8, 1) * down_ref[rows, :]
        )

    sums = [jnp.zeros((1, 2 * HD), floats)] * 3
    for part in range(length // block):
        rows = pl.ds(part * block, block)
        parts = (
            turn_back(rows, dq[:, rows].T),
            turn_back(rows, dk[rows, :]),
            dv[rows, :],
        )
        for kind in range(3):
            sums[kind] = sums[kind] + jnp.sum(parts[kind], axis=0, keepdims=True)
        qs[rows, :] = parts[0].astype(halves)
        ks[rows, :] = parts[1].astype(halves)
        vs[rows, :] = parts[2].astype(halves)
    for kind in range(3):
        bias_ref[kind : kind + 1, :] = sums[kind]

        def write(ref, rows, content, kind=kind):
            ref[kind, rows, :] = content

        held = (qs, ks, vs)[kind]
        fetch_rows(place_ref, out_own, out_other, lambda rows, held=held: held[rows, :], write)


MESH_IDS = pl.DeviceIdType.MESH
CHUNKS = 4
CHUNK = QUARTER // CHUNKS


def remote(source, goal, send_sem, recv_sem, where):
    return pltpu.make_async_remote_copy(
        src_ref=source,
        dst_ref=goal,
        send_sem=send_sem,
        recv_sem=recv_sem,
        device_id=where,
        device_id_type=MESH_IDS,
    )


class Sent:
    def __init__(self):
        self.moves = []

    def start(self, move, condition=None):
        self.moves.append((move, condition))
        guarded(condition, move.start)

    def finish(self):
        for move, condition in self.moves:
            guarded(condition, move.wait_send)


def guarded(condition, action):
    if condition is None:
        action()
    else:
        pl.when(condition)(action)


def greet(others):
    barrier = pltpu.get_barrier_semaphore()
    count = 0
    for where, condition in others:
        def signal(where=where):
            pl.semaphore_signal(barrier, inc=1, device_id=where, device_id_type=MESH_IDS)

        guarded(condition, signal)
        count = count + (1 if condition is None else condition.astype(jnp.int32))
    pl.semaphore_wait(barrier, count)


def line_peers(at_z, at_c):
    return [
        ({"z": jnp.maximum(at_z - 1, 0)}, at_z > 0),
        ({"z": jnp.minimum(at_z + 1, LINE - 1)}, at_z < LINE - 1),
        ({"c": 1 - at_c}, None),
    ]


class Reduce:
    def __init__(self, sent, at_z, at_c, send_ref, keep_ref, acc_ref, scratch):
        self.sent, self.at_z, self.at_c = sent, at_z, at_c
        self.send_ref, self.keep_ref, self.acc_ref = send_ref, keep_ref, acc_ref
        (
            self.came,
            self.down_from,
            self.above_from,
            self.down_to,
            self.above_to,
            self.core_out,
            self.core_in,
            self.down_out,
            self.down_in,
            self.above_out,
            self.above_in,
        ) = scratch

    def core_move(self, block, part):
        rows = pl.ds(block * QUARTER + part * CHUNK, CHUNK)
        return remote(
            self.send_ref.at[rows, :],
            self.came.at[rows, :],
            self.core_out.at[block, part],
            self.core_in.at[block, part],
            {"c": 1 - self.at_c},
        )

    def down_move(self, step, part):
        rows = pl.ds(part * CHUNK, CHUNK)
        return remote(
            self.down_from.at[step - 1, rows, :],
            self.down_to.at[step - 1, rows, :],
            self.down_out.at[step - 1, part],
            self.down_in.at[step - 1, part],
            {"z": jnp.maximum(self.at_z - 1, 0)},
        )

    def above_move(self, step, part):
        rows = pl.ds(part * CHUNK, CHUNK)
        return remote(
            self.above_from.at[step - 1, rows, :],
            self.above_to.at[step - 1, rows, :],
            self.above_out.at[step - 1, part],
            self.above_in.at[step - 1, part],
            {"z": jnp.minimum(self.at_z + 1, LINE - 1)},
        )

    def local(self, block, part):
        rows = pl.ds(block * QUARTER + part * CHUNK, CHUNK)
        return self.keep_ref[rows, :] + self.came[rows, :].astype(jnp.float32)

    def stage(self, step, part):
        at_z, rows = self.at_z, pl.ds(part * CHUNK, CHUNK)
        last = LINE - 1
        if step == 0:
            for block in (1, 3, 2, 0):
                self.sent.start(self.core_move(block, part))
            return
        if step <= last:
            for block in {1: (1, 3), 2: (2,), 3: (0,)}[step]:
                self.core_move(block, part).wait_recv()
            falling = at_z >= LINE - step
            rising = at_z <= step - 1

            def lead_down():
                self.down_from[step - 1, rows, :] = self.local(step, part).astype(jnp.bfloat16)

            def add_down():
                self.down_move(step - 1, part).wait_recv()
                held = self.down_to[step - 2, rows, :].astype(jnp.float32)
                self.down_from[step - 1, rows, :] = (self.local(step, part) + held).astype(
                    jnp.bfloat16
                )

            def lead_above():
                self.above_from[step - 1, rows, :] = self.local(LINE - step, part).astype(
                    jnp.bfloat16
                )

            def add_above():
                self.above_move(step - 1, part).wait_recv()
                held = self.above_to[step - 2, rows, :].astype(jnp.float32)
                self.above_from[step - 1, rows, :] = (
                    self.local(LINE - step, part) + held
                ).astype(jnp.bfloat16)

            pl.when(at_z == last)(lead_down)
            if step > 1:
                pl.when(falling & (at_z < last))(add_down)
            self.sent.start(self.down_move(step, part), falling)
            pl.when(at_z == 0)(lead_above)
            if step > 1:
                pl.when(rising & (at_z > 0))(add_above)
            self.sent.start(self.above_move(step, part), rising)
            return
        self.acc_ref[...] = self.local(0, part)

        @pl.when(at_z < last)
        def _():
            self.down_move(last, part).wait_recv()
            self.acc_ref[...] += self.down_to[last - 1, rows, :].astype(jnp.float32)

        @pl.when(at_z > 0)
        def _():
            self.above_move(last, part).wait_recv()
            self.acc_ref[...] += self.above_to[last - 1, rows, :].astype(jnp.float32)


def reduce_scratch(width):
    halves = jnp.bfloat16
    steps = (LINE - 1, CHUNKS)
    dma = pltpu.SemaphoreType.DMA
    return [
        pltpu.VMEM((LINE * QUARTER, width), halves),
        pltpu.VMEM((LINE - 1, QUARTER, width), halves),
        pltpu.VMEM((LINE - 1, QUARTER, width), halves),
        pltpu.VMEM((LINE - 1, QUARTER, width), halves),
        pltpu.VMEM((LINE - 1, QUARTER, width), halves),
        dma((LINE, CHUNKS)),
        dma((LINE, CHUNKS)),
        dma(steps),
        dma(steps),
        dma(steps),
        dma(steps),
    ]


class Gather:
    def __init__(self, sent, at_z, at_c, full_ref, scratch):
        self.sent, self.at_z, self.at_c, self.full = sent, at_z, at_c, full_ref
        (
            self.down_out,
            self.down_in,
            self.above_out,
            self.above_in,
            self.core_out,
            self.core_in,
        ) = scratch

    def rows(self, slot, part):
        return pl.ds(slot * QUARTER + part * CHUNK, CHUNK)

    def down_move(self, step, part):
        return remote(
            self.full.at[self.rows(step - 1, part), :],
            self.full.at[self.rows(step, part), :],
            self.down_out.at[step - 1, part],
            self.down_in.at[step - 1, part],
            {"z": jnp.maximum(self.at_z - 1, 0)},
        )

    def above_move(self, step, part):
        return remote(
            self.full.at[self.rows((LINE + 1 - step) % LINE, part), :],
            self.full.at[self.rows(LINE - step, part), :],
            self.above_out.at[step - 1, part],
            self.above_in.at[step - 1, part],
            {"z": jnp.minimum(self.at_z + 1, LINE - 1)},
        )

    def core_move(self, slot, part):
        return remote(
            self.full.at[self.rows(slot, part), :],
            self.full.at[self.rows(LINE + slot, part), :],
            self.core_out.at[slot, part],
            self.core_in.at[slot, part],
            {"c": 1 - self.at_c},
        )

    def stage(self, step, part):
        at_z, last = self.at_z, LINE - 1
        if step == 0:
            self.sent.start(self.down_move(1, part), at_z > 0)
            self.sent.start(self.above_move(1, part), at_z < last)
            self.sent.start(self.core_move(0, part))
            return
        if step <= last:
            from_above = at_z + step <= last
            from_below = at_z >= step
            guarded(from_above, self.down_move(step, part).wait_recv)
            if step < last:
                self.sent.start(self.down_move(step + 1, part), from_above & (at_z > 0))
            guarded(from_below, self.above_move(step, part).wait_recv)
            if step < last:
                self.sent.start(self.above_move(step + 1, part), from_below & (at_z < last))
            self.sent.start(self.core_move(step, part), from_above)
            self.sent.start(self.core_move(LINE - step, part), from_below)
            return
        for slot in range(LINE):
            self.core_move(slot, part).wait_recv()


def gather_scratch():
    dma = pltpu.SemaphoreType.DMA
    steps = (LINE - 1, CHUNKS)
    return [dma(steps)] * 4 + [dma((LINE, CHUNKS))] * 2


def pipeline(stages):
    for tick in range(CHUNKS + len(stages) - 1):
        for depth in range(len(stages)):
            part = tick - depth
            if 0 <= part < CHUNKS:
                stages[depth](part)


def row_norm(matrix_in):
    center = jnp.mean(matrix_in, axis=-1, keepdims=True)
    centered = matrix_in - center
    inverse = lax.rsqrt(jnp.mean(centered * centered, axis=-1, keepdims=True) + epsilon)
    return (centered * inverse, inverse)


REDUCE_REFS = 11
GATHER_REFS = 6


def middle_back_kernel(
    send_ref,
    keep_ref,
    residual_ref,
    grad_ref,
    gain_ref,
    full_ref,
    turned_ref,
    sums_ref,
    acc_ref,
    *scratch,
):
    at_z, at_c = lax.axis_index("z"), lax.axis_index("c")
    greet(line_peers(at_z, at_c))
    sent = Sent()
    reduce = Reduce(sent, at_z, at_c, send_ref, keep_ref, acc_ref, scratch[:REDUCE_REFS])
    gather = Gather(sent, at_z, at_c, full_ref, scratch[REDUCE_REFS:])
    sums_ref[...] = jnp.zeros_like(sums_ref)

    def settle(part):
        rows = pl.ds(part * CHUNK, CHUNK)
        reduce.stage(LINE, part)
        incoming = acc_ref[...]
        normed, inverse = row_norm(residual_ref[rows, :])
        sums_ref[0:1, :] += jnp.sum(incoming * normed, axis=0, keepdims=True)
        sums_ref[1:2, :] += jnp.sum(incoming, axis=0, keepdims=True)
        turned = grad_ref[rows, :].astype(jnp.float32) + norm_back(
            incoming, normed, inverse, gain_ref[...]
        )
        turned_ref[rows, :] = turned
        full_ref[rows, :] = turned.astype(full_ref.dtype)
        gather.stage(0, part)

    for part in range(CHUNKS):
        reduce.stage(0, part)
    pipeline(
        [functools.partial(reduce.stage, step) for step in range(1, LINE)]
        + [settle]
        + [functools.partial(gather.stage, step) for step in range(1, LINE + 1)]
    )
    sent.finish()


def last_kernel(
    send_ref,
    keep_ref,
    base_ref,
    turned_ref,
    gain_ref,
    early_ref,
    spread_ref,
    total_ref,
    acc_ref,
    *scratch,
):
    at_z, at_x, at_y, at_c = (lax.axis_index(name) for name in ("z", "x", "y", "c"))
    peers = [({"c": 1 - at_c}, None), ({"y": 1 - at_y}, None), ({"x": 1 - at_x}, None)]
    peers += [({"z": lax.rem(at_z + step, LINE)}, None) for step in range(1, LINE)]
    greet(peers)
    sent = Sent()
    reduce = Reduce(sent, at_z, at_c, send_ref, keep_ref, acc_ref, scratch[:REDUCE_REFS])
    spread_out, spread_in, folds, came, lines, fold_out, fold_in, line_out, line_in = scratch[
        REDUCE_REFS:
    ]
    folds[0] = early_ref[...]
    half = folds.shape[2] // 2
    span = half // LINE

    def spread_move(kind, part, arriving=False):
        slot, where, across = {
            "core": (0, {"c": 1 - at_c}, False),
            "across": (1, {"y": 1 - at_y}, False),
            "both": (2, {"c": 1 - at_c}, True),
        }[kind]
        seq, core = (1 - at_y if across else at_y), at_c
        if arriving:
            seq = 1 - seq if kind == "across" else seq
            core = 1 - core if kind != "across" else core
        rows = pl.ds(pl.multiple_of(core * QUARTER + part * CHUNK, CHUNK), CHUNK)
        return remote(
            spread_ref.at[seq, rows, :],
            spread_ref.at[seq, rows, :],
            spread_out.at[slot, part],
            spread_in.at[slot, part],
            where,
        )

    def settle(part):
        rows = pl.ds(part * CHUNK, CHUNK)
        reduce.stage(LINE, part)
        incoming = acc_ref[...]
        normed, inverse = row_norm(base_ref[rows, :])
        folds[0, 0:1, :] += jnp.sum(incoming * normed, axis=0, keepdims=True)
        folds[0, 1:2, :] += jnp.sum(incoming, axis=0, keepdims=True)
        turned = turned_ref[rows, :] + norm_back(incoming, normed, inverse, gain_ref[...])
        turned = turned.astype(spread_ref.dtype)
        goal = pl.ds(pl.multiple_of(at_c * QUARTER + part * CHUNK, CHUNK), CHUNK)
        for rel_x in range(2):
            for line in range(LINE):
                lanes = pl.multiple_of((2 * line + jnp.abs(at_x - rel_x)) * span, span)
                start = rel_x * half + line * span
                spread_ref[at_y, goal, pl.ds(lanes, span)] = turned[:, start : start + span]
        sent.start(spread_move("across", part))
        sent.start(spread_move("core", part))

    def pass_on(part):
        spread_move("across", part, arriving=True).wait_recv()
        sent.start(spread_move("both", part))

    for part in range(CHUNKS):
        reduce.stage(0, part)
    pipeline(
        [functools.partial(reduce.stage, step) for step in range(1, LINE)] + [settle, pass_on]
    )
    for slot, where in enumerate(({"c": 1 - at_c}, {"y": 1 - at_y}, {"x": 1 - at_x})):
        move = remote(folds.at[slot], came.at[slot], fold_out.at[slot], fold_in.at[slot], where)
        sent.start(move)
        move.wait_recv()
        if slot < 2:
            folds[slot + 1] = folds[slot] + came[slot]
        else:
            folds[3, :, :half] = folds[2, :, :half] + came[2, :, half:]
            folds[3, :, half:] = folds[2, :, half:] + came[2, :, :half]

    def line_move(step, arriving=False):
        origin = lax.rem(at_z + LINE - step, LINE) if arriving else at_z
        return remote(
            folds.at[3],
            lines.at[origin],
            line_out.at[step - 1],
            line_in.at[step - 1],
            {"z": lax.rem(at_z + step, LINE)},
        )

    for step in range(1, LINE):
        sent.start(line_move(step))
    lines[at_z] = folds[3]
    for step in range(1, LINE):
        line_move(step, arriving=True).wait_recv()
    total_ref[...] = (lines[0] + lines[1]) + (lines[2] + lines[3])
    for part in range(CHUNKS):
        spread_move("core", part, arriving=True).wait_recv()
        spread_move("both", part, arriving=True).wait_recv()
    sent.finish()


UNITS = 7


def pair_peers(at_z, at_x, at_y, at_c):
    peers = [({"c": 1 - at_c}, None), ({"y": 1 - at_y}, None), ({"x": 1 - at_x}, None)]
    return peers + [({"z": lax.rem(at_z + step, LINE)}, None) for step in range(1, LINE)]


def spots():
    return tuple(lax.axis_index(name) for name in ("z", "x", "y", "c"))


def feature_lanes(at_x, rel_x, line, span):
    return pl.ds(pl.multiple_of((2 * line + jnp.abs(at_x - rel_x)) * span, span), span)


def open_kernel(
    lengths_ref,
    rows_ref,
    grad_ref,
    gains_ref,
    qkv_ref,
    out_ref,
    gate_ref,
    up_ref,
    down_ref,
    full_ref,
    base_ref,
    grads_ref,
    turned_ref,
    cos_ref,
    high_ref,
    low_ref,
    all_qkv,
    all_out,
    all_gate_up,
    all_down,
    local_sem,
    *scratch,
):
    floats = jnp.float32
    at_z, at_x, at_y, at_c = spots()
    greet(pair_peers(at_z, at_x, at_y, at_c))
    sent = Sent()
    gather = Gather(sent, at_z, at_c, full_ref, scratch[:GATHER_REFS])
    trade_out, trade_in, flip_out, flip_in = scratch[GATHER_REFS:]
    rows_of, head_part = out_ref.shape[0], out_ref.shape[1] // LINE
    wide = gate_ref.shape[1] // LINE

    def unit(index, quarter):
        if index < 3:
            lanes = pl.ds(pl.multiple_of(quarter * head_part, head_part), head_part)
            return qkv_ref.at[index, :, lanes], all_qkv, index * head_part, head_part
        if index == 3:
            lanes = pl.ds(pl.multiple_of(quarter * head_part, head_part), head_part)
            return out_ref.at[:, lanes], all_out, 0, head_part
        lanes = pl.ds(pl.multiple_of(quarter * wide, wide), wide)
        if index < 6:
            source = (gate_ref, up_ref)[index - 4]
            return source.at[:, lanes], all_gate_up, (index - 4) * wide, wide
        return down_ref.at[:, lanes], all_down, 0, wide

    groups = ((0, 1, 2), (3,), (4, 5), (6,))
    arrays = (all_qkv, all_out, all_gate_up, all_down)

    def block_rows(turn):
        block = lax.rem(at_z + LINE - turn, LINE) * rows_of
        return pl.ds(pl.multiple_of(block, rows_of), rows_of)

    def trade_move(index, step, arriving=False):
        source, goal, base, size = unit(index, lax.rem(at_z + step, LINE))
        rows = block_rows(step if arriving else 0)
        return remote(
            source,
            goal.at[0, 0, rows, base : base + size],
            trade_out.at[index, step - 1],
            trade_in.at[index, step - 1],
            {"z": lax.rem(at_z + step, LINE)},
        )

    def local_move(index):
        source, goal, base, size = unit(index, at_z)
        return pltpu.make_async_copy(
            source, goal.at[0, 0, block_rows(0), base : base + size], local_sem.at[index]
        )

    def flip_move(which, kind, turn):
        rows = block_rows(turn)
        array = arrays[which]
        source, goal, where = (
            ((0, 0), (1, 0), {"x": 1 - at_x}),
            ((0, 0), (0, 1), {"y": 1 - at_y}),
            ((1, 0), (1, 1), {"y": 1 - at_y})
            if turn % 2 == 0
            else ((0, 1), (1, 1), {"x": 1 - at_x}),
        )[kind]
        return remote(
            array.at[source[0], source[1], rows, :],
            array.at[goal[0], goal[1], rows, :],
            flip_out.at[which * 3 + kind, turn],
            flip_in.at[which * 3 + kind, turn],
            where,
        )

    def start_trades(which):
        for step in (2, 1, 3):
            for index in groups[which]:
                sent.start(trade_move(index, step))

    def pass_first(which, turn):
        for index in groups[which]:
            if turn == 0:
                local_move(index).wait()
            else:
                trade_move(index, turn, arriving=True).wait_recv()
        sent.start(flip_move(which, 0, turn))
        sent.start(flip_move(which, 1, turn))

    def pass_second(which, turn):
        flip_move(which, 0 if turn % 2 == 0 else 1, turn).wait_recv()
        sent.start(flip_move(which, 2, turn))

    def pass_last(which, turn):
        flip_move(which, 1 if turn % 2 == 0 else 0, turn).wait_recv()
        flip_move(which, 2, turn).wait_recv()

    for index in range(UNITS):
        local_move(index).start()
    start_trades(0)
    start_trades(1)
    for which in range(4):
        pass_first(which, 0)

    own = pl.ds(pl.multiple_of(at_c * QUARTER, QUARTER), QUARTER)
    half = base_ref.shape[1] // 2
    span = half // LINE
    for rel_x in range(2):
        for line in range(LINE):
            lanes = feature_lanes(at_x, rel_x, line, span)
            goal = slice(rel_x * half + line * span, rel_x * half + (line + 1) * span)
            base_ref[:, goal] = rows_ref[at_y, own, lanes].astype(floats)
            grads_ref[:, goal] = grad_ref[at_y, own, lanes]
            turned_ref[:, goal] = gains_ref[:, lanes]
    for part in range(CHUNKS):
        rows = pl.ds(part * CHUNK, CHUNK)
        normed = row_norm(base_ref[rows, :])[0]
        full_ref[rows, :] = (normed * turned_ref[0:1, :] + turned_ref[1:2, :]).astype(full_ref.dtype)
        gather.stage(0, part)
    start_trades(2)

    length = cos_ref.shape[0]
    places = lax.broadcasted_iota(jnp.int32, (8, length), 1)
    begin = jnp.zeros((8, length), jnp.int32)
    total = jnp.int32(0)
    for doc in range(lengths_ref.shape[1]):
        size = lengths_ref[at_y, doc]
        total = total + size
        begin = begin + jnp.where(places >= total, size, 0)
    halfway = ROT // 2
    exponent = lax.broadcasted_iota(jnp.int32, (8, length), 0).astype(floats) * (2.0 / ROT)
    angles = (places - begin).astype(floats) * jnp.exp(-math.log(10000.0) * exponent)
    lane = lax.broadcasted_iota(jnp.int32, (8, 2 * HD), 1) % HD
    kind = lax.broadcasted_iota(jnp.int32, (8, 2 * HD), 0)
    low = jnp.where(lane == kind, 1.0, 0.0)
    high = jnp.where(lane == kind + halfway, 1.0, 0.0)
    still = jnp.where(lane[0:1] < ROT, 0.0, 1.0)

    def expand(table, choice):
        return lax.dot_general(
            table,
            choice,
            (((0,), (0,)), ((), ())),
            precision=lax.Precision.HIGHEST,
            preferred_element_type=floats,
        )

    cosine, sine = jnp.cos(angles), jnp.sin(angles)
    cos_ref[...] = expand(cosine, low + high) + still
    high_ref[...] = expand(sine, high)
    low_ref[...] = expand(sine, -low)

    for turn in range(1, LINE):
        pass_first(0, turn)
    for part in range(CHUNKS):
        gather.stage(1, part)
    start_trades(3)
    for which in range(4):
        pass_second(which, 0)
    for turn in range(1, LINE):
        pass_first(1, turn)
    for turn in range(1, LINE):
        pass_second(0, turn)
    for part in range(CHUNKS):
        gather.stage(2, part)
    for turn in range(1, LINE):
        pass_first(2, turn)
        pass_second(1, turn)
    for part in range(CHUNKS):
        gather.stage(3, part)
    for turn in range(1, LINE):
        pass_first(3, turn)
        pass_second(2, turn)
    for turn in range(1, LINE):
        pass_second(3, turn)
    for part in range(CHUNKS):
        gather.stage(LINE, part)
    for which in range(4):
        for turn in range(LINE):
            pass_last(which, turn)
    sent.finish()


def project_kernel(
    rows_ref,
    weight_ref,
    bias_ref,
    cos_ref,
    high_ref,
    low_ref,
    own_ref,
    other_ref,
    going_ref,
    out_sem,
    in_sem,
):
    floats = jnp.float32
    at_z, at_x, at_y, at_c = spots()
    greet([({"x": 1 - at_x}, None)])
    sent = Sent()
    width = 2 * HD
    half = weight_ref.shape[2]
    crossed = at_x ^ at_y
    group = 2 * QUARTER

    def compute(part, goal, index):
        rows = pl.ds(index * group, group)
        product = jnp.dot(rows_ref[rows, :half], weight_ref[0, part], preferred_element_type=floats)
        product = product + jnp.dot(
            rows_ref[rows, half:], weight_ref[1, part], preferred_element_type=floats
        )
        for block in range(2):
            rel = index * 2 + block
            rel_c, rel_z = rel // LINE, rel % LINE
            place = (
                lax.rem(at_z + rel_z, LINE) * (4 * QUARTER)
                + at_x * (2 * QUARTER)
                + jnp.abs(at_c - rel_c) * QUARTER
            )
            table = pl.ds(pl.multiple_of(place, QUARTER), QUARTER)
            lines = slice(block * QUARTER, (block + 1) * QUARTER)
            for kind in range(3):
                content = product[lines, kind * width : (kind + 1) * width]
                content = content + bias_ref[part * 3 + kind]
                if kind < 2:
                    content = (
                        content * cos_ref[table, :]
                        + pltpu.roll(content, 8, 1) * high_ref[table, :]
                        + pltpu.roll(content, width - 8, 1) * low_ref[table, :]
                    )
                goal[kind, pl.ds(rel * QUARTER, QUARTER), :] = content.astype(goal.dtype)

    def move(index):
        rows = pl.ds(index * group, group)
        return remote(
            going_ref.at[:, rows, :],
            other_ref.at[:, rows, :],
            out_sem.at[index],
            in_sem.at[index],
            {"x": 1 - at_x},
        )

    count = rows_ref.shape[0] // group
    for index in range(count):
        compute(1 - crossed, going_ref, index)
        sent.start(move(index))
    for index in range(count):
        compute(crossed, own_ref, index)
    for index in range(count):
        move(index).wait_recv()
    sent.finish()


def middle_kernel(
    own_ref,
    going_ref,
    weight_ref,
    base_ref,
    gains_ref,
    full_ref,
    residual_ref,
    both_ref,
    send_ref,
    keep_ref,
    acc_ref,
    flip_out,
    flip_in,
    *scratch,
):
    floats = jnp.float32
    at_z, at_x, at_y, at_c = spots()
    greet(line_peers(at_z, at_c) + [({"x": 1 - at_x}, None)])
    sent = Sent()
    reduce = Reduce(sent, at_z, at_c, send_ref, keep_ref, acc_ref, scratch[:REDUCE_REFS])
    gather = Gather(sent, at_z, at_c, full_ref, scratch[REDUCE_REFS:])
    crossed = at_x ^ at_y
    width = own_ref.shape[1]
    half = weight_ref.shape[2]
    rows_of = own_ref.shape[0] // 2

    def flip_move(side):
        rows = pl.ds(side * rows_of, rows_of)
        return remote(
            going_ref.at[rows, :],
            both_ref.at[1, rows, :],
            flip_out.at[side],
            flip_in.at[side],
            {"x": 1 - at_x},
        )

    sent.start(flip_move(1))
    sent.start(flip_move(0))
    both_ref[0] = own_ref[...]
    for side, goal in ((1, send_ref), (0, keep_ref)):
        flip_move(side).wait_recv()
        rows = slice(side * rows_of, (side + 1) * rows_of)
        for rel_x in range(2):
            product = lax.dot_general(
                both_ref[0, rows, :],
                weight_ref[rel_x, crossed],
                (((1,), (1,)), ((), ())),
                preferred_element_type=floats,
            )
            product = product + lax.dot_general(
                both_ref[1, rows, :],
                weight_ref[rel_x, 1 - crossed],
                (((1,), (1,)), ((), ())),
                preferred_element_type=floats,
            )
            goal[:, rel_x * half : (rel_x + 1) * half] = product.astype(goal.dtype)
        if side == 1:
            for part in range(CHUNKS):
                reduce.stage(0, part)

    def settle(part):
        rows = pl.ds(part * CHUNK, CHUNK)
        reduce.stage(LINE, part)
        residual = base_ref[rows, :] + acc_ref[...]
        residual_ref[rows, :] = residual
        normed = row_norm(residual)[0]
        full_ref[rows, :] = (normed * gains_ref[2:3, :] + gains_ref[3:4, :]).astype(full_ref.dtype)
        gather.stage(0, part)

    pipeline(
        [functools.partial(reduce.stage, step) for step in range(1, LINE)]
        + [settle]
        + [functools.partial(gather.stage, step) for step in range(1, LINE + 1)]
    )
    sent.finish()


def feed_kernel(
    low_ref,
    grad_ref,
    up_weight,
    down_weight,
    hidden_ref,
    turned_ref,
):
    floats = jnp.float32
    half, wide = down_weight.shape[2:]
    for part in range(2):
        gate_a, gate_b = up_weight.at[0, part], up_weight.at[1, part]
        back_a, back_b = down_weight.at[0, part], down_weight.at[1, part]
        gate_up = jnp.dot(low_ref[:, :half], gate_a[...], preferred_element_type=floats)
        gate_up = gate_up + jnp.dot(low_ref[:, half:], gate_b[...], preferred_element_type=floats)
        grad_hidden = jnp.dot(grad_ref[:, :half], back_a[...], preferred_element_type=floats)
        grad_hidden = grad_hidden + jnp.dot(
            grad_ref[:, half:], back_b[...], preferred_element_type=floats
        )
        gate, up_part = gate_up[:, :wide], gate_up[:, wide:]
        sigmoid_gate = jax.nn.sigmoid(gate)
        silu = gate * sigmoid_gate
        hidden_ref[:, part * wide : (part + 1) * wide] = (silu * up_part).astype(hidden_ref.dtype)
        grad_gate = grad_hidden * up_part * sigmoid_gate * (1.0 + gate * (1.0 - sigmoid_gate))
        base = 2 * part * wide
        turned_ref[:, base : base + wide] = grad_gate.astype(turned_ref.dtype)
        turned_ref[:, base + wide : base + 2 * wide] = (grad_hidden * silu).astype(turned_ref.dtype)


def spread_kernel(left_ref, weight_ref, send_ref, keep_ref):
    floats = jnp.float32
    half, width = weight_ref.shape[2:]
    rows = left_ref.shape[0] // 2
    for rel_x in range(2):
        base, first, second = rel_x * half, weight_ref.at[rel_x, 0], weight_ref.at[rel_x, 1]
        for goal, lines in ((send_ref, slice(rows, 2 * rows)), (keep_ref, slice(0, rows))):
            product = lax.dot_general(
                left_ref[lines, :width], first[...], (((1,), (1,)), ((), ())), preferred_element_type=floats
            )
            product = product + lax.dot_general(
                left_ref[lines, width:], second[...], (((1,), (1,)), ((), ())), preferred_element_type=floats
            )
            goal[:, base : base + half] = product.astype(goal.dtype)


def whole_specs(count):
    return [pl.BlockSpec(memory_space=pltpu.VMEM)] * count


def remote_call(kernel, number, shapes, scratch, name, in_specs=None, out_specs=None):
    def call(*operands):
        return pl.pallas_call(
            kernel,
            out_shape=shapes,
            in_specs=in_specs or whole_specs(len(operands)),
            out_specs=tuple(out_specs or whole_specs(len(shapes))),
            scratch_shapes=scratch,
            compiler_params=pltpu.CompilerParams(collective_id=number, has_side_effects=True),
            name=name,
        )(*operands)

    return call


def lane_tables(offset):
    lane = jnp.arange(2 * HD, dtype=jnp.int32) % HD
    halfway = ROT // 2
    exponent = (lane % halfway).astype(jnp.float32) * (2.0 / ROT)
    frequency = jnp.exp(-math.log(10000.0) * exponent)
    angles = offset.astype(jnp.float32)[:, None] * frequency[None, :]
    cosine, sine = (jnp.cos(angles), jnp.sin(angles))
    cosine = jnp.where(lane < ROT, cosine, 1.0)
    upper = jnp.where((lane >= halfway) & (lane < ROT), sine, 0.0)
    lower = jnp.where(lane < halfway, -sine, 0.0)
    return (cosine, upper, lower)


def line_gather(own, at_z):
    down, above = [own], [own]
    for step in range(1, LINE):
        down.append(
            lax.ppermute(down[-1], "z", [(k, k - 1) for k in range(1, LINE - step + 1)])
        )
        above.append(
            lax.ppermute(above[-1], "z", [(k, k + 1) for k in range(step - 1, LINE - 1)])
        )
    blocks = [own]
    for step in range(1, LINE):
        blocks.append(jnp.where(at_z + step < LINE, down[step], above[LINE - step]))
    return jnp.concatenate(blocks + [flip(block, "c") for block in blocks], axis=0)


def line_reduce(keep, send):
    together = keep + flip(send, "c").astype(jnp.float32)
    parts = together.reshape((LINE, QUARTER) + together.shape[1:])
    down = above = None
    for step in range(1, LINE):
        falling, rising = parts[step], parts[LINE - step]
        if down is not None:
            falling, rising = falling + down.astype(jnp.float32), rising + above.astype(jnp.float32)
        down = lax.ppermute(
            falling.astype(jnp.bfloat16), "z", [(k, k - 1) for k in range(LINE - step, LINE)]
        )
        above = lax.ppermute(
            rising.astype(jnp.bfloat16), "z", [(k, k + 1) for k in range(step)]
        )
    return parts[0] + down.astype(jnp.float32) + above.astype(jnp.float32)


def line_trade(parts, at_z):
    held = jnp.zeros_like(parts)
    mine = lax.dynamic_index_in_dim(parts, at_z, 0, keepdims=True)
    held = lax.dynamic_update_slice_in_dim(held, mine, at_z, 0)
    for step in range(1, LINE):
        going = lax.dynamic_index_in_dim(parts, lax.rem(at_z + step, LINE), 0, keepdims=True)
        came = lax.ppermute(going, "z", [(k, (k + step) % LINE) for k in range(LINE)])
        held = lax.dynamic_update_slice_in_dim(held, came, lax.rem(at_z + LINE - step, LINE), 0)
    return held


def widen(parts, at_z):
    near = line_trade(parts, at_z)
    near = near.reshape(near.shape[0] * near.shape[1], near.shape[2])
    half = near.shape[0] // 2
    over_x, over_y = flip(near, "x"), flip(near, "y")
    over_xy = jnp.concatenate([flip(over_x[:half], "y"), flip(over_y[half:], "x")], axis=0)
    return (near, over_x, over_y, over_xy)


def narrow(total, at_z, first):
    floats, halves = jnp.float32, jnp.bfloat16
    half_rows, half_cols = total.shape[0] // 2, total.shape[1] // 2
    if first == "x":
        came = flip(total[half_rows:].astype(halves), "x").astype(floats)
        total = total[:half_rows] + came
        came = flip(total[:, half_cols:].astype(halves), "y").astype(floats)
        total = total[:, :half_cols] + came
    else:
        came = flip(total[:, half_cols:].astype(halves), "y").astype(floats)
        total = total[:, :half_cols] + came
        came = flip(total[half_rows:].astype(halves), "x").astype(floats)
        total = total[:half_rows] + came
    parts = total.astype(halves).reshape(LINE, half_rows // LINE, half_cols)
    return line_trade(parts, at_z)


def block_device(
    block_input,
    doc_lengths,
    ln1_gain,
    ln1_bias,
    w_qkv,
    qkv_bias,
    w_out,
    ln2_gain,
    ln2_bias,
    w_gate_up,
    w_down,
    grad_y,
):
    floats, halves = jnp.float32, jnp.bfloat16
    at_z, at_x, at_y, at_c = (lax.axis_index(name) for name in ("z", "x", "y", "c"))
    model_width = block_input.shape[2]
    shard_len = block_input.shape[1]
    head_cols = w_out.shape[1]
    hidden_cols = w_down.shape[1]
    rows_owned = w_out.shape[0]
    wide = -(-hidden_cols // (LINE * QUARTER)) * QUARTER
    cut = head_cols // LINE
    tokens = 2 * LINE * QUARTER

    def features(content):
        lead = content.shape[:-1]
        split = content.reshape(lead + (LINE, 2, rows_owned))
        near = lax.dynamic_index_in_dim(split, at_x, split.ndim - 2, keepdims=False)
        far = lax.dynamic_index_in_dim(split, 1 - at_x, split.ndim - 2, keepdims=False)
        flat = lead + (LINE * rows_owned,)
        return jnp.concatenate([near.reshape(flat), far.reshape(flat)], axis=-1)

    def plain_features(content):
        lead = content.shape[:-1]
        split = content.reshape(lead + (2, LINE, rows_owned))
        even = jnp.where(at_x == 0, split[..., 0, :, :], split[..., 1, :, :])
        odd = jnp.where(at_x == 0, split[..., 1, :, :], split[..., 0, :, :])
        return jnp.stack([even, odd], axis=-2).reshape(lead + (model_width,))

    def own_rows(content):
        seq_rows = lax.dynamic_index_in_dim(content, at_y, 0, keepdims=False)
        return features(lax.dynamic_slice_in_dim(seq_rows, at_c * QUARTER, QUARTER, 0))

    def spread_output(content):
        content = plain_features(content).astype(halves)
        beside = flip(content, "c")
        pair = jnp.concatenate(
            [
                jnp.where(at_c == 0, content, beside),
                jnp.where(at_c == 0, beside, content),
            ],
            axis=0,
        )
        across = flip(pair, "y")
        return jnp.stack(
            [jnp.where(at_y == 0, pair, across), jnp.where(at_y == 0, across, pair)], axis=0
        )

    lengths = lax.dynamic_index_in_dim(doc_lengths, at_y, 0, keepdims=False)
    length = 2 * tokens
    block = 256
    place = jnp.stack([at_z, at_x, at_c]).astype(jnp.int32)

    def grown(matrix):
        return jnp.pad(matrix, ((0, 0), (0, LINE * wide - hidden_cols)))

    smem = pl.BlockSpec(memory_space=pltpu.SMEM)
    vmem = pl.BlockSpec(memory_space=pltpu.VMEM)
    kept = pl.BlockSpec(memory_space=pl.ANY)
    half_rows = model_width // 2
    full_shape = jax.ShapeDtypeStruct((tokens, model_width), halves)
    own_shape = jax.ShapeDtypeStruct((QUARTER, model_width), floats)
    table_shape = jax.ShapeDtypeStruct((length, cut), floats)
    dma = pltpu.SemaphoreType.DMA

    def pieces(width):
        return jax.ShapeDtypeStruct((2, 2, half_rows, width), halves)

    (
        first_low,
        input_wide,
        grad_own,
        gains,
        table_cos,
        table_high,
        table_low,
        full_qkv,
        full_out,
        full_gate_up,
        full_down,
    ) = remote_call(
        open_kernel,
        1,
        (
            full_shape,
            own_shape,
            jax.ShapeDtypeStruct((QUARTER, model_width), halves),
            jax.ShapeDtypeStruct((4, model_width), floats),
            table_shape,
            table_shape,
            table_shape,
            pieces(3 * cut),
            pieces(cut),
            pieces(2 * wide),
            pieces(wide),
        ),
        [dma((UNITS,))] + gather_scratch() + [dma((UNITS, LINE - 1))] * 2 + [dma((12, LINE))] * 2,
        "open",
        in_specs=[smem] + [vmem] * 8,
        out_specs=[vmem] * 7 + [kept] * 4,
    )(
        doc_lengths,
        block_input,
        grad_y,
        jnp.stack([ln1_gain, ln1_bias, ln2_gain, ln2_bias]),
        jnp.swapaxes(w_qkv, 0, 1),
        w_out,
        grown(w_gate_up[:, 0]),
        grown(w_gate_up[:, 1]),
        grown(w_down),
    )
    crossed = at_x ^ at_y
    own_bias = lax.dynamic_slice_in_dim(qkv_bias, at_z * cut, cut, 1)
    bias_parts = jnp.concatenate([own_bias, flip(own_bias, "y")], axis=0)[:, None, :]
    qkv_shape = jax.ShapeDtypeStruct((3, tokens, cut), halves)
    qkv_own, qkv_other = remote_call(
        project_kernel,
        5,
        (qkv_shape, qkv_shape),
        [pltpu.VMEM((3, tokens, cut), halves), dma((LINE,)), dma((LINE,))],
        "project",
    )(first_low, full_qkv, bias_parts, table_cos, table_high, table_low)

    grad_lines = [grad_own]
    for step in range(1, LINE):
        grad_lines.append(
            lax.ppermute(grad_own, "z", [(k, (k + LINE - step) % LINE) for k in range(LINE)])
        )
    grad_lines = jnp.concatenate(grad_lines, axis=0)
    grad_rows = jnp.concatenate([grad_lines, flip(grad_lines, "c")], axis=0)

    half_shape = jax.ShapeDtypeStruct((tokens, cut), halves)
    out_own, out_other, lse = pl.pallas_call(
        functools.partial(attend_kernel, block),
        out_shape=(half_shape, half_shape, jax.ShapeDtypeStruct((2, length), floats)),
        in_specs=[smem, smem] + whole_specs(2),
        out_specs=tuple(whole_specs(3)),
        scratch_shapes=[pltpu.VMEM((1, length), jnp.int32)]
        + [pltpu.VMEM((length, cut), halves)] * 3
        + [pltpu.VMEM((cut, length), halves), pltpu.VMEM((cut, length), floats)],
        name="attend",
    )(place, lengths, qkv_own, qkv_other)

    half = tokens // 2
    send_shape = jax.ShapeDtypeStruct((half, model_width), halves)
    keep_shape = jax.ShapeDtypeStruct((half, model_width), floats)
    acc = pltpu.VMEM((CHUNK, model_width), floats)

    def spread(left, pieces):
        return pl.pallas_call(
            spread_kernel,
            out_shape=(send_shape, keep_shape),
            in_specs=whole_specs(2),
            out_specs=tuple(whole_specs(2)),
            name="spread",
        )(left, pieces)

    second_low, residual, attended = remote_call(
        middle_kernel,
        2,
        (full_shape, own_shape, jax.ShapeDtypeStruct((2, tokens, cut), halves)),
        [pltpu.VMEM((half, model_width), halves), pltpu.VMEM((half, model_width), floats), acc]
        + [dma((2,))] * 2
        + reduce_scratch(model_width)
        + gather_scratch(),
        "middle",
    )(out_own, out_other, full_out, input_wide, gains)
    step_rows = tokens // 2
    hidden, grad_gate_up = pl.pallas_call(
        feed_kernel,
        out_shape=(
            jax.ShapeDtypeStruct((tokens, 2 * wide), halves),
            jax.ShapeDtypeStruct((tokens, 4 * wide), halves),
        ),
        grid=(tokens // step_rows,),
        in_specs=[pl.BlockSpec((step_rows, model_width), lambda row: (row, 0))] * 2 + whole_specs(2),
        out_specs=(
            pl.BlockSpec((step_rows, 2 * wide), lambda row: (row, 0)),
            pl.BlockSpec((step_rows, 4 * wide), lambda row: (row, 0)),
        ),
        name="feed",
    )(second_low, grad_rows, full_gate_up, full_down)
    residual_low, grad_residual, sums2 = remote_call(
        middle_back_kernel,
        3,
        (full_shape, own_shape, jax.ShapeDtypeStruct((8, model_width), floats)),
        [acc] + reduce_scratch(model_width) + gather_scratch(),
        "middle_back",
    )(*spread(grad_gate_up, full_gate_up), residual, grad_own, gains[2:3])
    (second_low, grad_rows, hidden, grad_gate_up, out_left) = lax.optimization_barrier(
        (second_low, grad_rows, hidden, grad_gate_up, hidden, residual_low)
    )[:5]
    out_send, out_keep = spread(out_left, full_down)
    block_output = spread_output(residual + line_reduce(out_keep, out_send))

    def product(left_rows, right_rows):
        return lax.dot_general(
            left_rows, right_rows, (((0,), (0,)), ((), ())), preferred_element_type=floats
        )

    joined_out = jnp.concatenate(
        [jnp.concatenate([full_out[k, 0], full_out[k, 1]], axis=1) for k in range(2)], axis=0
    )
    grad_attended = jnp.dot(residual_low, joined_out, preferred_element_type=floats).astype(halves)
    g_gate_up = narrow(product(second_low, grad_gate_up), at_z, "x")
    g_down = narrow(product(grad_rows, hidden), at_z, "y")
    grad_near, grad_far = grad_attended[:, :cut], grad_attended[:, cut:]
    grad_mine = jnp.where(crossed == 0, grad_near, grad_far)
    grad_their = flip(jnp.where(crossed == 0, grad_far, grad_near), "x")

    back_own, back_other, bias_sums = pl.pallas_call(
        functools.partial(attend_back_kernel, block),
        out_shape=(qkv_shape, qkv_shape, jax.ShapeDtypeStruct((3, cut), floats)),
        in_specs=[smem, smem] + whole_specs(9),
        out_specs=tuple(whole_specs(3)),
        scratch_shapes=[
            pltpu.VMEM((1, length), jnp.int32),
            pltpu.VMEM((length, cut), halves),
            pltpu.VMEM((length, cut), halves),
            pltpu.VMEM((cut, length), halves),
            pltpu.VMEM((length, cut), halves),
            pltpu.VMEM((length, cut), halves),
            pltpu.VMEM((length, cut), halves),
            pltpu.VMEM((cut, length), floats),
            pltpu.VMEM((length, cut), floats),
            pltpu.VMEM((length, cut), floats),
            pltpu.VMEM((16, length), floats),
        ],
        name="attend_back",
    )(
        place,
        lengths,
        qkv_own,
        qkv_other,
        jnp.stack([out_own, out_other]),
        grad_mine,
        grad_their,
        lse,
        table_cos,
        table_high,
        table_low,
    )
    came_back = flip(back_other, "x")
    near = jnp.where(crossed == 0, back_own, came_back)
    far = jnp.where(crossed == 0, came_back, back_own)
    grad_qkv = jnp.concatenate([near[0], near[1], near[2], far[0], far[1], far[2]], axis=1)
    rows_wide = jax.ShapeDtypeStruct((2, shard_len, model_width), halves)
    early = jnp.roll(sums2, 2, axis=0)
    grad_input, sums = remote_call(
        last_kernel,
        4,
        (rows_wide, jax.ShapeDtypeStruct((8, model_width), floats)),
        [acc]
        + reduce_scratch(model_width)
        + [
            dma((3, CHUNKS)),
            dma((3, CHUNKS)),
            pltpu.VMEM((4, 8, model_width), floats),
            pltpu.VMEM((3, 8, model_width), floats),
            pltpu.VMEM((LINE, 8, model_width), floats),
            dma((3,)),
            dma((3,)),
            dma((LINE - 1,)),
            dma((LINE - 1,)),
        ],
        "last",
    )(*spread(grad_qkv, full_qkv), input_wide, grad_residual, gains[0:1], early)
    sums = plain_features(sums[:4])
    g_qkv = narrow(product(first_low, grad_qkv), at_z, "y")
    near = jnp.where(crossed == 0, attended[0], attended[1])
    far = jnp.where(crossed == 0, attended[1], attended[0])
    g_out = narrow(product(residual_low, jnp.concatenate([near, far], axis=1)), at_z, "y")
    bias_sums = bias_sums + flip(bias_sums, "y")
    bias_sums = jnp.where(crossed == 0, bias_sums, flip(bias_sums, "x"))
    bias_all = jnp.zeros((LINE, 3, cut), floats)
    bias_all = lax.dynamic_update_slice_in_dim(bias_all, bias_sums[None], at_z, 0)
    for step in range(1, LINE):
        came = lax.ppermute(bias_sums, "z", [(k, (k + step) % LINE) for k in range(LINE)])
        bias_all = lax.dynamic_update_slice_in_dim(
            bias_all, came[None], lax.rem(at_z + LINE - step, LINE), 0
        )
    g_bias = jnp.swapaxes(bias_all, 0, 1).reshape(3, head_cols)

    def columns(parts, offset, size, count):
        matrix = jnp.swapaxes(parts[:, :, offset : offset + size], 0, 1)
        return matrix.reshape(rows_owned, LINE * size)[:, :count].astype(floats)

    grad_w_qkv = jnp.stack([columns(g_qkv, kind * cut, cut, head_cols) for kind in range(3)], axis=1)
    grad_w_gate_up = jnp.stack(
        [columns(g_gate_up, kind * wide, wide, hidden_cols) for kind in range(2)], axis=1
    )
    return (
        block_output,
        grad_input,
        sums[0],
        sums[1],
        grad_w_qkv,
        g_bias,
        columns(g_out, 0, cut, head_cols),
        sums[2],
        sums[3],
        grad_w_gate_up,
        columns(g_down, 0, wide, hidden_cols),
    )


def solution(mesh):
    sizes = (mesh.shape["fsdp"], mesh.shape["tp"])
    if sizes == (2 * LINE, 4):
        names = ("z", "x", "y", "c")
        rows, cols = ("z", "x"), ("y", "c")
        mesh = Mesh(mesh.devices.reshape(LINE, 2, 2, 2), names)
        device_step = block_device
    else:
        rows, cols = "fsdp", "tp"
        device_step = on_device
    placed = (
        P(None, rows, None),
        P(),
        P(),
        P(),
        P(rows, None, cols),
        P(None, cols),
        P(rows, cols),
        P(),
        P(),
        P(rows, None, cols),
        P(rows, cols),
        P(None, rows, None),
    )
    return jax.shard_map(
        device_step,
        mesh=mesh,
        in_specs=placed,
        out_specs=(
            P(None, rows, None),
            P(None, rows, None),
            P(),
            P(),
            P(rows, None, cols),
            P(None, cols),
            P(rows, cols),
            P(),
            P(),
            P(rows, None, cols),
            P(rows, cols),
        ),
        check_vma=False,
    )
```
